256 devices in a mesh: dp: 32 (over x_hi, z, core), tensor: 8 (over x_lo, y).
Axes of the slice: x: 4 (x_hi: 2, x_lo: 2; x = x_hi * 2 + x_lo), y: 4, z: 8, core: 2. Of those that a mesh axis runs over, the one named last changes fastest.
Arguments:
- hidden: bfloat16 [10240, 18432], P('dp', 'tensor'), may hold values from -6 to 6
- fixed_down_weight: bfloat16 [18432, 4608], P('tensor', 'dp'), may hold values from -4 to 4
- lowrank_factor_b: bfloat16 [18432, 16], P('tensor'), may hold values from -0.046875 to 0.046875
- lowrank_factor_a: bfloat16 [16, 4608], P(None, 'dp'), may hold values from -1.5 to 1.5
- magnitude: float32 [4608], P('tensor'), may hold values from 0.5 to 2
- cotangent: bfloat16 [10240, 4608], P('dp', 'tensor'), may hold values from -0.05908203 to 0.05908203
Outputs:
- mixed: bfloat16 [10240, 4608], P('dp', 'tensor')
- gradient_column_scale: float32 [4608], P(('tensor', 'dp'))
- gradient_factor_a: float32 [16, 4608], P(None, ('tensor', 'dp'))
- gradient_factor_b: float32 [18432, 16], P(('tensor', 'dp'))
The draws below stay inside these ranges and needn't reach their ends.
All inputs are finite; a program needn't handle non-finite values.
Results may differ from the reference program's by a relative error of at most 0.0054.
Values may be sent and summed in bfloat16 or wider, within the bound.
A program may use at most 128 MiB of HBM per device.

```python
import math
import jax
import jax.numpy as jnp
from jax import lax

MODEL_WIDTH = 4608
HALF_FEEDFORWARD = 18432
ADAPTER_RANK = 16
TOK_DEV = 320
TOKENS = 10240
N_DP = 32


def draw_fixed_down_weight(key, part):
    base = jax.random.truncated_normal(key, -4.0, 4.0, (HALF_FEEDFORWARD, MODEL_WIDTH), jnp.float32) * HALF_FEEDFORWARD ** (-0.5)
    ramp = 0.5 + jnp.arange(HALF_FEEDFORWARD, dtype=jnp.float32) / (HALF_FEEDFORWARD - 1)
    return (base * ramp[:, None]).astype(jnp.bfloat16)


def raised(array, rng, source, target, shards_of, factor):
    owner, partner = [(jnp.arange(array.shape[dim]) // (array.shape[dim] // shards_of)).reshape([-1 if axis == dim else 1 for axis in range(array.ndim)]) for dim in (source, target)]
    chosen = jax.random.permutation(rng, shards_of)[partner]
    strong = (owner == chosen) | (owner == (partner + shards_of // 2) % shards_of)
    return jnp.where(strong, factor * array, array)


def levels(key, extent, shards, low, largest):
    factor_of = 1.0
    for axis_at, shards_of in shards:
        steps = jax.random.uniform(jax.random.fold_in(jax.random.fold_in(key, 6), axis_at), (shards_of,), jnp.float32, low / len(shards), largest / len(shards))
        factor_of = factor_of * jnp.repeat(jnp.exp(steps), extent[axis_at] // shards_of).reshape((-1,) + (1,) * (len(extent) - 1 - axis_at))
    return factor_of


def normal_values(rng, extent, deviation, limit, pieces=(), held_as=jnp.bfloat16):
    gain = levels(rng, extent, pieces, -0.22, 0.18) if pieces else 1.0
    values = jax.random.normal(rng, extent, jnp.float32) * deviation * gain
    return jnp.minimum(jnp.maximum(values, -limit), limit).astype(held_as)


def bell_draw_with(own_key, extent, spread, bound, cuts, heavy, held_as=jnp.bfloat16):
    array = spread * jax.random.normal(own_key, extent, jnp.float32)
    if cuts:
        array = array * levels(own_key, extent, cuts, -0.22, 0.18)
    return jnp.clip(raised(array, jax.random.fold_in(own_key, 3), *heavy), -bound, bound).astype(held_as)


def setup_inputs(seed: int = 0) -> dict:
    arg_keys = jax.random.split(jax.random.key(seed), 7)
    return {
        "hidden": bell_draw_with(arg_keys[0], (TOKENS, HALF_FEEDFORWARD), 1.0, 6.0, ((0, 32), (1, 8)), (0, 1, 32, 2.75)),
        "fixed_down_weight": draw_fixed_down_weight(jax.random.fold_in(arg_keys[6], 71), 0),
        "lowrank_factor_b": normal_values(arg_keys[2], (HALF_FEEDFORWARD, ADAPTER_RANK), HALF_FEEDFORWARD ** -0.5, 0.046875, ((0, 8),)),
        "lowrank_factor_a": normal_values(arg_keys[3], (ADAPTER_RANK, MODEL_WIDTH), ADAPTER_RANK ** -0.5, 1.5, ((1, 32),)),
        "magnitude": jnp.clip(jnp.exp(math.log(2.0) - 1.3862944 * jax.random.uniform(arg_keys[4], (MODEL_WIDTH,), jnp.float32) ** levels(arg_keys[4], (MODEL_WIDTH,), ((0, 8),), -0.2, 0.2)), 0.5, 2.0),
        "cotangent": bell_draw_with(arg_keys[5], (TOKENS, MODEL_WIDTH), ((TOK_DEV * N_DP) ** -0.5), 0.05908203, ((0, 32), (1, 8)), (0, 1, 32, 2.75)),
    }


def squared_column_entries(fixed_down_weight, lowrank_factor_b, lowrank_factor_a):
    w_blocks = fixed_down_weight.reshape(8, HALF_FEEDFORWARD // 8, MODEL_WIDTH)
    factor_b_blocks = lowrank_factor_b.reshape(8, HALF_FEEDFORWARD // 8, ADAPTER_RANK)

    def one_block(pair):
        weight_tile_block, factor_b_block = pair
        combined_weight = weight_tile_block.astype(jnp.float32) + jnp.dot(factor_b_block, lowrank_factor_a, preferred_element_type=jnp.float32)
        return lax.optimization_barrier(jnp.sum(combined_weight * combined_weight, axis=0))
    return lax.optimization_barrier(jnp.sum(lax.map(one_block, (w_blocks, factor_b_blocks)), axis=0))

def reference(hidden, fixed_down_weight, lowrank_factor_b, lowrank_factor_a, magnitude, cotangent):
    column_norm_values = jnp.sqrt(squared_column_entries(fixed_down_weight, lowrank_factor_b, lowrank_factor_a) + 1e-06)
    scale = magnitude / column_norm_values
    lowrank_update = jnp.dot(hidden, lowrank_factor_b, preferred_element_type=jnp.float32)
    lowrank_block_update = lowrank_update.astype(jnp.bfloat16)
    prenorm_output = jnp.dot(hidden, fixed_down_weight, preferred_element_type=jnp.float32) + jnp.dot(lowrank_block_update, lowrank_factor_a, preferred_element_type=jnp.float32)
    mixed = (prenorm_output * scale).astype(jnp.bfloat16)
    cot = cotangent.astype(jnp.float32)
    gradient_column_scale = lax.optimization_barrier(jnp.sum(cot * prenorm_output, axis=0)) / column_norm_values
    prenorm_gradient_b = (cot * scale).astype(jnp.bfloat16)
    gradient_factor_a = jnp.dot(lowrank_block_update.T, prenorm_gradient_b, preferred_element_type=jnp.float32)
    backward_factor_b = jnp.dot(prenorm_gradient_b, lowrank_factor_a.T, preferred_element_type=jnp.float32).astype(jnp.bfloat16)
    gradient_factor_b = jnp.dot(hidden.T, backward_factor_b, preferred_element_type=jnp.float32)
    return (mixed, gradient_column_scale, gradient_factor_a, gradient_factor_b)
```

```python
import functools

import jax
import jax.numpy as jnp
from jax import lax
from jax.experimental import pallas as pl
from jax.experimental.pallas import tpu as pltpu
from jax.sharding import PartitionSpec as P

TOK, HID, COLS, OUT = 320, 2304, 144, 576
MESH = pl.DeviceIdType.MESH
F32, BF = jnp.float32, jnp.bfloat16
CHUNKS = ((0, 80), (80, 64))


def remote(src, dst, send, recv, dp, tensor):
    return pltpu.make_async_remote_copy(
        src_ref=src, dst_ref=dst, send_sem=send, recv_sem=recv,
        device_id=(dp, tensor), device_id_type=MESH,
    )


def kernel(h_ref, w_ref, out_ref, toks, wts, outgoing, arrived, turned, halves,
           loc_sem, w_send, w_recv, t_send, t_recv, y_send, y_recv, x_send, x_recv):
    dp, tensor = lax.axis_index("dp"), lax.axis_index("tensor")
    x_hi, z, core = dp // 16, (dp // 2) % 8, dp % 2
    x_lo, y = tensor // 4, tensor % 4
    other = 1 - core

    def dp_of(a, b, c):
        return a * 16 + b * 2 + c

    load_h = pltpu.make_async_copy(h_ref, toks.at[0, pl.ds(core * TOK, TOK)], loc_sem.at[0])
    load_w = pltpu.make_async_copy(w_ref, wts.at[0], loc_sem.at[1])
    load_h.start()
    load_w.start()

    barrier = pltpu.get_barrier_semaphore()
    peers = [(dp_of(x_hi, (z + 1) % 8, core), tensor), (dp_of(x_hi, (z + 7) % 8, core), tensor),
             (dp_of(x_hi, z, other), tensor)]
    for k in range(1, 4):
        for c in range(2):
            peers.append((dp_of(x_hi, z, c), x_lo * 4 + (y + k) % 4))
    for k in range(1, 4):
        xx = (2 * x_hi + x_lo + k) % 4
        for c in range(2):
            peers.append((dp_of(xx // 2, z, c), (xx % 2) * 4 + y))
    for p in peers:
        pl.semaphore_signal(barrier, inc=1, device_id=p, device_id_type=MESH)
    pl.semaphore_wait(barrier, len(peers))

    def w_copy(side, k, ch):
        at, n = CHUNKS[ch]
        src = 0 if k == 1 else 2 * (k - 1) - 1 + side
        dst = 7 if k == 4 else 2 * k - 1 + side
        to = (z + 1) % 8 if side == 0 else (z + 7) % 8
        return remote(wts.at[src, pl.ds(at, n)], wts.at[dst, pl.ds(at, n)],
                      w_send.at[side, k - 1, ch], w_recv.at[dst, ch], dp_of(x_hi, to, core), tensor)

    load_w.wait()
    w_copy(0, 1, 0).start()
    w_copy(1, 1, 1).start()
    w_copy(0, 1, 1).start()
    w_copy(1, 1, 0).start()
    load_h.wait()
    mine = pl.ds(core * TOK, TOK)
    own_tok = toks.at[0, mine]
    to_other = remote(own_tok, toks.at[0, mine], t_send.at[0], t_recv.at[0], dp_of(x_hi, z, other), tensor)
    to_far = remote(own_tok, toks.at[1, mine], t_send.at[1], t_recv.at[1], dp_of(1 - x_hi, z, core), tensor)
    relay = remote(toks.at[1, mine], toks.at[1, mine], t_send.at[2], t_recv.at[2], dp_of(x_hi, z, other), tensor)
    to_other.start()
    to_far.start()

    def zsrc_of(j):
        k = (j + 1) // 2
        return (z + 8 + k - 2 * k * (j % 2)) % 8

    def y_copy(j, g):
        zs = zsrc_of(j)
        return remote(outgoing.at[j, g], arrived.at[y, zs % 2, core], y_send.at[j, g],
                      y_recv.at[y, zs % 2, core], dp_of(x_hi, z, g), x_lo * 4 + zs // 2)

    def local(j, g):
        return jnp.logical_and(zsrc_of(j) // 2 == y, core == g)

    def item(j, g):
        p = lax.dot_general(toks[g], wts[j], (((1,), (1,)), ((), ())), preferred_element_type=F32)
        p = p.T.astype(BF)
        here = local(j, g)

        @pl.when(here)
        def _():
            arrived[y, zsrc_of(j) % 2, core] = p

        @pl.when(jnp.logical_not(here))
        def _():
            outgoing[j, g] = p
            y_copy(j, g).start()

    def items(lo, hi, g):
        def body(j, carry):
            item(j, g)
            return carry
        lax.fori_loop(lo, hi, body, 0)

    to_other.wait_recv()
    items(0, 1, 0)
    for k in (1, 2, 3):
        for first in (0, 1):
            for side in (0, 1):
                ch = first if side == 0 else 1 - first
                w_copy(side, k, ch).wait_recv()
                if k < 3 or first == 0:
                    w_copy(side, k + 1, ch).start()
        items(2 * k - 1, 2 * k + 1, 0)
        if k == 2:
            to_far.wait_recv()
            relay.start()
            relay.wait_recv()
            items(0, 5, 1)
    items(5, 7, 1)
    w_copy(0, 4, 0).wait_recv()
    w_copy(1, 4, 1).wait_recv()
    items(7, 8, 0)
    items(7, 8, 1)

    tok_hi = jnp.where(core == 0, x_hi, 1 - x_hi)

    def x_copy(zp, ct):
        return remote(turned.at[zp, pl.ds(ct * TOK, TOK)], halves.at[x_lo, zp], x_send.at[zp, ct],
                      x_recv.at[x_lo, zp], dp_of(tok_hi, z, ct), x_hi * 4 + y)

    def to_self(ct):
        return jnp.logical_and(jnp.logical_and(tok_hi == x_hi, x_lo == x_hi), core == ct)

    for zp in range(2):
        parts = []
        for cs in range(2):
            for k in range(4):
                ys = (y + k) % 4
                away = jnp.logical_or(k > 0, core != cs)

                def arrive(ys=ys, cs=cs):
                    remote(outgoing.at[0, 0], arrived.at[ys, zp, cs], y_send.at[0, 0], y_recv.at[ys, zp, cs],
                           dp, tensor).wait_recv()
                if k == 0:
                    pl.when(core != cs)(arrive)
                else:
                    arrive()
            total = arrived[0, zp, cs].astype(F32)
            for ys in range(1, 4):
                total = total + arrived[ys, zp, cs].astype(F32)
            parts.append(total)
        both = jnp.concatenate(parts, axis=0).T.astype(BF)
        turned[zp] = both
        for ct in range(2):
            @pl.when(to_self(ct))
            def _():
                halves[x_lo, zp] = both[ct * TOK:(ct + 1) * TOK]

            @pl.when(jnp.logical_not(to_self(ct)))
            def _():
                x_copy(zp, ct).start()

    for zp in range(2):
        for xl in range(2):
            sx_hi = x_lo
            score = jnp.where(sx_hi == x_hi, 0, 1)
            own = jnp.logical_and(jnp.logical_and(sx_hi == x_hi, xl == x_lo), score == core)

            @pl.when(jnp.logical_not(own))
            def _():
                remote(turned.at[0, pl.ds(0, TOK)], halves.at[xl, zp], x_send.at[0, 0], x_recv.at[xl, zp],
                       dp, tensor).wait_recv()
        out_ref[:, zp * 288:(zp + 1) * 288] = halves[0, zp].astype(F32) + halves[1, zp].astype(F32)

    for k in (1, 2, 3, 4):
        for side in (0, 1):
            for ch in (0, 1):
                if k < 4 or ch == side:
                    w_copy(side, k, ch).wait_send()
    to_other.wait_send()
    to_far.wait_send()
    relay.wait_send()
    def drain(j, carry):
        for g in range(2):
            @pl.when(jnp.logical_not(local(j, g)))
            def _():
                y_copy(j, g).wait_send()
        return carry
    lax.fori_loop(0, 8, drain, 0)
    for zp in range(2):
        for ct in range(2):
            @pl.when(jnp.logical_not(to_self(ct)))
            def _():
                x_copy(zp, ct).wait_send()


def products(hidden, w_turned):
    any_spec = pl.BlockSpec(memory_space=pl.ANY)
    dma = pltpu.SemaphoreType.DMA
    return pl.pallas_call(
        kernel,
        name="products",
        out_shape=jax.ShapeDtypeStruct((TOK, OUT), F32),
        in_specs=[any_spec, any_spec],
        out_specs=pl.BlockSpec(memory_space=pltpu.VMEM),
        scratch_shapes=[
            pltpu.VMEM((2, 2 * TOK, HID), BF),
            pltpu.VMEM((8, COLS, HID), BF),
            pltpu.VMEM((8, 2, COLS, 2 * TOK), BF),
            pltpu.VMEM((4, 2, 2, COLS, 2 * TOK), BF),
            pltpu.VMEM((2, 2 * TOK, 288), BF),
            pltpu.VMEM((2, 2, TOK, 288), BF),
            dma((2,)), dma((2, 4, 2)), dma((8, 2)), dma((3,)), dma((3,)),
            dma((8, 2)), dma((4, 2, 2)), dma((2, 2)), dma((2, 2)),
        ],
        compiler_params=pltpu.CompilerParams(
            collective_id=0, has_side_effects=True, vmem_limit_bytes=48 * 1024 * 1024
        ),
    )(hidden, w_turned)


def copy_for_each(array, axis):
    copies = jnp.broadcast_to(array, (lax.axis_size(axis), *array.shape))
    return lax.all_to_all(copies, axis, split_axis=0, concat_axis=0, tiled=True)


def taken_together(array, axis):
    return copy_for_each(array, axis).sum(axis=0)


def packed_total(arrays, axis):
    ends = [0]
    for a in arrays:
        ends.append(ends[-1] + a.size)
    so_far = taken_together(jnp.concatenate([a.ravel() for a in arrays]), axis)
    return tuple((so_far[b:e].reshape(a.shape) for a, b, e in zip(arrays, ends, ends[1:])))


def joined_along(pieces, dim):
    lengths = list(pieces.shape[1:])
    lengths[dim] *= pieces.shape[0]
    return jnp.moveaxis(pieces, 0, dim).reshape(lengths)


def collect(array, axis, dim):
    return joined_along(copy_for_each(array, axis), dim)


def rows_first(arrays, axis, dims):
    turned = [jnp.moveaxis(a, dim, 0) for a, dim in zip(arrays, dims)]
    both = jnp.concatenate([t.reshape(len(t), -1) for t in turned], axis=1)
    result, at, done = (lax.all_gather(both, axis, axis=0, tiled=True), 0, [])
    for t, dim in zip(turned, dims):
        piece = result[:, at : at + t[0].size].reshape(-1, *t.shape[1:])
        done.append(jnp.moveaxis(piece, 0, dim))
        at += t[0].size
    return tuple(done)


def in_blocks(array, dim, length):
    lengths = array.shape
    pieces = array.reshape(*lengths[:dim], length, lengths[dim] // length, *lengths[dim + 1 :])
    return jnp.moveaxis(pieces, dim, 0)


def sum_at_owner(array, axis, dim):
    length = lax.axis_size(axis)
    pieces = lax.all_to_all(in_blocks(array, dim, length), axis, 0, 0, tiled=True)
    return jnp.sum(pieces.astype(jnp.float32), axis=0)


def summed_on_arrival(array, axis, dim):
    pieces = in_blocks(array, dim, lax.axis_size(axis))
    arrived = lax.all_to_all(pieces, axis, split_axis=0, concat_axis=0, tiled=True)
    return arrived.sum(axis=0)


def body(hidden, fixed_down_weight, lowrank_factor_b, lowrank_factor_a, magnitude, cotangent):
    rank = lowrank_factor_b.shape[1]
    dp_count = lax.axis_size("dp")
    out_cols = magnitude.shape[0]
    own = lax.axis_index("tensor")
    lowrank_portion = jnp.dot(hidden, lowrank_factor_b, preferred_element_type=jnp.float32)
    combined_weight = fixed_down_weight.astype(jnp.float32) + jnp.dot(
        lowrank_factor_b, lowrank_factor_a, preferred_element_type=jnp.float32
    )
    local_sq = jnp.sum(combined_weight * combined_weight, axis=0)
    low_full, block_sq = packed_total((lowrank_portion, local_sq), "tensor")
    col_sq = collect(block_sq, "dp", 0)
    full_a = lax.all_gather(lowrank_factor_a, "dp", axis=1, tiled=True)
    column_norm_values = jnp.sqrt(col_sq + 1e-06)
    own_norms = lax.dynamic_slice_in_dim(column_norm_values, own * out_cols, out_cols, 0)
    scale = magnitude / own_norms
    lowrank_block_update = low_full.astype(jnp.bfloat16)
    summed = products(hidden, fixed_down_weight.T)
    own_a = lax.dynamic_slice_in_dim(full_a, own * out_cols, out_cols, 1)
    prenorm_output = summed + jnp.dot(
        lowrank_block_update, own_a, preferred_element_type=jnp.float32
    )
    mixed = (prenorm_output * scale).astype(jnp.bfloat16)
    cot = cotangent.astype(jnp.float32)
    mag_part = jnp.sum(cot * prenorm_output, axis=0) / own_norms
    prenorm_gradient_b = (cot * scale).astype(jnp.bfloat16)
    factor_a_portion = jnp.dot(
        lowrank_block_update.T, prenorm_gradient_b, preferred_element_type=jnp.float32
    )
    back_part = jnp.dot(prenorm_gradient_b, own_a.T, preferred_element_type=jnp.float32)
    backward_factor_b = taken_together(back_part, "tensor").astype(jnp.bfloat16)
    b_part = jnp.dot(hidden.T, backward_factor_b, preferred_element_type=jnp.float32)
    piece_cols = out_cols // dp_count
    piece_rows = b_part.shape[0] // dp_count
    stacked = jnp.concatenate(
        [
            mag_part.reshape(dp_count, piece_cols),
            factor_a_portion.reshape(rank, dp_count, piece_cols)
            .transpose(1, 0, 2)
            .reshape(dp_count, rank * piece_cols),
            b_part.reshape(dp_count, piece_rows * rank),
        ],
        axis=1,
    )
    reduced = summed_on_arrival(stacked, "dp", 0)
    gradient_column_scale = reduced[0, :piece_cols]
    gradient_factor_a = reduced[0, piece_cols : piece_cols + rank * piece_cols].reshape(
        rank, piece_cols
    )
    gradient_factor_b = reduced[0, piece_cols + rank * piece_cols :].reshape(piece_rows, rank)
    return (mixed, gradient_column_scale, gradient_factor_a, gradient_factor_b)


def solution(mesh):
    return jax.shard_map(
        body,
        mesh=mesh,
        in_specs=(
            P("dp", "tensor"),
            P("tensor", "dp"),
            P("tensor", None),
            P(None, "dp"),
            P("tensor"),
            P("dp", "tensor"),
        ),
        out_specs=(
            P("dp", "tensor"),
            P(("tensor", "dp")),
            P(None, ("tensor", "dp")),
            P(("tensor", "dp"), None),
        ),
        check_vma=False,
    )
```

```python
import functools

import jax
import jax.numpy as jnp
from jax import lax
from jax.experimental import pallas as pl
from jax.experimental.pallas import tpu as pltpu
from jax.sharding import PartitionSpec as P

TOK, HID, COLS, OUT = 320, 2304, 144, 576
MESH = pl.DeviceIdType.MESH
F32, BF = jnp.float32, jnp.bfloat16
CHUNKS = ((0, 80), (80, 64))


def remote(src, dst, send, recv, dp, tensor):
    return pltpu.make_async_remote_copy(
        src_ref=src, dst_ref=dst, send_sem=send, recv_sem=recv,
        device_id=(dp, tensor), device_id_type=MESH,
    )


def kernel(h_ref, w_ref, b_ref, a_ref, mag_ref, cot_ref, mixed_ref, grads_ref, gmag_ref,
           toks, wts, outgoing, arrived, turned, halves,
           sq_out, sq_in, msg_f, msg, msgs, a_all, sq_all, low_in, back_in, low_out, back_out, dpre, extra,
           spread, spread_in, plane, plane_in, mag_out, mag_in,
           loc_sem, w_send, w_recv, t_send, t_recv, y_send, y_recv, x_send, x_recv,
           s_send, s_recv, m_send, m_recv, l_send, l_recv, b_send, b_recv, d_send, d_recv, p_send, p_recv,
           g_send, g_recv):
    dp, tensor = lax.axis_index("dp"), lax.axis_index("tensor")
    x_hi, z, core = dp // 16, (dp // 2) % 8, dp % 2
    x_lo, y = tensor // 4, tensor % 4
    other = 1 - core

    def dp_of(a, b, c):
        return a * 16 + b * 2 + c

    load_h = pltpu.make_async_copy(h_ref, toks.at[0, pl.ds(core * TOK, TOK)], loc_sem.at[0])
    load_w = pltpu.make_async_copy(w_ref, wts.at[0], loc_sem.at[1])
    load_h.start()
    load_w.start()

    barrier = pltpu.get_barrier_semaphore()

    def greet(p):
        pl.semaphore_signal(barrier, inc=1, device_id=p, device_id_type=MESH)

    near = []
    for k in range(1, 4):
        near.append((dp_of(x_hi, z, core), x_lo * 4 + (y + k) % 4))
        near.append((dp_of(x_hi, z, other), x_lo * 4 + (y + k) % 4))
    for k in range(4):
        near.append((dp, (1 - x_lo) * 4 + (y + k) % 4))
    near.append((dp_of(x_hi, z, other), (1 - x_lo) * 4 + y))
    for c in range(2):
        near.append((dp_of(1 - x_hi, z, c), (1 - x_lo) * 4 + y))
    for p in near:
        greet(p)

    def greet_dp(i, carry):
        greet(((dp + i) % 32, tensor))
        return carry
    lax.fori_loop(1, 32, greet_dp, 0)

    mine = pl.ds(pl.multiple_of(core * TOK, TOK), TOK)
    owner = dp // 4
    load_w.wait()
    merged = wts[0].astype(F32) + lax.dot_general(
        a_ref[...], b_ref[...], (((0,), (0,)), ((), ())), preferred_element_type=F32)
    squares = merged * merged
    lanes = squares[:, 0:128]
    for i in range(1, 18):
        lanes = lanes + squares[:, 128 * i:128 * (i + 1)]
    own_sq = jnp.sum(lanes.T, axis=0, keepdims=True)
    sq_row = jnp.broadcast_to(own_sq, (8, COLS))

    @pl.when(owner == tensor)
    def _():
        sq_in[tensor] = sq_row

    @pl.when(owner != tensor)
    def _():
        sq_out[...] = sq_row

    load_h.wait()
    low_part = lax.dot_general(b_ref[...], toks[0, mine], (((1,), (1,)), ((), ())), preferred_element_type=F32)
    low_out[...] = low_part
    low_in[tensor] = low_part
    spread[...] = jnp.zeros_like(spread)
    msg_f[...] = jnp.zeros_like(msg_f)

    pl.semaphore_wait(barrier, len(near) + 31)

    def w_copy(side, k, ch):
        at, n = CHUNKS[ch]
        src = 0 if k == 1 else 2 * (k - 1) - 1 + side
        dst = 7 if k == 4 else 2 * k - 1 + side
        to = (z + 1) % 8 if side == 0 else (z + 7) % 8
        return remote(wts.at[src, pl.ds(at, n)], wts.at[dst, pl.ds(at, n)],
                      w_send.at[side, k - 1, ch], w_recv.at[dst, ch], dp_of(x_hi, to, core), tensor)

    w_copy(0, 1, 0).start()
    w_copy(1, 1, 1).start()
    w_copy(0, 1, 1).start()
    w_copy(1, 1, 0).start()
    own_tok = toks.at[0, mine]
    to_other = remote(own_tok, toks.at[0, mine], t_send.at[0], t_recv.at[0], dp_of(x_hi, z, other), tensor)
    to_far = remote(own_tok, toks.at[1, mine], t_send.at[1], t_recv.at[1], dp_of(1 - x_hi, z, core), tensor)
    relay = remote(toks.at[1, mine], toks.at[1, mine], t_send.at[2], t_recv.at[2], dp_of(x_hi, z, other), tensor)
    sq_copy = remote(sq_out, sq_in.at[tensor], s_send.at[0], s_recv.at[tensor], dp, owner)

    @pl.when(owner != tensor)
    def _():
        sq_copy.start()
    to_other.start()
    to_far.start()

    def over_tensor(src, dst, send, recv, act):
        def body(i, carry):
            to = (tensor + i) % 8
            if act == "recv":
                remote(src, dst.at[to], send.at[i], recv.at[to], dp, to).wait_recv()
            elif act == "start":
                remote(src, dst.at[tensor], send.at[i], recv.at[tensor], dp, to).start()
            else:
                remote(src, dst.at[tensor], send.at[i], recv.at[tensor], dp, to).wait_send()
            return carry
        lax.fori_loop(1, 8, body, 0)

    over_tensor(low_out, low_in, l_send, l_recv, "start")

    def zsrc_of(j):
        k = (j + 1) // 2
        return (z + 8 + k - 2 * k * (j % 2)) % 8

    def y_copy(j, g):
        zs = zsrc_of(j)
        return remote(outgoing.at[j, g], arrived.at[y, zs % 2, core], y_send.at[j, g],
                      y_recv.at[y, zs % 2, core], dp_of(x_hi, z, g), x_lo * 4 + zs // 2)

    def local(j, g):
        return jnp.logical_and(zsrc_of(j) // 2 == y, core == g)

    def item(j, g):
        p = lax.dot_general(toks[g], wts[j], (((1,), (1,)), ((), ())), preferred_element_type=F32)
        p = p.T.astype(BF)
        here = local(j, g)

        @pl.when(here)
        def _():
            arrived[y, zsrc_of(j) % 2, core] = p

        @pl.when(jnp.logical_not(here))
        def _():
            outgoing[j, g] = p
            y_copy(j, g).start()

    def items(lo, hi, g):
        def body(j, carry):
            item(j, g)
            return carry
        lax.fori_loop(lo, hi, body, 0)

    def msg_copy(i):
        return remote(msg, msgs.at[dp % 4], m_send.at[i], m_recv.at[dp % 4], (dp + i) % 32, tensor)

    def publish():
        def arrive(i, carry):
            frm = (tensor + i) % 8
            remote(sq_out, sq_in.at[frm], s_send.at[0], s_recv.at[frm], dp, frm).wait_recv()
            return carry
        lax.fori_loop(1, 8, arrive, 0)
        total = sq_in[0]
        for i in range(1, 8):
            total = total + sq_in[i]
        total = total[0:1]
        high = total.astype(BF).astype(F32)
        rest = total - high
        msg_f[:, 0:COLS] = a_ref[...].astype(F32)
        for i in range(3):
            msg_f[i:i + 1, 144:192] = high[:, 48 * i:48 * (i + 1)]
            msg_f[3 + i:4 + i, 144:192] = rest[:, 48 * i:48 * (i + 1)]
        packed = msg_f[...].astype(BF)
        msg[...] = packed
        msgs[dp % 4] = packed

        def send(i, carry):
            msg_copy(i).start()
            return carry
        lax.fori_loop(1, 32, send, 0)

    def receive():
        for j in range(4):
            @pl.when(dp != tensor * 4 + j)
            def _():
                remote(msg, msgs.at[j], m_send.at[0], m_recv.at[j], dp, tensor).wait_recv()
        for j in range(4):
            m = msgs[j].astype(F32)
            a_all[:, COLS * j:COLS * (j + 1)] = m[:, 0:COLS]
            for i in range(3):
                at = COLS * j + 48 * i
                sq_all[:, at:at + 48] = m[i:i + 1, 144:192] + m[3 + i:4 + i, 144:192]

    def norms():
        return jnp.sqrt(sq_all[...] + 1e-6)

    def backward():
        scale = mag_ref[...] / norms()
        d = (cot_ref[...].astype(F32) * scale).astype(BF)
        dpre[...] = d
        back = lax.dot_general(a_all[...].astype(BF), d, (((1,), (1,)), ((), ())), preferred_element_type=F32)
        back_out[...] = back
        back_in[tensor] = back
        over_tensor(back_out, back_in, b_send, b_recv, "start")

    group = x_hi * 2 + core

    def spread_copy(i):
        to = (group + i) % 4
        return remote(spread.at[to], spread_in.at[group], d_send.at[i], d_recv.at[group],
                      dp_of(to // 2, z, to % 2), tensor)

    def gradients():
        over_tensor(low_out, low_in, l_send, l_recv, "recv")
        over_tensor(back_out, back_in, b_send, b_recv, "recv")
        low, back = low_in[0], back_in[0]
        for i in range(1, 8):
            low = low + low_in[i]
            back = back + back_in[i]
        low, back = low.astype(BF), back.astype(BF)
        grad_b = jnp.dot(back, toks[0, mine], preferred_element_type=F32)
        grad_a = jnp.dot(low, dpre[...], preferred_element_type=F32)
        for x in range(2):
            for zz in range(8):
                for c in range(2):
                    i = x * 16 + zz * 2 + c
                    spread[x * 2 + c, zz, :, 0:72] = grad_b[:, 72 * i:72 * (i + 1)]
                    spread[x * 2 + c, zz, :, 72:90] = grad_a[:, 18 * i:18 * (i + 1)]
        for i in range(1, 4):
            spread_copy(i).start()
        extra[...] = lax.dot_general(low, a_all[...].astype(BF), (((0,), (0,)), ((), ())),
                                     preferred_element_type=F32)

    def plane_copy(i):
        to = (z + i) % 8
        return remote(plane.at[to], plane_in.at[z], p_send.at[i], p_recv.at[z], dp_of(x_hi, to, core), tensor)

    def sum_plane():
        total = spread[group]
        for i in range(1, 4):
            frm = (group + i) % 4
            remote(spread.at[0], spread_in.at[frm], d_send.at[0], d_recv.at[frm], dp, tensor).wait_recv()
            total = total + spread_in[frm]
        plane[...] = total

        def send(i, carry):
            plane_copy(i).start()
            return carry
        lax.fori_loop(1, 8, send, 0)

    def sum_planes():
        total = plane[z]
        for i in range(1, 8):
            frm = (z + i) % 8
            remote(plane.at[0], plane_in.at[frm], p_send.at[0], p_recv.at[frm], dp, tensor).wait_recv()
            total = total + plane_in[frm]
        grads_ref[...] = total

    def ring(k, first):
        for side in (0, 1):
            ch = first if side == 0 else 1 - first
            w_copy(side, k, ch).wait_recv()
            if k < 3 or first == 0:
                w_copy(side, k + 1, ch).start()

    to_other.wait_recv()
    items(0, 1, 0)
    pl.when(owner == tensor)(publish)
    ring(1, 0)
    receive()
    backward()
    ring(1, 1)
    items(1, 3, 0)
    gradients()
    ring(2, 0)
    sum_plane()
    ring(2, 1)
    items(3, 5, 0)
    to_far.wait_recv()
    relay.start()
    relay.wait_recv()
    items(0, 5, 1)
    ring(3, 0)
    sum_planes()
    ring(3, 1)
    items(5, 7, 0)
    items(5, 7, 1)
    w_copy(0, 4, 0).wait_recv()
    w_copy(1, 4, 1).wait_recv()
    items(7, 8, 0)
    items(7, 8, 1)

    tok_hi = jnp.where(core == 0, x_hi, 1 - x_hi)

    def x_copy(zp, ct):
        return remote(turned.at[zp, pl.ds(ct * TOK, TOK)], halves.at[x_lo, zp], x_send.at[zp, ct],
                      x_recv.at[x_lo, zp], dp_of(tok_hi, z, ct), x_hi * 4 + y)

    def to_self(ct):
        return jnp.logical_and(jnp.logical_and(tok_hi == x_hi, x_lo == x_hi), core == ct)

    for zp in range(2):
        parts = []
        for cs in range(2):
            for k in range(4):
                ys = (y + k) % 4
                away = jnp.logical_or(k > 0, core != cs)

                def arrive(ys=ys, cs=cs):
                    remote(outgoing.at[0, 0], arrived.at[ys, zp, cs], y_send.at[0, 0], y_recv.at[ys, zp, cs],
                           dp, tensor).wait_recv()
                if k == 0:
                    pl.when(core != cs)(arrive)
                else:
                    arrive()
            total = arrived[0, zp, cs].astype(F32)
            for ys in range(1, 4):
                total = total + arrived[ys, zp, cs].astype(F32)
            parts.append(total)
        both = jnp.concatenate(parts, axis=0).T.astype(BF)
        turned[zp] = both
        for ct in range(2):
            @pl.when(to_self(ct))
            def _():
                halves[x_lo, zp] = both[ct * TOK:(ct + 1) * TOK]

            @pl.when(jnp.logical_not(to_self(ct)))
            def _():
                x_copy(zp, ct).start()

    for zp in range(2):
        for xl in range(2):
            sx_hi = x_lo
            score = jnp.where(sx_hi == x_hi, 0, 1)
            own = jnp.logical_and(jnp.logical_and(sx_hi == x_hi, xl == x_lo), score == core)

            @pl.when(jnp.logical_not(own))
            def _():
                remote(turned.at[0, pl.ds(0, TOK)], halves.at[xl, zp], x_send.at[0, 0], x_recv.at[xl, zp],
                       dp, tensor).wait_recv()
        cols = slice(zp * 288, (zp + 1) * 288)
        extra[:, cols] = extra[:, cols] + (halves[0, zp].astype(F32) + halves[1, zp].astype(F32))
    pre = extra[...]
    norm = norms()
    mag_row = jnp.sum(cot_ref[...].astype(F32) * pre, axis=0, keepdims=True) / norm
    for i in range(32):
        mag_out[i, :, 0:18] = mag_row[:, 18 * i:18 * (i + 1)]

    def mag_copy(i):
        to = (dp + i) % 32
        return remote(mag_out.at[to], mag_in.at[dp], g_send.at[i], g_recv.at[dp], to, tensor)

    def mag_start(i, carry):
        mag_copy(i).start()
        return carry
    lax.fori_loop(1, 32, mag_start, 0)
    mixed_ref[...] = (pre * (mag_ref[...] / norm)).astype(BF)

    for k in (1, 2, 3, 4):
        for side in (0, 1):
            for ch in (0, 1):
                if k < 4 or ch == side:
                    w_copy(side, k, ch).wait_send()
    @pl.when(owner != tensor)
    def _():
        sq_copy.wait_send()

    @pl.when(owner == tensor)
    def _():
        def sent(i, carry):
            msg_copy(i).wait_send()
            return carry
        lax.fori_loop(1, 32, sent, 0)
    over_tensor(low_out, low_in, l_send, l_recv, "send")
    over_tensor(back_out, back_in, b_send, b_recv, "send")
    for i in range(1, 4):
        spread_copy(i).wait_send()

    def plane_sent(i, carry):
        plane_copy(i).wait_send()
        return carry
    lax.fori_loop(1, 8, plane_sent, 0)
    to_other.wait_send()
    to_far.wait_send()
    relay.wait_send()
    def drain(j, carry):
        for g in range(2):
            @pl.when(jnp.logical_not(local(j, g)))
            def _():
                y_copy(j, g).wait_send()
        return carry
    lax.fori_loop(0, 8, drain, 0)
    for zp in range(2):
        for ct in range(2):
            @pl.when(jnp.logical_not(to_self(ct)))
            def _():
                x_copy(zp, ct).wait_send()

    def mag_arrive(i, total):
        frm = (dp + i) % 32
        remote(mag_out.at[0], mag_in.at[frm], g_send.at[0], g_recv.at[frm], dp, tensor).wait_recv()
        return total + mag_in[frm]
    gmag_ref[...] = lax.fori_loop(1, 32, mag_arrive, mag_out[dp])

    def mag_sent(i, carry):
        mag_copy(i).wait_send()
        return carry
    lax.fori_loop(1, 32, mag_sent, 0)


def body(hidden, weight, factor_b, factor_a, magnitude, cotangent):
    any_spec, vmem_spec = pl.BlockSpec(memory_space=pl.ANY), pl.BlockSpec(memory_space=pltpu.VMEM)
    dma, vmem = pltpu.SemaphoreType.DMA, pltpu.VMEM
    mixed, grads, gmag = pl.pallas_call(
        kernel,
        name="dora",
        out_shape=(jax.ShapeDtypeStruct((TOK, OUT), BF), jax.ShapeDtypeStruct((16, 128), F32),
                   jax.ShapeDtypeStruct((1, 128), F32)),
        in_specs=[any_spec, any_spec] + [vmem_spec] * 4,
        out_specs=(vmem_spec,) * 3,
        scratch_shapes=[
            vmem((2, 2 * TOK, HID), BF),
            vmem((8, COLS, HID), BF),
            vmem((8, 2, COLS, 2 * TOK), BF),
            vmem((4, 2, 2, COLS, 2 * TOK), BF),
            vmem((2, 2 * TOK, 288), BF),
            vmem((2, 2, TOK, 288), BF),
            vmem((8, COLS), F32), vmem((8, 8, COLS), F32),
            vmem((16, 256), F32), vmem((16, 256), BF), vmem((4, 16, 256), BF),
            vmem((16, OUT), F32), vmem((1, OUT), F32),
            vmem((8, 16, TOK), F32), vmem((8, 16, TOK), F32), vmem((16, TOK), F32), vmem((16, TOK), F32),
            vmem((TOK, OUT), BF), vmem((TOK, OUT), F32),
            vmem((4, 8, 16, 128), F32), vmem((4, 8, 16, 128), F32),
            vmem((8, 16, 128), F32), vmem((8, 16, 128), F32),
            vmem((32, 1, 128), F32), vmem((32, 1, 128), F32),
            dma((2,)), dma((2, 4, 2)), dma((8, 2)), dma((3,)), dma((3,)),
            dma((8, 2)), dma((4, 2, 2)), dma((2, 2)), dma((2, 2)),
            dma((1,)), dma((8,)), dma((32,)), dma((4,)), dma((8,)), dma((8,)), dma((8,)), dma((8,)),
            dma((4,)), dma((4,)), dma((8,)), dma((8,)), dma((32,)), dma((32,)),
        ],
        compiler_params=pltpu.CompilerParams(
            collective_id=0, has_side_effects=True, vmem_limit_bytes=48 * 1024 * 1024
        ),
    )(hidden, weight.T, factor_b.T, factor_a, magnitude.reshape(1, OUT), cotangent)
    return mixed, gmag[0, :18], grads[:, 72:90], grads[:, :72].T


def solution(mesh):
    return jax.shard_map(
        body,
        mesh=mesh,
        in_specs=(
            P("dp", "tensor"),
            P("tensor", "dp"),
            P("tensor", None),
            P(None, "dp"),
            P("tensor"),
            P("dp", "tensor"),
        ),
        out_specs=(
            P("dp", "tensor"),
            P(("tensor", "dp")),
            P(None, ("tensor", "dp")),
            P(("tensor", "dp"), None),
        ),
        check_vma=False,
    )
```

```python
import functools

import jax
import jax.numpy as jnp
from jax import lax
from jax.experimental import pallas as pl
from jax.experimental.pallas import tpu as pltpu
from jax.sharding import PartitionSpec as P

TOK, HID, COLS, OUT, HALF = 320, 2304, 144, 576, 288
MESH = pl.DeviceIdType.MESH
F32, BF = jnp.float32, jnp.bfloat16
CHUNKS = ((0, 80), (80, 64))
FIRST, LAST = 192, 128
PARTS = ((0, 2 * FIRST), (2 * FIRST, 2 * LAST))


def remote(src, dst, send, recv, dp, tensor):
    return pltpu.make_async_remote_copy(
        src_ref=src, dst_ref=dst, send_sem=send, recv_sem=recv,
        device_id=(dp, tensor), device_id_type=MESH,
    )


def kernel(h_ref, w_ref, b_hbm, a_hbm, mag_hbm, cot_hbm, mixed_ref, grads_ref, gmag_ref,
           b_ref, a_ref, mag_ref, cot_ref, own, toks, wts, outgoing, arrived, turned, halves,
           sq_out, sq_in, msg_f, msg, msgs, a_all, sq_all, norms, scales, low_in, back_in, low_out, back_out,
           dpre, extra, cots,
           spread, spread_in, plane, plane_in, mag_out, mag_in, sums, results,
           loc_sem, w_send, w_recv, t_send, t_recv, y_send, y_recv, x_send, x_recv,
           s_send, s_recv, m_send, m_recv, l_send, l_recv, b_send, b_recv, d_send, d_recv, p_send, p_recv,
           g_send, g_recv):
    dp, tensor = lax.axis_index("dp"), lax.axis_index("tensor")
    x_hi, z, core = dp // 16, (dp // 2) % 8, dp % 2
    x_lo, y = tensor // 4, tensor % 4
    other = 1 - core

    def dp_of(a, b, c):
        return a * 16 + b * 2 + c

    def rows(part, of):
        if part == 0:
            return pl.ds(of * FIRST, FIRST), pl.ds(0, FIRST)
        return pl.ds(2 * FIRST + of * LAST, LAST), pl.ds(FIRST, LAST)

    load_h = pltpu.make_async_copy(h_ref, own, loc_sem.at[0])
    place = []
    for part in range(2):
        there, here = rows(part, core)
        place.append(pltpu.make_async_copy(h_ref.at[here], toks.at[0, there], loc_sem.at[6 + part]))
    load_w = pltpu.make_async_copy(w_ref, wts.at[0], loc_sem.at[1])
    loads = [pltpu.make_async_copy(src, dst, loc_sem.at[2 + i]) for i, (src, dst) in enumerate(
        ((a_hbm, a_ref), (b_hbm, b_ref), (mag_hbm, mag_ref), (cot_hbm, cot_ref)))]
    load_w.start()
    loads[0].start()
    loads[1].start()
    load_h.start()
    place[0].start()
    place[1].start()
    loads[2].start()
    loads[3].start()

    barrier = pltpu.get_barrier_semaphore()

    def greet(p):
        pl.semaphore_signal(barrier, inc=1, device_id=p, device_id_type=MESH)

    near = []
    for k in range(1, 4):
        near.append((dp_of(x_hi, z, core), x_lo * 4 + (y + k) % 4))
        near.append((dp_of(x_hi, z, other), x_lo * 4 + (y + k) % 4))
    for k in range(4):
        near.append((dp, (1 - x_lo) * 4 + (y + k) % 4))
    near.append((dp_of(x_hi, z, other), (1 - x_lo) * 4 + y))
    for c in range(2):
        near.append((dp_of(1 - x_hi, z, c), (1 - x_lo) * 4 + y))
    for p in near:
        greet(p)

    def greet_dp(i, carry):
        greet(((dp + i) % 32, tensor))
        return carry
    lax.fori_loop(1, 32, greet_dp, 0)

    owner = dp // 4
    load_w.wait()
    loads[0].wait()
    loads[1].wait()
    merged = wts[0].astype(F32) + lax.dot_general(
        a_ref[...], b_ref[...], (((0,), (0,)), ((), ())), preferred_element_type=F32)
    squares = merged * merged
    lanes = squares[:, 0:128]
    for i in range(1, 18):
        lanes = lanes + squares[:, 128 * i:128 * (i + 1)]
    own_sq = jnp.sum(lanes.T, axis=0, keepdims=True)
    sq_row = jnp.broadcast_to(own_sq, (8, COLS))

    @pl.when(owner == tensor)
    def _():
        sq_in[tensor] = sq_row

    @pl.when(owner != tensor)
    def _():
        sq_out[...] = sq_row

    load_h.wait()
    low_part = lax.dot_general(b_ref[...], own[...], (((1,), (1,)), ((), ())), preferred_element_type=F32)
    low_out[...] = low_part
    low_in[tensor] = low_part
    spread[...] = jnp.zeros_like(spread)
    msg_f[...] = jnp.zeros_like(msg_f)

    loads[2].wait()
    loads[3].wait()
    with jax.named_scope('barrier_wait'):
        pl.semaphore_wait(barrier, len(near) + 31)

    def w_copy(side, k, ch):
        at, n = CHUNKS[ch]
        src = 0 if k == 1 else 2 * (k - 1) - 1 + side
        dst = 7 if k == 4 else 2 * k - 1 + side
        to = (z + 1) % 8 if side == 0 else (z + 7) % 8
        return remote(wts.at[src, pl.ds(at, n)], wts.at[dst, pl.ds(at, n)],
                      w_send.at[side, k - 1, ch], w_recv.at[dst, ch], dp_of(x_hi, to, core), tensor)

    w_copy(0, 1, 0).start()
    w_copy(1, 1, 1).start()
    w_copy(0, 1, 1).start()
    w_copy(1, 1, 0).start()
    to_other, to_far, relay = [], [], []
    for part in range(2):
        there, here = rows(part, core)
        to_other.append(remote(own.at[here], toks.at[0, there], t_send.at[0, part], t_recv.at[0, part],
                               dp_of(x_hi, z, other), tensor))
        to_far.append(remote(own.at[here], toks.at[1, there], t_send.at[1, part], t_recv.at[1, part],
                             dp_of(1 - x_hi, z, core), tensor))
        relay.append(remote(toks.at[1, there], toks.at[1, there], t_send.at[2, part], t_recv.at[2, part],
                            dp_of(x_hi, z, other), tensor))

    sq_copy = remote(sq_out, sq_in.at[tensor], s_send.at[0], s_recv.at[tensor], dp, owner)

    @pl.when(owner != tensor)
    def _():
        sq_copy.start()

    def over_tensor(src, dst, send, recv, act):
        def body(i, carry):
            to = (tensor + i) % 8
            if act == "recv":
                remote(src, dst.at[to], send.at[i], recv.at[to], dp, to).wait_recv()
            elif act == "start":
                remote(src, dst.at[tensor], send.at[i], recv.at[tensor], dp, to).start()
            else:
                remote(src, dst.at[tensor], send.at[i], recv.at[tensor], dp, to).wait_send()
            return carry
        lax.fori_loop(1, 8, body, 0)

    to_other[0].start()
    to_other[1].start()
    over_tensor(low_out, low_in, l_send, l_recv, "start")
    to_far[0].start()
    to_far[1].start()

    def zsrc_of(j):
        k = (j + 1) // 2
        return (z + 8 + k - 2 * k * (j % 2)) % 8

    def summer(j, g):
        return (zsrc_of(j) + 2 * g + core) % 4

    def y_copy(j, g, part):
        lanes = pl.ds(*PARTS[part])
        return remote(outgoing.at[j, g, :, lanes], arrived.at[j, y, :, lanes], y_send.at[j, g, part],
                      y_recv.at[j, y, part], dp, x_lo * 4 + summer(j, g))

    def local(j, g):
        return summer(j, g) == y

    def item(j, g, parts=(0, 1)):
        lo, hi = PARTS[parts[0]][0], sum(PARTS[parts[-1]])
        p = lax.dot_general(toks[g, lo:hi], wts[j], (((1,), (1,)), ((), ())), preferred_element_type=F32)
        p = p.T.astype(BF)
        here = local(j, g)

        @pl.when(here)
        def _():
            arrived[j, y, :, lo:hi] = p

        @pl.when(jnp.logical_not(here))
        def _():
            outgoing[j, g, :, lo:hi] = p
            for part in parts:
                y_copy(j, g, part).start()

    def items(lo, hi, g, parts=(0, 1)):
        def body(j, carry):
            item(j, g, parts)
            return carry
        lax.fori_loop(lo, hi, body, 0)

    def items_both(lo, hi):
        def body(i, carry):
            item(lo + i // 2, i % 2)
            return carry
        lax.fori_loop(0, 2 * (hi - lo), body, 0)

    def msg_copy(i):
        return remote(msg, msgs.at[dp % 4], m_send.at[i], m_recv.at[dp % 4], (dp + i) % 32, tensor)

    def publish():
        def arrive(i, carry):
            frm = (tensor + i) % 8
            remote(sq_out, sq_in.at[frm], s_send.at[0], s_recv.at[frm], dp, frm).wait_recv()
            return carry
        lax.fori_loop(1, 8, arrive, 0)
        total = sq_in[0]
        for i in range(1, 8):
            total = total + sq_in[i]
        total = total[0:1]
        high = total.astype(BF).astype(F32)
        rest = total - high
        msg_f[:, 0:COLS] = a_ref[...].astype(F32)
        for i in range(3):
            msg_f[i:i + 1, 144:192] = high[:, 48 * i:48 * (i + 1)]
            msg_f[3 + i:4 + i, 144:192] = rest[:, 48 * i:48 * (i + 1)]
        packed = msg_f[...].astype(BF)
        msg[...] = packed
        msgs[dp % 4] = packed

        def send(i, carry):
            msg_copy(i).start()
            return carry
        lax.fori_loop(1, 32, send, 0)

    def receive():
        for j in range(4):
            @pl.when(dp != tensor * 4 + j)
            def _():
                remote(msg, msgs.at[j], m_send.at[0], m_recv.at[j], dp, tensor).wait_recv()
        for j in range(4):
            m = msgs[j].astype(F32)
            zp, at = j // 2, COLS * (j % 2)
            a_all[zp, :, at:at + COLS] = m[:, 0:COLS]
            for i in range(3):
                sq_all[zp, :, at + 48 * i:at + 48 * (i + 1)] = m[i:i + 1, 144:192] + m[3 + i:4 + i, 144:192]

    def backward():
        back = None
        mags = mag_ref[...].reshape(1, OUT)
        for zp in range(2):
            norm = jnp.sqrt(sq_all[zp] + 1e-6)
            scale = mags[:, HALF * zp:HALF * (zp + 1)] / norm
            norms[zp] = norm
            scales[zp] = scale
            cot = cot_ref[:, HALF * zp:HALF * (zp + 1)].astype(F32)
            cots[zp] = cot
            d = (cot * scale).astype(BF)
            dpre[zp] = d
            part = lax.dot_general(a_all[zp].astype(BF), d, (((1,), (1,)), ((), ())), preferred_element_type=F32)
            back = part if back is None else back + part
        back_out[...] = back
        back_in[tensor] = back
        over_tensor(back_out, back_in, b_send, b_recv, "start")

    group = x_hi * 2 + core

    def spread_copy(i):
        to = (group + i) % 4
        return remote(spread.at[to], spread_in.at[group], d_send.at[i], d_recv.at[group],
                      dp_of(to // 2, z, to % 2), tensor)

    def gradients():
        over_tensor(low_out, low_in, l_send, l_recv, "recv")
        over_tensor(back_out, back_in, b_send, b_recv, "recv")
        low, back = low_in[0], back_in[0]
        for i in range(1, 8):
            low = low + low_in[i]
            back = back + back_in[i]
        low, back = low.astype(BF), back.astype(BF)
        grad_b = jnp.dot(back, own[...], preferred_element_type=F32)
        grad_a = [jnp.dot(low, dpre[zp], preferred_element_type=F32) for zp in range(2)]
        for x in range(2):
            for zz in range(8):
                for c in range(2):
                    i = x * 16 + zz * 2 + c
                    spread[x * 2 + c, zz, :, 0:72] = grad_b[:, 72 * i:72 * (i + 1)]
                    spread[x * 2 + c, zz, :, 72:90] = grad_a[x][:, 18 * (i % 16):18 * (i % 16 + 1)]
        for i in range(1, 4):
            spread_copy(i).start()
        for zp in range(2):
            extra[zp] = lax.dot_general(low, a_all[zp].astype(BF), (((0,), (0,)), ((), ())),
                                        preferred_element_type=F32)

    def plane_copy(i):
        to = (z + i) % 8
        return remote(plane.at[to], plane_in.at[z], p_send.at[i], p_recv.at[z], dp_of(x_hi, to, core), tensor)

    def sum_plane():
        total = spread[group]
        for i in range(1, 4):
            frm = (group + i) % 4
            remote(spread.at[0], spread_in.at[frm], d_send.at[0], d_recv.at[frm], dp, tensor).wait_recv()
            total = total + spread_in[frm]
        plane[...] = total

        def send(i, carry):
            plane_copy(i).start()
            return carry
        lax.fori_loop(1, 8, send, 0)

    def sum_planes():
        total = plane[z]
        for i in range(1, 8):
            frm = (z + i) % 8
            remote(plane.at[0], plane_in.at[frm], p_send.at[0], p_recv.at[frm], dp, tensor).wait_recv()
            total = total + plane_in[frm]
        grads_ref[...] = total

    def ring(k, first):
        for side in (0, 1):
            ch = first if side == 0 else 1 - first
            w_copy(side, k, ch).wait_recv()
            if k < 3 or first == 0:
                w_copy(side, k + 1, ch).start()

    def x_copy(j, g, ct):
        zs = zsrc_of(j)
        tok_hi = jnp.where(g == 0, x_hi, 1 - x_hi)
        return remote(turned.at[j, ct], halves.at[x_lo, zs % 2, core], x_send.at[j, ct],
                      x_recv.at[x_lo, zs % 2, core], dp_of(tok_hi, z, ct), x_hi * 4 + zs // 2)

    def to_self(j, g, ct):
        same = jnp.logical_and(g == 0, x_lo == x_hi)
        return jnp.logical_and(same, jnp.logical_and(zsrc_of(j) // 2 == y, core == ct))

    def active(j, g):
        return summer(j, g) == y

    def stage_two(j, g):
        for k in range(1, 4):
            ys = (y + k) % 4
            for part in range(2):
                lanes = pl.ds(*PARTS[part])
                remote(outgoing.at[0, 0, :, lanes], arrived.at[j, ys, :, lanes], y_send.at[0, 0, part],
                       y_recv.at[j, ys, part], dp, tensor).wait_recv()
        total = arrived[j, 0].astype(F32)
        for ys in range(1, 4):
            total = total + arrived[j, ys].astype(F32)
        total = total.astype(BF)
        for ct in range(2):
            part = jnp.concatenate(
                [total[:, ct * FIRST:(ct + 1) * FIRST],
                 total[:, 2 * FIRST + ct * LAST:2 * FIRST + (ct + 1) * LAST]], axis=1)
            mine_too = to_self(j, g, ct)

            @pl.when(mine_too)
            def _():
                halves[x_lo, zsrc_of(j) % 2, core] = part

            @pl.when(jnp.logical_not(mine_too))
            def _():
                turned[j, ct] = part
                x_copy(j, g, ct).start()

    def second(lo, hi, g):
        def unit(j, carry):
            pl.when(active(j, g))(lambda: stage_two(j, g))
            return carry
        lax.fori_loop(lo, hi, unit, 0)

    def steps_of(zp):
        away = (2 * y + zp - z + 8) % 8
        return jnp.where(away > 4, 8 - away, away)

    with jax.named_scope("a0"):
        for part in range(2):
            place[part].wait()
            to_other[part].wait_recv()
    items(0, 1, 0)
    with jax.named_scope("a1_publish"):
        pl.when(owner == tensor)(publish)
    with jax.named_scope("a2_ring10"):
        ring(1, 0)
    with jax.named_scope("a3_ring11"):
        ring(1, 1)
    items(1, 3, 0)
    with jax.named_scope("a4_far0"):
        to_far[0].wait_recv()
    relay[0].start()
    with jax.named_scope("a5_ring20"):
        ring(2, 0)
    with jax.named_scope("a6_relay0"):
        relay[0].wait_recv()
    items(0, 3, 1, (0,))
    with jax.named_scope("a7_receive"):
        receive()
    backward()
    with jax.named_scope("a8_ring21"):
        ring(2, 1)
    items(3, 5, 0)
    items(3, 5, 1, (0,))
    with jax.named_scope("a9_far1"):
        to_far[1].wait_recv()
    relay[1].start()
    second(0, 3, 0)
    with jax.named_scope("aa_relay1"):
        relay[1].wait_recv()
    items(0, 5, 1, (1,))
    with jax.named_scope("ab_ring30"):
        ring(3, 0)
    with jax.named_scope("b0_grads"):
        gradients()
    with jax.named_scope("b1_ring31"):
        ring(3, 1)
    with jax.named_scope("b2_items"):
        items_both(5, 7)
    with jax.named_scope("b3_plane"):
        sum_plane()
    with jax.named_scope("b4_second"):
        second(3, 5, 0)
    with jax.named_scope("b5_last"):
        w_copy(0, 4, 0).wait_recv()
        w_copy(1, 4, 1).wait_recv()
    with jax.named_scope("b6_items"):
        items_both(7, 8)
    with jax.named_scope("b8_second"):
        second(0, 5, 1)
    with jax.named_scope("b9_second"):
        second(5, 7, 0)
        second(5, 7, 1)
    with jax.named_scope("ba_second"):
        second(7, 8, 0)
        second(7, 8, 1)

    def finish(i, carry):
        zp = jnp.where(steps_of(0) <= steps_of(1), i, 1 - i)
        parts = []
        for cs in range(2):
            for xl in range(2):
                far = jnp.where(x_lo == x_hi, 0, 1)
                frm = (2 * y + zp + 2 * far + cs) % 4
                own = jnp.logical_and(jnp.logical_and(x_lo == x_hi, xl == x_lo),
                                      jnp.logical_and(frm == y, core == cs))

                @pl.when(jnp.logical_not(own))
                def _():
                    remote(turned.at[0, 0], halves.at[xl, zp, cs], x_send.at[0, 0], x_recv.at[xl, zp, cs],
                           dp, tensor).wait_recv()
            parts.append(halves[0, zp, cs].astype(F32) + halves[1, zp, cs].astype(F32))
        pre = extra[zp] + jnp.concatenate(parts, axis=0).T
        sums[zp] = jnp.sum(cots[zp] * pre, axis=0, keepdims=True) / norms[zp]
        results[zp] = pre * scales[zp]
        return carry
    with jax.named_scope("c0_finish"):
        lax.fori_loop(0, 2, finish, 0)
    for i in range(32):
        mag_out[i, :, 0:18] = sums[i // 16][:, 18 * (i % 16):18 * (i % 16 + 1)]

    def mag_copy(i):
        to = (dp + i) % 32
        return remote(mag_out.at[to], mag_in.at[dp], g_send.at[i], g_recv.at[dp], to, tensor)

    def mag_start(i, carry):
        mag_copy(i).start()
        return carry
    with jax.named_scope("c1_mag"):
        lax.fori_loop(1, 32, mag_start, 0)
    with jax.named_scope("b7_planes"):
        sum_planes()
    with jax.named_scope("c2_mixed"):
        for zp in range(2):
            mixed_ref[:, HALF * zp:HALF * (zp + 1)] = results[zp].astype(BF)

    for k in (1, 2, 3, 4):
        for side in (0, 1):
            for ch in (0, 1):
                if k < 4 or ch == side:
                    w_copy(side, k, ch).wait_send()
    @pl.when(owner != tensor)
    def _():
        sq_copy.wait_send()

    @pl.when(owner == tensor)
    def _():
        def sent(i, carry):
            msg_copy(i).wait_send()
            return carry
        lax.fori_loop(1, 32, sent, 0)
    over_tensor(low_out, low_in, l_send, l_recv, "send")
    over_tensor(back_out, back_in, b_send, b_recv, "send")
    for i in range(1, 4):
        spread_copy(i).wait_send()

    def plane_sent(i, carry):
        plane_copy(i).wait_send()
        return carry
    lax.fori_loop(1, 8, plane_sent, 0)
    for copies in (to_other, to_far, relay):
        for part in range(2):
            copies[part].wait_send()
    def drain(j, carry):
        for g in range(2):
            @pl.when(jnp.logical_not(local(j, g)))
            def _():
                for part in range(2):
                    y_copy(j, g, part).wait_send()
        return carry
    lax.fori_loop(0, 8, drain, 0)

    def drain_two(j, carry):
        for g in range(2):
            for ct in range(2):
                @pl.when(jnp.logical_and(active(j, g), jnp.logical_not(to_self(j, g, ct))))
                def _():
                    x_copy(j, g, ct).wait_send()
        return carry
    lax.fori_loop(0, 8, drain_two, 0)

    def mag_arrive(i, total):
        frm = (dp + i) % 32
        remote(mag_out.at[0], mag_in.at[frm], g_send.at[0], g_recv.at[frm], dp, tensor).wait_recv()
        return total + mag_in[frm]
    with jax.named_scope("c3_gmag"):
        gmag_ref[...] = lax.fori_loop(1, 32, mag_arrive, mag_out[dp])

    def mag_sent(i, carry):
        mag_copy(i).wait_send()
        return carry
    lax.fori_loop(1, 32, mag_sent, 0)


def body(hidden, weight, factor_b, factor_a, magnitude, cotangent):
    any_spec, vmem_spec = pl.BlockSpec(memory_space=pl.ANY), pl.BlockSpec(memory_space=pltpu.VMEM)
    dma, vmem = pltpu.SemaphoreType.DMA, pltpu.VMEM
    mixed, grads, gmag = pl.pallas_call(
        kernel,
        name="dora",
        out_shape=(jax.ShapeDtypeStruct((TOK, OUT), BF), jax.ShapeDtypeStruct((16, 128), F32),
                   jax.ShapeDtypeStruct((1, 128), F32)),
        in_specs=[any_spec] * 6,
        out_specs=(vmem_spec,) * 3,
        scratch_shapes=[
            vmem((16, HID), BF), vmem((16, COLS), BF), vmem((OUT,), F32), vmem((TOK, OUT), BF), vmem((TOK, HID), BF),
            vmem((2, 2 * TOK, HID), BF),
            vmem((8, COLS, HID), BF),
            vmem((8, 2, COLS, 2 * TOK), BF),
            vmem((8, 4, COLS, 2 * TOK), BF),
            vmem((8, 2, COLS, TOK), BF),
            vmem((2, 2, 2, COLS, TOK), BF),
            vmem((8, COLS), F32), vmem((8, 8, COLS), F32),
            vmem((16, 256), F32), vmem((16, 256), BF), vmem((4, 16, 256), BF),
            vmem((2, 16, HALF), F32), vmem((2, 1, HALF), F32), vmem((2, 1, HALF), F32), vmem((2, 1, HALF), F32),
            vmem((8, 16, TOK), F32), vmem((8, 16, TOK), F32), vmem((16, TOK), F32), vmem((16, TOK), F32),
            vmem((2, TOK, HALF), BF), vmem((2, TOK, HALF), F32), vmem((2, TOK, HALF), F32),
            vmem((4, 8, 16, 128), F32), vmem((4, 8, 16, 128), F32),
            vmem((8, 16, 128), F32), vmem((8, 16, 128), F32),
            vmem((32, 1, 128), F32), vmem((32, 1, 128), F32), vmem((2, 1, HALF), F32), vmem((2, TOK, HALF), F32),
            dma((8,)), dma((2, 4, 2)), dma((8, 2)), dma((3, 2)), dma((3, 2)),
            dma((8, 2, 2)), dma((8, 4, 2)), dma((8, 2)), dma((2, 2, 2)),
            dma((1,)), dma((8,)), dma((32,)), dma((4,)), dma((8,)), dma((8,)), dma((8,)), dma((8,)),
            dma((4,)), dma((4,)), dma((8,)), dma((8,)), dma((32,)), dma((32,)),
        ],
        compiler_params=pltpu.CompilerParams(
            collective_id=0, has_side_effects=True, vmem_limit_bytes=48 * 1024 * 1024
        ),
    )(hidden, weight.T, factor_b.T, factor_a, magnitude, cotangent)
    return mixed, gmag[0, :18], grads[:, 72:90], grads[:, :72].T


def solution(mesh):
    return jax.shard_map(
        body,
        mesh=mesh,
        in_specs=(
            P("dp", "tensor"),
            P("tensor", "dp"),
            P("tensor", None),
            P(None, "dp"),
            P("tensor"),
            P("dp", "tensor"),
        ),
        out_specs=(
            P("dp", "tensor"),
            P(("tensor", "dp")),
            P(None, ("tensor", "dp")),
            P(("tensor", "dp"), None),
        ),
        check_vma=False,
    )
```

```python
import functools

import jax
import jax.numpy as jnp
from jax import lax
from jax.experimental import pallas as pl
from jax.experimental.pallas import tpu as pltpu
from jax.sharding import PartitionSpec as P

TOK, HID, COLS, OUT, HALF = 320, 2304, 144, 576, 288
MESH = pl.DeviceIdType.MESH
F32, BF = jnp.float32, jnp.bfloat16
CHUNKS = ((0, 80), (80, 64))
FIRST, LAST = 192, 128
PARTS = ((0, 2 * FIRST), (2 * FIRST, 2 * LAST))
WHOLE = 5
FAR = (WHOLE + 1) // 2


def remote(src, dst, send, recv, dp, tensor):
    return pltpu.make_async_remote_copy(
        src_ref=src, dst_ref=dst, send_sem=send, recv_sem=recv,
        device_id=(dp, tensor), device_id_type=MESH,
    )


def kernel(h_ref, w_ref, b_hbm, a_hbm, mag_hbm, cot_hbm, mixed_ref, grads_ref, gmag_ref,
           b_ref, a_ref, mag_ref, cot_ref, own, toks, wts, outgoing, arrived, turned, halves,
           sq_out, sq_in, msg_f, msg, msgs, a_all, sq_all, norms, scales, low_in, back_in, low_out, back_out,
           dpre, extra, cots,
           spread, spread_in, plane, plane_in, mag_out, mag_in, sums, results,
           loc_sem, w_send, w_recv, t_send, t_recv, y_send, y_recv, x_send, x_recv,
           s_send, s_recv, m_send, m_recv, l_send, l_recv, b_send, b_recv, d_send, d_recv, p_send, p_recv,
           g_send, g_recv,
           arrived_w, turned_a, turned_b, whole_a, whole_b, flat, e_recv, f_send, f_recv, met):
    dp, tensor = lax.axis_index("dp"), lax.axis_index("tensor")
    x_hi, z, core = dp // 16, (dp // 2) % 8, dp % 2
    x_lo, y = tensor // 4, tensor % 4
    other = 1 - core

    def dp_of(a, b, c):
        return a * 16 + b * 2 + c

    def rows(part, of):
        if part == 0:
            return pl.ds(of * FIRST, FIRST), pl.ds(0, FIRST)
        return pl.ds(2 * FIRST + of * LAST, LAST), pl.ds(FIRST, LAST)

    load_h = pltpu.make_async_copy(h_ref, own, loc_sem.at[0])
    place = []
    for part in range(2):
        there, here = rows(part, core)
        place.append(pltpu.make_async_copy(h_ref.at[here], toks.at[0, there], loc_sem.at[6 + part]))
    load_w = pltpu.make_async_copy(w_ref, wts.at[0], loc_sem.at[1])
    loads = [pltpu.make_async_copy(src, dst, loc_sem.at[2 + i]) for i, (src, dst) in enumerate(
        ((a_hbm, a_ref), (b_hbm, b_ref), (mag_hbm, mag_ref), (cot_hbm, cot_ref)))]
    load_w.start()
    loads[0].start()
    loads[1].start()
    load_h.start()
    place[0].start()
    place[1].start()
    loads[2].start()
    loads[3].start()

    barrier = pltpu.get_barrier_semaphore()

    def greet(p):
        pl.semaphore_signal(barrier, inc=1, device_id=p, device_id_type=MESH)

    near = [(dp, (tensor + k) % 8) for k in range(1, 8)]
    near += [(dp_of(x_hi, (z + 1) % 8, core), tensor), (dp_of(x_hi, (z + 7) % 8, core), tensor),
             (dp_of(x_hi, z, other), tensor), (dp_of(1 - x_hi, z, core), tensor), (dp_of(1 - x_hi, z, other), tensor)]
    for p in near:
        greet(p)
    spread[...] = jnp.zeros_like(spread)
    msg_f[...] = jnp.zeros_like(msg_f)
    load_w.wait()
    load_h.wait()
    with jax.named_scope('barrier_wait'):
        pl.semaphore_wait(barrier, len(near))

    def tell(k):
        for to in ((z + k) % 8, (z + 8 - k) % 8)[:1 if k == 4 else 2]:
            pl.semaphore_signal(met.at[k // 2], inc=1, device_id=(dp_of(x_hi, to, core), tensor), device_id_type=MESH)

    tell(1)

    def w_copy(side, k, ch):
        at, n = CHUNKS[ch]
        src = 0 if k == 1 else 2 * (k - 1) - 1 + side
        dst = 7 if k == 4 else 2 * k - 1 + side
        to = (z + 1) % 8 if side == 0 else (z + 7) % 8
        return remote(wts.at[src, pl.ds(at, n)], wts.at[dst, pl.ds(at, n)],
                      w_send.at[side, k - 1, ch], w_recv.at[dst, ch], dp_of(x_hi, to, core), tensor)

    w_copy(0, 1, 0).start()
    w_copy(1, 1, 1).start()
    w_copy(0, 1, 1).start()
    w_copy(1, 1, 0).start()
    to_other, to_far, relay = [], [], []
    for part in range(2):
        there, here = rows(part, core)
        to_other.append(remote(own.at[here], toks.at[0, there], t_send.at[0, part], t_recv.at[0, part],
                               dp_of(x_hi, z, other), tensor))
        to_far.append(remote(own.at[here], toks.at[1, there], t_send.at[1, part], t_recv.at[1, part],
                             dp_of(1 - x_hi, z, core), tensor))
        relay.append(remote(toks.at[1, there], toks.at[1, there], t_send.at[2, part], t_recv.at[2, part],
                            dp_of(x_hi, z, other), tensor))

    to_other[0].start()
    to_other[1].start()

    owner = dp // 4
    loads[0].wait()
    loads[1].wait()
    merged = wts[0].astype(F32) + lax.dot_general(
        a_ref[...], b_ref[...], (((0,), (0,)), ((), ())), preferred_element_type=F32)
    squares = merged * merged
    lanes = squares[:, 0:128]
    for i in range(1, 18):
        lanes = lanes + squares[:, 128 * i:128 * (i + 1)]
    own_sq = jnp.sum(lanes.T, axis=0, keepdims=True)
    sq_row = jnp.broadcast_to(own_sq, (8, COLS))

    @pl.when(owner == tensor)
    def _():
        sq_in[tensor] = sq_row

    @pl.when(owner != tensor)
    def _():
        sq_out[...] = sq_row

    low_part = lax.dot_general(b_ref[...], own[...], (((1,), (1,)), ((), ())), preferred_element_type=F32)
    low_out[...] = low_part
    low_in[tensor] = low_part
    sq_copy = remote(sq_out, sq_in.at[tensor], s_send.at[0], s_recv.at[tensor], dp, owner)

    @pl.when(owner != tensor)
    def _():
        sq_copy.start()

    def over_tensor(src, dst, send, recv, act):
        def body(i, carry):
            to = (tensor + i) % 8
            if act == "recv":
                remote(src, dst.at[to], send.at[i], recv.at[to], dp, to).wait_recv()
            elif act == "start":
                remote(src, dst.at[tensor], send.at[i], recv.at[tensor], dp, to).start()
            else:
                remote(src, dst.at[tensor], send.at[i], recv.at[tensor], dp, to).wait_send()
            return carry
        lax.fori_loop(1, 8, body, 0)

    over_tensor(low_out, low_in, l_send, l_recv, "start")
    to_far[0].start()
    to_far[1].start()

    pl.semaphore_wait(met.at[0], 2)
    tell(2)
    loads[2].wait()
    loads[3].wait()

    def zsrc_of(j):
        k = (j + 1) // 2
        return (z + 8 + k - 2 * k * (j % 2)) % 8

    def summer(j, g):
        return (zsrc_of(j) + 2 * g + core) % 4

    def y_copy(j, g, part):
        zs, lanes = zsrc_of(j), pl.ds(*PARTS[part])
        return remote(outgoing.at[j, g, :, lanes], arrived.at[zs % 2, y, core, :, lanes], y_send.at[j, g, part],
                      y_recv.at[zs % 2, y, core, part], dp_of(x_hi, z, g), x_lo * 4 + zs // 2)

    def local_near(j, g):
        return jnp.logical_and(zsrc_of(j) // 2 == y, core == g)

    def local(j, g):
        return summer(j, g) == y

    def share_lo(g, part):
        return (part + g) % 2

    def e_copy(j, g, part):
        at, n = PARTS[part]
        return remote(outgoing.at[j, g, :, pl.ds(at, n)], arrived_w.at[j - WHOLE, tensor, :, pl.ds(0, n)],
                      y_send.at[j, g, part], e_recv.at[j, tensor], dp, share_lo(g, part) * 4 + summer(j, g))

    def local_whole(j, g, part):
        return jnp.logical_and(local(j, g), share_lo(g, part) == x_lo)

    def item(j, g, parts, whole):
        lo, hi = PARTS[parts[0]][0], sum(PARTS[parts[-1]])
        p = lax.dot_general(toks[g, lo:hi], wts[j], (((1,), (1,)), ((), ())), preferred_element_type=F32)
        p = p.T.astype(BF)
        if whole:
            for part in parts:
                at, n = PARTS[part]
                piece = p[:, at - lo:at - lo + n]
                here = local_whole(j, g, part)

                @pl.when(here)
                def _():
                    arrived_w[j - WHOLE, tensor, :, 0:n] = piece

                @pl.when(jnp.logical_not(here))
                def _():
                    outgoing[j, g, :, at:at + n] = piece
                    e_copy(j, g, part).start()
            return
        here = local_near(j, g)

        @pl.when(here)
        def _():
            arrived[zsrc_of(j) % 2, y, core, :, lo:hi] = p

        @pl.when(jnp.logical_not(here))
        def _():
            outgoing[j, g, :, lo:hi] = p
            for part in parts:
                y_copy(j, g, part).start()

    def split(lo, hi):
        mid = min(max(lo, WHOLE), hi)
        return [(a, b, w) for a, b, w in ((lo, mid, False), (mid, hi, True)) if b > a]

    def items(lo, hi, g, parts=(0, 1)):
        for a, b, whole in split(lo, hi):
            def body(j, carry, whole=whole):
                item(j, g, parts, whole)
                return carry
            lax.fori_loop(a, b, body, 0)

    def items_both(lo, hi):
        for a, b, whole in split(lo, hi):
            def body(i, carry, a=a, whole=whole):
                item(a + i // 2, i % 2, (0, 1), whole)
                return carry
            lax.fori_loop(0, 2 * (b - a), body, 0)

    def msg_copy(i):
        return remote(msg, msgs.at[dp % 4], m_send.at[i], m_recv.at[dp % 4], (dp + i) % 32, tensor)

    def publish():
        def arrive(i, carry):
            frm = (tensor + i) % 8
            remote(sq_out, sq_in.at[frm], s_send.at[0], s_recv.at[frm], dp, frm).wait_recv()
            return carry
        lax.fori_loop(1, 8, arrive, 0)
        total = sq_in[0]
        for i in range(1, 8):
            total = total + sq_in[i]
        total = total[0:1]
        high = total.astype(BF).astype(F32)
        rest = total - high
        msg_f[:, 0:COLS] = a_ref[...].astype(F32)
        for i in range(3):
            msg_f[i:i + 1, 144:192] = high[:, 48 * i:48 * (i + 1)]
            msg_f[3 + i:4 + i, 144:192] = rest[:, 48 * i:48 * (i + 1)]
        packed = msg_f[...].astype(BF)
        msg[...] = packed
        msgs[dp % 4] = packed

        def send(i, carry):
            msg_copy(i).start()
            return carry
        lax.fori_loop(1, 32, send, 0)

    def receive():
        for j in range(4):
            @pl.when(dp != tensor * 4 + j)
            def _():
                remote(msg, msgs.at[j], m_send.at[0], m_recv.at[j], dp, tensor).wait_recv()
        for j in range(4):
            m = msgs[j].astype(F32)
            zp, at = j // 2, COLS * (j % 2)
            a_all[zp, :, at:at + COLS] = m[:, 0:COLS]
            for i in range(3):
                sq_all[zp, :, at + 48 * i:at + 48 * (i + 1)] = m[i:i + 1, 144:192] + m[3 + i:4 + i, 144:192]

    def backward():
        back = None
        mags = mag_ref[...].reshape(1, OUT)
        for zp in range(2):
            norm = jnp.sqrt(sq_all[zp] + 1e-6)
            scale = mags[:, HALF * zp:HALF * (zp + 1)] / norm
            norms[zp] = norm
            scales[zp] = scale
            cot = cot_ref[:, HALF * zp:HALF * (zp + 1)].astype(F32)
            cots[zp] = cot
            d = (cot * scale).astype(BF)
            dpre[zp] = d
            part = lax.dot_general(a_all[zp].astype(BF), d, (((1,), (1,)), ((), ())), preferred_element_type=F32)
            back = part if back is None else back + part
        back_out[...] = back
        back_in[tensor] = back
        over_tensor(back_out, back_in, b_send, b_recv, "start")

    group = x_hi * 2 + core

    def spread_copy(i):
        to = (group + i) % 4
        return remote(spread.at[to], spread_in.at[group], d_send.at[i], d_recv.at[group],
                      dp_of(to // 2, z, to % 2), tensor)

    def gradients():
        over_tensor(low_out, low_in, l_send, l_recv, "recv")
        over_tensor(back_out, back_in, b_send, b_recv, "recv")
        low, back = low_in[0], back_in[0]
        for i in range(1, 8):
            low = low + low_in[i]
            back = back + back_in[i]
        low, back = low.astype(BF), back.astype(BF)
        grad_b = jnp.dot(back, own[...], preferred_element_type=F32)
        grad_a = [jnp.dot(low, dpre[zp], preferred_element_type=F32) for zp in range(2)]
        for x in range(2):
            for zz in range(8):
                for c in range(2):
                    i = x * 16 + zz * 2 + c
                    spread[x * 2 + c, zz, :, 0:72] = grad_b[:, 72 * i:72 * (i + 1)]
                    spread[x * 2 + c, zz, :, 72:90] = grad_a[x][:, 18 * (i % 16):18 * (i % 16 + 1)]
        for i in range(1, 4):
            spread_copy(i).start()
        for zp in range(2):
            extra[zp] = lax.dot_general(low, a_all[zp].astype(BF), (((0,), (0,)), ((), ())),
                                        preferred_element_type=F32)

    def plane_copy(i):
        to = (z + i) % 8
        return remote(plane.at[to], plane_in.at[z], p_send.at[i], p_recv.at[z], dp_of(x_hi, to, core), tensor)

    def sum_plane():
        total = spread[group]
        for i in range(1, 4):
            frm = (group + i) % 4
            remote(spread.at[0], spread_in.at[frm], d_send.at[0], d_recv.at[frm], dp, tensor).wait_recv()
            total = total + spread_in[frm]
        plane[...] = total

        def send(i, carry):
            plane_copy(i).start()
            return carry
        lax.fori_loop(1, 8, send, 0)

    def sum_planes():
        total = plane[z]
        for i in range(1, 8):
            frm = (z + i) % 8
            remote(plane.at[0], plane_in.at[frm], p_send.at[0], p_recv.at[frm], dp, tensor).wait_recv()
            total = total + plane_in[frm]
        grads_ref[...] = total

    def ring(k, first):
        for side in (0, 1):
            ch = first if side == 0 else 1 - first
            w_copy(side, k, ch).wait_recv()
            if k < 3 or first == 0:
                w_copy(side, k + 1, ch).start()

    def x_copy(zp, ct):
        tok_hi = jnp.where(core == 0, x_hi, 1 - x_hi)
        return remote(turned.at[zp, ct], halves.at[x_lo, zp], x_send.at[zp, ct],
                      x_recv.at[x_lo, zp], dp_of(tok_hi, z, ct), x_hi * 4 + y)

    def near_self(ct):
        return jnp.logical_and(x_lo == x_hi, jnp.logical_and(core == 0, ct == 0))

    def to_self(j, g, ct):
        same = jnp.logical_and(g == 0, x_lo == x_hi)
        return jnp.logical_and(same, jnp.logical_and(zsrc_of(j) // 2 == y, core == ct))

    def active(j, g):
        return summer(j, g) == y

    def stage_near(zp):
        parts = [[], []]
        for cs in range(2):
            for k in range(4):
                ys = (y + k) % 4

                def arrive(ys=ys, cs=cs):
                    for part in range(2):
                        lanes = pl.ds(*PARTS[part])
                        remote(outgoing.at[0, 0, :, lanes], arrived.at[zp, ys, cs, :, lanes], y_send.at[0, 0, part],
                               y_recv.at[zp, ys, cs, part], dp, tensor).wait_recv()
                if k == 0:
                    pl.when(core != cs)(arrive)
                else:
                    arrive()
            total = arrived[zp, 0, cs].astype(F32)
            for ys in range(1, 4):
                total = total + arrived[zp, ys, cs].astype(F32)
            total = total.astype(BF)
            for ct in range(2):
                parts[ct] += [total[:, ct * FIRST:(ct + 1) * FIRST],
                              total[:, 2 * FIRST + ct * LAST:2 * FIRST + (ct + 1) * LAST]]
        for ct in range(2):
            both = jnp.concatenate(parts[ct], axis=1)

            @pl.when(near_self(ct))
            def _():
                halves[x_lo, zp] = both

            @pl.when(jnp.logical_not(near_self(ct)))
            def _():
                turned[zp, ct] = both
                x_copy(zp, ct).start()

    def f_copy(j, g, ct, part):
        zs = zsrc_of(j)
        tok_hi = jnp.where(g == 0, x_hi, 1 - x_hi)
        src, dst = ((turned_a, whole_a), (turned_b, whole_b))[part]
        return remote(src.at[j - WHOLE, ct], dst.at[zs % 2, core], f_send.at[j, ct],
                      f_recv.at[zs % 2, core, part], dp_of(tok_hi, z, ct), x_hi * 4 + zs // 2)

    def stage_whole(j, g):
        for part in range(2):
            @pl.when(share_lo(g, part) == x_lo)
            def _(part=part):
                n = PARTS[part][1]
                for k in range(1, 8):
                    frm = (tensor + k) % 8
                    remote(outgoing.at[0, 0, :, pl.ds(0, n)], arrived_w.at[j - WHOLE, frm, :, pl.ds(0, n)],
                           y_send.at[0, 0, part], e_recv.at[j, frm], dp, tensor).wait_recv()
                total = arrived_w[j - WHOLE, 0, :, 0:n].astype(F32)
                for k in range(1, 8):
                    total = total + arrived_w[j - WHOLE, k, :, 0:n].astype(F32)
                total = total.astype(BF)
                src, dst = ((turned_a, whole_a), (turned_b, whole_b))[part]
                for ct in range(2):
                    piece = total[:, ct * (n // 2):(ct + 1) * (n // 2)]
                    mine_too = to_self(j, g, ct)

                    @pl.when(mine_too)
                    def _():
                        dst[zsrc_of(j) % 2, core] = piece

                    @pl.when(jnp.logical_not(mine_too))
                    def _():
                        src[j - WHOLE, ct] = piece
                        f_copy(j, g, ct, part).start()

    def second(lo, hi, g):
        def unit(j, carry):
            pl.when(active(j, g))(lambda: stage_whole(j, g))
            return carry
        lax.fori_loop(lo, hi, unit, 0)

    def near_units(which, lo, hi):
        def unit(zp, carry):
            step = steps_of(zp)
            here = jnp.logical_and(jnp.logical_and(step >= lo, step <= hi), core == which)
            pl.when(here)(lambda: stage_near(zp))
            return carry
        lax.fori_loop(0, 2, unit, 0)

    def steps_of(zp):
        away = (2 * y + zp - z + 8) % 8
        return jnp.where(away > 4, 8 - away, away)

    with jax.named_scope("a0"):
        for part in range(2):
            place[part].wait()
            to_other[part].wait_recv()
    items(0, 1, 0)
    pl.semaphore_wait(met.at[1], 2)
    tell(4)

    def publish_when_met():
        pl.semaphore_wait(met.at[2], 1)
        publish()
    with jax.named_scope("a1_publish"):
        pl.when(owner == tensor)(publish_when_met)
    with jax.named_scope("a2_ring10"):
        ring(1, 0)

    @pl.when(owner != tensor)
    def _():
        pl.semaphore_wait(met.at[2], 1)
    with jax.named_scope("a3_ring11"):
        ring(1, 1)
    items(1, 3, 0)
    with jax.named_scope("a4_far0"):
        to_far[0].wait_recv()
    relay[0].start()
    with jax.named_scope("a5_ring20"):
        ring(2, 0)
    with jax.named_scope("a6_relay0"):
        relay[0].wait_recv()
    items(0, 3, 1, (0,))
    with jax.named_scope("a8_ring21"):
        ring(2, 1)
    items(3, 5, 0)
    items(3, 5, 1, (0,))
    with jax.named_scope("a9_far1"):
        to_far[1].wait_recv()
    relay[1].start()
    with jax.named_scope("aa_receive"):
        receive()
    backward()
    with jax.named_scope("aa_relay1"):
        relay[1].wait_recv()
    items(0, 5, 1, (1,))
    with jax.named_scope("ab_ring30"):
        ring(3, 0)
    with jax.named_scope("ac_near"):
        near_units(0, 0, 1)
    with jax.named_scope("b1_ring31"):
        ring(3, 1)
    with jax.named_scope("b2_items"):
        items_both(5, 7)
    with jax.named_scope("b3_grads"):
        gradients()
    with jax.named_scope("b5_last"):
        w_copy(0, 4, 0).wait_recv()
        w_copy(1, 4, 1).wait_recv()
    with jax.named_scope("b6_items"):
        items_both(7, 8)
    with jax.named_scope("b7_second"):
        second(5, 7, 0)
        second(5, 7, 1)
    with jax.named_scope("b8_near"):
        near_units(0, 2, 2)
        near_units(1, 0, 1)
    with jax.named_scope("ba_second"):
        second(7, 8, 0)
        second(7, 8, 1)
    with jax.named_scope("bb_near"):
        near_units(1, 2, 2)

    def finish(i, carry):
        zp = jnp.where(steps_of(0) <= steps_of(1), i, 1 - i)
        away = jnp.where(x_lo == x_hi, 0, 1)
        whole = steps_of(zp) >= FAR

        @pl.when(jnp.logical_not(whole))
        def _():
            for xl in range(2):
                own_part = jnp.logical_and(jnp.logical_and(x_lo == x_hi, xl == x_lo), core == 0)

                @pl.when(jnp.logical_not(own_part))
                def _():
                    remote(turned.at[0, 0], halves.at[xl, zp], x_send.at[0, 0], x_recv.at[xl, zp],
                           dp, tensor).wait_recv()
            both = halves[0, zp].astype(F32) + halves[1, zp].astype(F32)
            for cs in range(2):
                flat[cs * COLS:(cs + 1) * COLS, :] = both[:, cs * TOK:(cs + 1) * TOK]

        @pl.when(whole)
        def _():
            for cs in range(2):
                for part in range(2):
                    frm = (2 * y + zp + 2 * away + cs) % 4
                    own_part = jnp.logical_and(jnp.logical_and(x_lo == x_hi, (part + away) % 2 == x_lo),
                                               jnp.logical_and(frm == y, core == cs))
                    src, dst = ((turned_a, whole_a), (turned_b, whole_b))[part]

                    @pl.when(jnp.logical_not(own_part))
                    def _():
                        remote(src.at[0, 0], dst.at[zp, cs], f_send.at[0, 0], f_recv.at[zp, cs, part],
                               dp, tensor).wait_recv()
                flat[cs * COLS:(cs + 1) * COLS, 0:FIRST] = whole_a[zp, cs].astype(F32)
                flat[cs * COLS:(cs + 1) * COLS, FIRST:TOK] = whole_b[zp, cs].astype(F32)
        pre = extra[zp] + flat[...].T
        sums[zp] = jnp.sum(cots[zp] * pre, axis=0, keepdims=True) / norms[zp]
        results[zp] = pre * scales[zp]
        return carry
    with jax.named_scope("c0_finish"):
        lax.fori_loop(0, 2, finish, 0)
    for i in range(32):
        mag_out[i, :, 0:18] = sums[i // 16][:, 18 * (i % 16):18 * (i % 16 + 1)]

    def mag_copy(i):
        to = (dp + i) % 32
        return remote(mag_out.at[to], mag_in.at[dp], g_send.at[i], g_recv.at[dp], to, tensor)

    def mag_start(i, carry):
        mag_copy(i).start()
        return carry
    with jax.named_scope("c1_mag"):
        lax.fori_loop(1, 32, mag_start, 0)
    with jax.named_scope("c3_plane"):
        sum_plane()
    with jax.named_scope("c2_mixed"):
        for zp in range(2):
            mixed_ref[:, HALF * zp:HALF * (zp + 1)] = results[zp].astype(BF)
    with jax.named_scope("c4_planes"):
        sum_planes()

    for k in (1, 2, 3, 4):
        for side in (0, 1):
            for ch in (0, 1):
                if k < 4 or ch == side:
                    w_copy(side, k, ch).wait_send()
    @pl.when(owner != tensor)
    def _():
        sq_copy.wait_send()

    @pl.when(owner == tensor)
    def _():
        def sent(i, carry):
            msg_copy(i).wait_send()
            return carry
        lax.fori_loop(1, 32, sent, 0)
    over_tensor(low_out, low_in, l_send, l_recv, "send")
    over_tensor(back_out, back_in, b_send, b_recv, "send")
    for i in range(1, 4):
        spread_copy(i).wait_send()

    def plane_sent(i, carry):
        plane_copy(i).wait_send()
        return carry
    lax.fori_loop(1, 8, plane_sent, 0)
    for copies in (to_other, to_far, relay):
        for part in range(2):
            copies[part].wait_send()
    def drain(j, carry):
        for g in range(2):
            @pl.when(jnp.logical_not(local_near(j, g)))
            def _():
                for part in range(2):
                    y_copy(j, g, part).wait_send()
        return carry
    lax.fori_loop(0, WHOLE, drain, 0)

    def drain_near(zp, carry):
        for ct in range(2):
            @pl.when(jnp.logical_and(steps_of(zp) < FAR, jnp.logical_not(near_self(ct))))
            def _():
                x_copy(zp, ct).wait_send()
        return carry
    lax.fori_loop(0, 2, drain_near, 0)

    def drain_whole(j, carry):
        for g in range(2):
            for part in range(2):
                @pl.when(jnp.logical_not(local_whole(j, g, part)))
                def _():
                    e_copy(j, g, part).wait_send()
                for ct in range(2):
                    @pl.when(jnp.logical_and(local_whole(j, g, part), jnp.logical_not(to_self(j, g, ct))))
                    def _():
                        f_copy(j, g, ct, part).wait_send()
        return carry
    lax.fori_loop(WHOLE, 8, drain_whole, 0)

    def mag_arrive(i, total):
        frm = (dp + i) % 32
        remote(mag_out.at[0], mag_in.at[frm], g_send.at[0], g_recv.at[frm], dp, tensor).wait_recv()
        return total + mag_in[frm]
    with jax.named_scope("c5_gmag"):
        gmag_ref[...] = lax.fori_loop(1, 32, mag_arrive, mag_out[dp])

    def mag_sent(i, carry):
        mag_copy(i).wait_send()
        return carry
    lax.fori_loop(1, 32, mag_sent, 0)


def body(hidden, weight, factor_b, factor_a, magnitude, cotangent):
    hbm_spec, vmem_spec = pl.BlockSpec(memory_space=pltpu.HBM), pl.BlockSpec(memory_space=pltpu.VMEM)
    dma, vmem = pltpu.SemaphoreType.DMA, pltpu.VMEM
    mixed, grads, gmag = pl.pallas_call(
        kernel,
        name="dora",
        out_shape=(jax.ShapeDtypeStruct((TOK, OUT), BF), jax.ShapeDtypeStruct((16, 128), F32),
                   jax.ShapeDtypeStruct((1, 128), F32)),
        in_specs=[hbm_spec] * 6,
        out_specs=(vmem_spec,) * 3,
        scratch_shapes=[
            vmem((16, HID), BF), vmem((16, COLS), BF), vmem((OUT,), F32), vmem((TOK, OUT), BF), vmem((TOK, HID), BF),
            vmem((2, 2 * TOK, HID), BF),
            vmem((8, COLS, HID), BF),
            vmem((8, 2, COLS, 2 * TOK), BF),
            vmem((2, 4, 2, COLS, 2 * TOK), BF),
            vmem((2, 2, COLS, 2 * TOK), BF),
            vmem((2, 2, COLS, 2 * TOK), BF),
            vmem((8, COLS), F32), vmem((8, 8, COLS), F32),
            vmem((16, 256), F32), vmem((16, 256), BF), vmem((4, 16, 256), BF),
            vmem((2, 16, HALF), F32), vmem((2, 1, HALF), F32), vmem((2, 1, HALF), F32), vmem((2, 1, HALF), F32),
            vmem((8, 16, TOK), F32), vmem((8, 16, TOK), F32), vmem((16, TOK), F32), vmem((16, TOK), F32),
            vmem((2, TOK, HALF), BF), vmem((2, TOK, HALF), F32), vmem((2, TOK, HALF), F32),
            vmem((4, 8, 16, 128), F32), vmem((4, 8, 16, 128), F32),
            vmem((8, 16, 128), F32), vmem((8, 16, 128), F32),
            vmem((32, 1, 128), F32), vmem((32, 1, 128), F32), vmem((2, 1, HALF), F32), vmem((2, TOK, HALF), F32),
            dma((8,)), dma((2, 4, 2)), dma((8, 2)), dma((3, 2)), dma((3, 2)),
            dma((8, 2, 2)), dma((2, 4, 2, 2)), dma((2, 2)), dma((2, 2)),
            dma((1,)), dma((8,)), dma((32,)), dma((4,)), dma((8,)), dma((8,)), dma((8,)), dma((8,)),
            dma((4,)), dma((4,)), dma((8,)), dma((8,)), dma((32,)), dma((32,)),
            vmem((8 - WHOLE, 8, COLS, 2 * FIRST), BF),
            vmem((8 - WHOLE, 2, COLS, FIRST), BF), vmem((8 - WHOLE, 2, COLS, LAST), BF),
            vmem((2, 2, COLS, FIRST), BF), vmem((2, 2, COLS, LAST), BF), vmem((2 * COLS, TOK), F32),
            dma((8, 8)), dma((8, 2)), dma((2, 2, 2)), pltpu.SemaphoreType.REGULAR((3,)),
        ],
        compiler_params=pltpu.CompilerParams(
            collective_id=0, has_side_effects=True, vmem_limit_bytes=48 * 1024 * 1024
        ),
    )(hidden, weight.T, factor_b.T, factor_a, magnitude, cotangent)
    return mixed, gmag[0, :18], grads[:, 72:90], grads[:, :72].T


def solution(mesh):
    return jax.shard_map(
        body,
        mesh=mesh,
        in_specs=(
            P("dp", "tensor"),
            P("tensor", "dp"),
            P("tensor", None),
            P(None, "dp"),
            P("tensor"),
            P("dp", "tensor"),
        ),
        out_specs=(
            P("dp", "tensor"),
            P(("tensor", "dp")),
            P(None, ("tensor", "dp")),
            P(("tensor", "dp"), None),
        ),
        check_vma=False,
    )
```

```python
import functools

import jax
import jax.numpy as jnp
from jax import lax
from jax.experimental import pallas as pl
from jax.experimental.pallas import tpu as pltpu
from jax.sharding import PartitionSpec as P

TOK, HID, COLS, OUT, HALF = 320, 2304, 144, 576, 288
MESH = pl.DeviceIdType.MESH
F32, BF = jnp.float32, jnp.bfloat16
CHUNKS = ((0, 80), (80, 64))
FIRST, LAST = 192, 128
PARTS = ((0, 2 * FIRST), (2 * FIRST, 2 * LAST))
WHOLE = 8
FAR = WHOLE // 2 + 1


def remote(src, dst, send, recv, dp, tensor):
    return pltpu.make_async_remote_copy(
        src_ref=src, dst_ref=dst, send_sem=send, recv_sem=recv,
        device_id=(dp, tensor), device_id_type=MESH,
    )


def kernel(h_ref, w_ref, b_hbm, a_hbm, mag_hbm, cot_hbm, mixed_ref, grads_ref, gmag_ref,
           b_ref, a_ref, mag_ref, cot_ref, own, toks, wts, outgoing, arrived, turned, halves,
           sq_out, sq_in, msg_f, msg, msgs, a_all, sq_all, norms, scales, low_in, back_in, low_out, back_out,
           dpre, extra, cots,
           spread, spread_in, plane, plane_in, mag_out, mag_in, sums, results,
           loc_sem, w_send, w_recv, t_send, t_recv, y_send, y_recv, x_send, x_recv,
           s_send, s_recv, m_send, m_recv, l_send, l_recv, b_send, b_recv, d_send, d_recv, p_send, p_recv,
           g_send, g_recv,
           arrived_w, turned_a, turned_b, whole_a, whole_b, flat, e_recv, f_send, f_recv, met):
    dp, tensor = lax.axis_index("dp"), lax.axis_index("tensor")
    x_hi, z, core = dp // 16, (dp // 2) % 8, dp % 2
    x_lo, y = tensor // 4, tensor % 4
    other = 1 - core

    def dp_of(a, b, c):
        return a * 16 + b * 2 + c

    def rows(part, of):
        if part == 0:
            return pl.ds(of * FIRST, FIRST), pl.ds(0, FIRST)
        return pl.ds(2 * FIRST + of * LAST, LAST), pl.ds(FIRST, LAST)

    load_h = pltpu.make_async_copy(h_ref, own, loc_sem.at[0])
    place = []
    for part in range(2):
        there, here = rows(part, core)
        place.append(pltpu.make_async_copy(h_ref.at[here], toks.at[0, there], loc_sem.at[6 + part]))
    load_w = pltpu.make_async_copy(w_ref, wts.at[0], loc_sem.at[1])
    loads = [pltpu.make_async_copy(src, dst, loc_sem.at[2 + i]) for i, (src, dst) in enumerate(
        ((a_hbm, a_ref), (b_hbm, b_ref), (mag_hbm, mag_ref), (cot_hbm, cot_ref)))]
    load_w.start()
    loads[0].start()
    loads[1].start()
    load_h.start()
    place[0].start()
    place[1].start()
    loads[2].start()
    loads[3].start()

    barrier = pltpu.get_barrier_semaphore()

    def greet(p):
        pl.semaphore_signal(barrier, inc=1, device_id=p, device_id_type=MESH)

    near = [(dp, (tensor + k) % 8) for k in range(1, 8)]
    near += [(dp_of(x_hi, (z + 1) % 8, core), tensor), (dp_of(x_hi, (z + 7) % 8, core), tensor),
             (dp_of(x_hi, z, other), tensor), (dp_of(1 - x_hi, z, core), tensor), (dp_of(1 - x_hi, z, other), tensor)]
    for p in near:
        greet(p)
    spread[...] = jnp.zeros_like(spread)
    msg_f[...] = jnp.zeros_like(msg_f)
    load_w.wait()
    load_h.wait()
    with jax.named_scope('barrier_wait'):
        pl.semaphore_wait(barrier, len(near))

    def tell(k):
        for to in ((z + k) % 8, (z + 8 - k) % 8)[:1 if k == 4 else 2]:
            pl.semaphore_signal(met.at[k // 2], inc=1, device_id=(dp_of(x_hi, to, core), tensor), device_id_type=MESH)

    tell(1)

    def w_copy(side, k, ch):
        at, n = CHUNKS[ch]
        src = 0 if k == 1 else 2 * (k - 1) - 1 + side
        dst = 7 if k == 4 else 2 * k - 1 + side
        to = (z + 1) % 8 if side == 0 else (z + 7) % 8
        return remote(wts.at[src, pl.ds(at, n)], wts.at[dst, pl.ds(at, n)],
                      w_send.at[side, k - 1, ch], w_recv.at[dst, ch], dp_of(x_hi, to, core), tensor)

    w_copy(0, 1, 0).start()
    w_copy(1, 1, 1).start()
    w_copy(0, 1, 1).start()
    w_copy(1, 1, 0).start()
    to_other, to_far, relay = [], [], []
    for part in range(2):
        there, here = rows(part, core)
        to_other.append(remote(own.at[here], toks.at[0, there], t_send.at[0, part], t_recv.at[0, part],
                               dp_of(x_hi, z, other), tensor))
        to_far.append(remote(own.at[here], toks.at[1, there], t_send.at[1, part], t_recv.at[1, part],
                             dp_of(1 - x_hi, z, core), tensor))
        relay.append(remote(toks.at[1, there], toks.at[1, there], t_send.at[2, part], t_recv.at[2, part],
                            dp_of(x_hi, z, other), tensor))

    to_other[0].start()
    to_other[1].start()

    owner = dp // 4
    loads[0].wait()
    loads[1].wait()
    merged = wts[0].astype(F32) + lax.dot_general(
        a_ref[...], b_ref[...], (((0,), (0,)), ((), ())), preferred_element_type=F32)
    squares = merged * merged
    lanes = squares[:, 0:128]
    for i in range(1, 18):
        lanes = lanes + squares[:, 128 * i:128 * (i + 1)]
    own_sq = jnp.sum(lanes.T, axis=0, keepdims=True)
    sq_row = jnp.broadcast_to(own_sq, (8, COLS))

    @pl.when(owner == tensor)
    def _():
        sq_in[tensor] = sq_row

    @pl.when(owner != tensor)
    def _():
        sq_out[...] = sq_row

    low_part = lax.dot_general(b_ref[...], own[...], (((1,), (1,)), ((), ())), preferred_element_type=F32)
    low_out[...] = low_part
    low_in[tensor] = low_part
    sq_copy = remote(sq_out, sq_in.at[tensor], s_send.at[0], s_recv.at[tensor], dp, owner)

    @pl.when(owner != tensor)
    def _():
        sq_copy.start()

    def over_tensor(src, dst, send, recv, act):
        def body(i, carry):
            to = (tensor + i) % 8
            if act == "recv":
                remote(src, dst.at[to], send.at[i], recv.at[to], dp, to).wait_recv()
            elif act == "start":
                remote(src, dst.at[tensor], send.at[i], recv.at[tensor], dp, to).start()
            else:
                remote(src, dst.at[tensor], send.at[i], recv.at[tensor], dp, to).wait_send()
            return carry
        lax.fori_loop(1, 8, body, 0)

    over_tensor(low_out, low_in, l_send, l_recv, "start")
    to_far[0].start()
    to_far[1].start()

    pl.semaphore_wait(met.at[0], 2)
    tell(2)
    loads[2].wait()
    loads[3].wait()

    def zsrc_of(j):
        k = (j + 1) // 2
        return (z + 8 + k - 2 * k * (j % 2)) % 8

    def summer_at(owner_y, g, of):
        return (owner_y + jnp.where(g == 0, 3 - 2 * of, 2 * of)) % 4

    def summer(j, g):
        return summer_at(zsrc_of(j) // 2, g, core)

    def y_copy(j, g, part):
        lanes = pl.ds(*PARTS[part])
        return remote(outgoing.at[j, g, :, lanes], arrived.at[j, y, :, lanes], y_send.at[j, g, part],
                      y_recv.at[j, y, part], dp, x_lo * 4 + summer(j, g))

    def local(j, g):
        return summer(j, g) == y

    def share_lo(g, part):
        return (part + g) % 2

    def e_copy(j, g, part):
        at, n = PARTS[part]
        return remote(outgoing.at[j, g, :, pl.ds(at, n)], arrived_w.at[j - WHOLE, tensor, :, pl.ds(0, n)],
                      y_send.at[j, g, part], e_recv.at[j, tensor], dp, share_lo(g, part) * 4 + summer(j, g))

    def local_whole(j, g, part):
        return jnp.logical_and(local(j, g), share_lo(g, part) == x_lo)

    def item(j, g, parts, whole):
        lo, hi = PARTS[parts[0]][0], sum(PARTS[parts[-1]])
        p = lax.dot_general(toks[g, lo:hi], wts[j], (((1,), (1,)), ((), ())), preferred_element_type=F32)
        p = p.T.astype(BF)
        if whole:
            for part in parts:
                at, n = PARTS[part]
                piece = p[:, at - lo:at - lo + n]
                here = local_whole(j, g, part)

                @pl.when(here)
                def _():
                    arrived_w[j - WHOLE, tensor, :, 0:n] = piece

                @pl.when(jnp.logical_not(here))
                def _():
                    outgoing[j, g, :, at:at + n] = piece
                    e_copy(j, g, part).start()
            return
        here = local(j, g)

        @pl.when(here)
        def _():
            arrived[j, y, :, lo:hi] = p

        @pl.when(jnp.logical_not(here))
        def _():
            outgoing[j, g, :, lo:hi] = p
            for part in parts:
                y_copy(j, g, part).start()

    def split(lo, hi):
        mid = min(max(lo, WHOLE), hi)
        return [(a, b, w) for a, b, w in ((lo, mid, False), (mid, hi, True)) if b > a]

    def items(lo, hi, g, parts=(0, 1)):
        for a, b, whole in split(lo, hi):
            def body(j, carry, whole=whole):
                item(j, g, parts, whole)
                return carry
            lax.fori_loop(a, b, body, 0)

    def items_both(lo, hi):
        for a, b, whole in split(lo, hi):
            def body(i, carry, a=a, whole=whole):
                item(a + i // 2, i % 2, (0, 1), whole)
                return carry
            lax.fori_loop(0, 2 * (b - a), body, 0)

    def msg_copy(i):
        return remote(msg, msgs.at[dp % 4], m_send.at[i], m_recv.at[dp % 4], (dp + i) % 32, tensor)

    def publish():
        def arrive(i, carry):
            frm = (tensor + i) % 8
            remote(sq_out, sq_in.at[frm], s_send.at[0], s_recv.at[frm], dp, frm).wait_recv()
            return carry
        lax.fori_loop(1, 8, arrive, 0)
        total = sq_in[0]
        for i in range(1, 8):
            total = total + sq_in[i]
        total = total[0:1]
        high = total.astype(BF).astype(F32)
        rest = total - high
        msg_f[:, 0:COLS] = a_ref[...].astype(F32)
        for i in range(3):
            msg_f[i:i + 1, 144:192] = high[:, 48 * i:48 * (i + 1)]
            msg_f[3 + i:4 + i, 144:192] = rest[:, 48 * i:48 * (i + 1)]
        packed = msg_f[...].astype(BF)
        msg[...] = packed
        msgs[dp % 4] = packed

        def send(i, carry):
            msg_copy(i).start()
            return carry
        lax.fori_loop(1, 32, send, 0)

    def receive():
        for j in range(4):
            @pl.when(dp != tensor * 4 + j)
            def _():
                remote(msg, msgs.at[j], m_send.at[0], m_recv.at[j], dp, tensor).wait_recv()
        for j in range(4):
            m = msgs[j].astype(F32)
            zp, at = j // 2, COLS * (j % 2)
            a_all[zp, :, at:at + COLS] = m[:, 0:COLS]
            for i in range(3):
                sq_all[zp, :, at + 48 * i:at + 48 * (i + 1)] = m[i:i + 1, 144:192] + m[3 + i:4 + i, 144:192]

    def backward():
        back = None
        mags = mag_ref[...].reshape(1, OUT)
        for zp in range(2):
            norm = jnp.sqrt(sq_all[zp] + 1e-6)
            scale = mags[:, HALF * zp:HALF * (zp + 1)] / norm
            norms[zp] = norm
            scales[zp] = scale
            cot = cot_ref[:, HALF * zp:HALF * (zp + 1)].astype(F32)
            cots[zp] = cot
            d = (cot * scale).astype(BF)
            dpre[zp] = d
            part = lax.dot_general(a_all[zp].astype(BF), d, (((1,), (1,)), ((), ())), preferred_element_type=F32)
            back = part if back is None else back + part
        back_out[...] = back
        back_in[tensor] = back
        over_tensor(back_out, back_in, b_send, b_recv, "start")

    group = x_hi * 2 + core

    def spread_copy(i):
        to = (group + i) % 4
        return remote(spread.at[to], spread_in.at[group], d_send.at[i], d_recv.at[group],
                      dp_of(to // 2, z, to % 2), tensor)

    def gradients():
        over_tensor(low_out, low_in, l_send, l_recv, "recv")
        over_tensor(back_out, back_in, b_send, b_recv, "recv")
        low, back = low_in[0], back_in[0]
        for i in range(1, 8):
            low = low + low_in[i]
            back = back + back_in[i]
        low, back = low.astype(BF), back.astype(BF)
        grad_b = jnp.dot(back, own[...], preferred_element_type=F32)
        grad_a = [jnp.dot(low, dpre[zp], preferred_element_type=F32) for zp in range(2)]
        for x in range(2):
            for zz in range(8):
                for c in range(2):
                    i = x * 16 + zz * 2 + c
                    spread[x * 2 + c, zz, :, 0:72] = grad_b[:, 72 * i:72 * (i + 1)]
                    spread[x * 2 + c, zz, :, 72:90] = grad_a[x][:, 18 * (i % 16):18 * (i % 16 + 1)]
        for i in range(1, 4):
            spread_copy(i).start()
        for zp in range(2):
            extra[zp] = lax.dot_general(low, a_all[zp].astype(BF), (((0,), (0,)), ((), ())),
                                        preferred_element_type=F32)

    def plane_copy(i):
        to = (z + i) % 8
        return remote(plane.at[to], plane_in.at[z], p_send.at[i], p_recv.at[z], dp_of(x_hi, to, core), tensor)

    def sum_plane():
        total = spread[group]
        for i in range(1, 4):
            frm = (group + i) % 4
            remote(spread.at[0], spread_in.at[frm], d_send.at[0], d_recv.at[frm], dp, tensor).wait_recv()
            total = total + spread_in[frm]
        plane[...] = total

        def send(i, carry):
            plane_copy(i).start()
            return carry
        lax.fori_loop(1, 8, send, 0)

    def sum_planes():
        total = plane[z]
        for i in range(1, 8):
            frm = (z + i) % 8
            remote(plane.at[0], plane_in.at[frm], p_send.at[0], p_recv.at[frm], dp, tensor).wait_recv()
            total = total + plane_in[frm]
        grads_ref[...] = total

    def ring(k, first):
        for side in (0, 1):
            ch = first if side == 0 else 1 - first
            w_copy(side, k, ch).wait_recv()
            if k < 3 or first == 0:
                w_copy(side, k + 1, ch).start()

    def x_copy(j, g, ct):
        zs = zsrc_of(j)
        tok_hi = jnp.where(g == 0, x_hi, 1 - x_hi)
        return remote(turned.at[j, ct], halves.at[x_lo, zs % 2, core], x_send.at[j, ct],
                      x_recv.at[x_lo, zs % 2, core], dp_of(tok_hi, z, ct), x_hi * 4 + zs // 2)

    def to_self(j, g, ct):
        same = jnp.logical_and(g == 0, x_lo == x_hi)
        return jnp.logical_and(same, jnp.logical_and(zsrc_of(j) // 2 == y, core == ct))

    def active(j, g):
        return summer(j, g) == y

    def stage_two(j, g):
        for k in range(1, 4):
            ys = (y + k) % 4
            for part in range(2):
                lanes = pl.ds(*PARTS[part])
                remote(outgoing.at[0, 0, :, lanes], arrived.at[j, ys, :, lanes], y_send.at[0, 0, part],
                       y_recv.at[j, ys, part], dp, tensor).wait_recv()
        total = arrived[j, 0].astype(F32)
        for ys in range(1, 4):
            total = total + arrived[j, ys].astype(F32)
        total = total.astype(BF)
        for ct in range(2):
            part = jnp.concatenate(
                [total[:, ct * FIRST:(ct + 1) * FIRST],
                 total[:, 2 * FIRST + ct * LAST:2 * FIRST + (ct + 1) * LAST]], axis=1)
            mine_too = to_self(j, g, ct)

            @pl.when(mine_too)
            def _():
                halves[x_lo, zsrc_of(j) % 2, core] = part

            @pl.when(jnp.logical_not(mine_too))
            def _():
                turned[j, ct] = part
                x_copy(j, g, ct).start()

    def f_copy(j, g, ct, part):
        zs = zsrc_of(j)
        tok_hi = jnp.where(g == 0, x_hi, 1 - x_hi)
        src, dst = ((turned_a, whole_a), (turned_b, whole_b))[part]
        return remote(src.at[j - WHOLE, ct], dst.at[zs % 2, core], f_send.at[j, ct],
                      f_recv.at[zs % 2, core, part], dp_of(tok_hi, z, ct), x_hi * 4 + zs // 2)

    def stage_whole(j, g):
        for part in range(2):
            @pl.when(share_lo(g, part) == x_lo)
            def _(part=part):
                n = PARTS[part][1]
                for k in range(1, 8):
                    frm = (tensor + k) % 8
                    remote(outgoing.at[0, 0, :, pl.ds(0, n)], arrived_w.at[j - WHOLE, frm, :, pl.ds(0, n)],
                           y_send.at[0, 0, part], e_recv.at[j, frm], dp, tensor).wait_recv()
                total = arrived_w[j - WHOLE, 0, :, 0:n].astype(F32)
                for k in range(1, 8):
                    total = total + arrived_w[j - WHOLE, k, :, 0:n].astype(F32)
                total = total.astype(BF)
                src, dst = ((turned_a, whole_a), (turned_b, whole_b))[part]
                for ct in range(2):
                    piece = total[:, ct * (n // 2):(ct + 1) * (n // 2)]
                    mine_too = to_self(j, g, ct)

                    @pl.when(mine_too)
                    def _():
                        dst[zsrc_of(j) % 2, core] = piece

                    @pl.when(jnp.logical_not(mine_too))
                    def _():
                        src[j - WHOLE, ct] = piece
                        f_copy(j, g, ct, part).start()

    def second(lo, hi, g):
        for a, b, whole in split(lo, hi):
            stage = stage_whole if whole else stage_two

            def unit(j, carry, stage=stage):
                pl.when(active(j, g))(lambda: stage(j, g))
                return carry
            lax.fori_loop(a, b, unit, 0)

    def steps_of(zp):
        away = (2 * y + zp - z + 8) % 8
        return jnp.where(away > 4, 8 - away, away)

    with jax.named_scope("a0"):
        for part in range(2):
            place[part].wait()
            to_other[part].wait_recv()
    items(0, 1, 0)
    pl.semaphore_wait(met.at[1], 2)
    tell(4)

    def publish_when_met():
        pl.semaphore_wait(met.at[2], 1)
        publish()
    with jax.named_scope("a1_publish"):
        pl.when(owner == tensor)(publish_when_met)
    with jax.named_scope("a2_ring10"):
        ring(1, 0)

    @pl.when(owner != tensor)
    def _():
        pl.semaphore_wait(met.at[2], 1)
    with jax.named_scope("a3_ring11"):
        ring(1, 1)
    items(1, 3, 0)
    with jax.named_scope("a4_far0"):
        to_far[0].wait_recv()
    relay[0].start()
    with jax.named_scope("a5_ring20"):
        ring(2, 0)
    with jax.named_scope("a6_relay0"):
        relay[0].wait_recv()
    items(0, 3, 1, (0,))
    with jax.named_scope("a8_ring21"):
        ring(2, 1)
    items(3, 5, 0)
    items(3, 5, 1, (0,))
    with jax.named_scope("a9_far1"):
        to_far[1].wait_recv()
    relay[1].start()
    with jax.named_scope("aa_receive"):
        receive()
    backward()
    with jax.named_scope("aa_second"):
        second(0, 3, 0)
    with jax.named_scope("ab_relay1"):
        relay[1].wait_recv()
    items(0, 5, 1, (1,))
    with jax.named_scope("ac_ring30"):
        ring(3, 0)
    with jax.named_scope("b1_ring31"):
        ring(3, 1)
    with jax.named_scope("b2_items"):
        items_both(5, 7)
    with jax.named_scope("b5_last"):
        w_copy(0, 4, 0).wait_recv()
        w_copy(1, 4, 1).wait_recv()
    with jax.named_scope("b6_items"):
        items_both(7, 8)
    with jax.named_scope("b7_second"):
        second(3, 5, 0)
    with jax.named_scope("b8_grads"):
        gradients()
    with jax.named_scope("b9_second"):
        second(0, 5, 1)
    with jax.named_scope("ba_second"):
        second(5, 7, 0)
        second(5, 7, 1)
    with jax.named_scope("bb_second"):
        second(7, 8, 0)
        second(7, 8, 1)

    def finish(i, carry):
        zp = jnp.where(steps_of(0) <= steps_of(1), i, 1 - i)
        away = jnp.where(x_lo == x_hi, 0, 1)
        whole = steps_of(zp) >= FAR

        @pl.when(jnp.logical_not(whole))
        def _():
            for cs in range(2):
                for xl in range(2):
                    frm = summer_at(y, away, cs)
                    own_part = jnp.logical_and(jnp.logical_and(x_lo == x_hi, xl == x_lo),
                                               jnp.logical_and(frm == y, core == cs))

                    @pl.when(jnp.logical_not(own_part))
                    def _():
                        remote(turned.at[0, 0], halves.at[xl, zp, cs], x_send.at[0, 0], x_recv.at[xl, zp, cs],
                               dp, tensor).wait_recv()
                flat[cs * COLS:(cs + 1) * COLS, :] = halves[0, zp, cs].astype(F32) + halves[1, zp, cs].astype(F32)

        @pl.when(whole)
        def _():
            for cs in range(2):
                for part in range(2):
                    frm = summer_at(y, away, cs)
                    own_part = jnp.logical_and(jnp.logical_and(x_lo == x_hi, (part + away) % 2 == x_lo),
                                               jnp.logical_and(frm == y, core == cs))
                    src, dst = ((turned_a, whole_a), (turned_b, whole_b))[part]

                    @pl.when(jnp.logical_not(own_part))
                    def _():
                        remote(src.at[0, 0], dst.at[zp, cs], f_send.at[0, 0], f_recv.at[zp, cs, part],
                               dp, tensor).wait_recv()
                flat[cs * COLS:(cs + 1) * COLS, 0:FIRST] = whole_a[zp, cs].astype(F32)
                flat[cs * COLS:(cs + 1) * COLS, FIRST:TOK] = whole_b[zp, cs].astype(F32)
        pre = extra[zp] + flat[...].T
        sums[zp] = jnp.sum(cots[zp] * pre, axis=0, keepdims=True) / norms[zp]
        results[zp] = pre * scales[zp]
        return carry
    with jax.named_scope("c0_finish"):
        lax.fori_loop(0, 2, finish, 0)
    for i in range(32):
        mag_out[i, :, 0:18] = sums[i // 16][:, 18 * (i % 16):18 * (i % 16 + 1)]

    def mag_copy(i):
        to = (dp + i) % 32
        return remote(mag_out.at[to], mag_in.at[dp], g_send.at[i], g_recv.at[dp], to, tensor)

    def mag_start(i, carry):
        mag_copy(i).start()
        return carry
    with jax.named_scope("c1_mag"):
        lax.fori_loop(1, 32, mag_start, 0)
    with jax.named_scope("c2_plane"):
        sum_plane()
    with jax.named_scope("c2_mixed"):
        for zp in range(2):
            mixed_ref[:, HALF * zp:HALF * (zp + 1)] = results[zp].astype(BF)
    with jax.named_scope("c4_planes"):
        sum_planes()

    for k in (1, 2, 3, 4):
        for side in (0, 1):
            for ch in (0, 1):
                if k < 4 or ch == side:
                    w_copy(side, k, ch).wait_send()
    @pl.when(owner != tensor)
    def _():
        sq_copy.wait_send()

    @pl.when(owner == tensor)
    def _():
        def sent(i, carry):
            msg_copy(i).wait_send()
            return carry
        lax.fori_loop(1, 32, sent, 0)
    over_tensor(low_out, low_in, l_send, l_recv, "send")
    over_tensor(back_out, back_in, b_send, b_recv, "send")
    for i in range(1, 4):
        spread_copy(i).wait_send()

    def plane_sent(i, carry):
        plane_copy(i).wait_send()
        return carry
    lax.fori_loop(1, 8, plane_sent, 0)
    for copies in (to_other, to_far, relay):
        for part in range(2):
            copies[part].wait_send()
    def drain(j, carry):
        for g in range(2):
            @pl.when(jnp.logical_not(local(j, g)))
            def _():
                for part in range(2):
                    y_copy(j, g, part).wait_send()
            for ct in range(2):
                @pl.when(jnp.logical_and(active(j, g), jnp.logical_not(to_self(j, g, ct))))
                def _():
                    x_copy(j, g, ct).wait_send()
        return carry
    lax.fori_loop(0, WHOLE, drain, 0)

    def drain_whole(j, carry):
        for g in range(2):
            for part in range(2):
                @pl.when(jnp.logical_not(local_whole(j, g, part)))
                def _():
                    e_copy(j, g, part).wait_send()
                for ct in range(2):
                    @pl.when(jnp.logical_and(local_whole(j, g, part), jnp.logical_not(to_self(j, g, ct))))
                    def _():
                        f_copy(j, g, ct, part).wait_send()
        return carry
    lax.fori_loop(WHOLE, 8, drain_whole, 0)

    def mag_arrive(i, total):
        frm = (dp + i) % 32
        remote(mag_out.at[0], mag_in.at[frm], g_send.at[0], g_recv.at[frm], dp, tensor).wait_recv()
        return total + mag_in[frm]
    with jax.named_scope("c5_gmag"):
        gmag_ref[...] = lax.fori_loop(1, 32, mag_arrive, mag_out[dp])

    def mag_sent(i, carry):
        mag_copy(i).wait_send()
        return carry
    lax.fori_loop(1, 32, mag_sent, 0)


def body(hidden, weight, factor_b, factor_a, magnitude, cotangent):
    hbm_spec, vmem_spec = pl.BlockSpec(memory_space=pltpu.HBM), pl.BlockSpec(memory_space=pltpu.VMEM)
    dma, vmem = pltpu.SemaphoreType.DMA, pltpu.VMEM
    mixed, grads, gmag = pl.pallas_call(
        kernel,
        name="dora",
        out_shape=(jax.ShapeDtypeStruct((TOK, OUT), BF), jax.ShapeDtypeStruct((16, 128), F32),
                   jax.ShapeDtypeStruct((1, 128), F32)),
        in_specs=[hbm_spec] * 6,
        out_specs=(vmem_spec,) * 3,
        scratch_shapes=[
            vmem((16, HID), BF), vmem((16, COLS), BF), vmem((OUT,), F32), vmem((TOK, OUT), BF), vmem((TOK, HID), BF),
            vmem((2, 2 * TOK, HID), BF),
            vmem((8, COLS, HID), BF),
            vmem((8, 2, COLS, 2 * TOK), BF),
            vmem((WHOLE, 4, COLS, 2 * TOK), BF),
            vmem((WHOLE, 2, COLS, TOK), BF),
            vmem((2, 2, 2, COLS, TOK), BF),
            vmem((8, COLS), F32), vmem((8, 8, COLS), F32),
            vmem((16, 256), F32), vmem((16, 256), BF), vmem((4, 16, 256), BF),
            vmem((2, 16, HALF), F32), vmem((2, 1, HALF), F32), vmem((2, 1, HALF), F32), vmem((2, 1, HALF), F32),
            vmem((8, 16, TOK), F32), vmem((8, 16, TOK), F32), vmem((16, TOK), F32), vmem((16, TOK), F32),
            vmem((2, TOK, HALF), BF), vmem((2, TOK, HALF), F32), vmem((2, TOK, HALF), F32),
            vmem((4, 8, 16, 128), F32), vmem((4, 8, 16, 128), F32),
            vmem((8, 16, 128), F32), vmem((8, 16, 128), F32),
            vmem((32, 1, 128), F32), vmem((32, 1, 128), F32), vmem((2, 1, HALF), F32), vmem((2, TOK, HALF), F32),
            dma((8,)), dma((2, 4, 2)), dma((8, 2)), dma((3, 2)), dma((3, 2)),
            dma((8, 2, 2)), dma((8, 4, 2)), dma((8, 2)), dma((2, 2, 2)),
            dma((1,)), dma((8,)), dma((32,)), dma((4,)), dma((8,)), dma((8,)), dma((8,)), dma((8,)),
            dma((4,)), dma((4,)), dma((8,)), dma((8,)), dma((32,)), dma((32,)),
            vmem((max(8 - WHOLE, 1), 8, COLS, 2 * FIRST), BF),
            vmem((max(8 - WHOLE, 1), 2, COLS, FIRST), BF), vmem((max(8 - WHOLE, 1), 2, COLS, LAST), BF),
            vmem((2, 2, COLS, FIRST), BF), vmem((2, 2, COLS, LAST), BF), vmem((2 * COLS, TOK), F32),
            dma((8, 8)), dma((8, 2)), dma((2, 2, 2)), pltpu.SemaphoreType.REGULAR((3,)),
        ],
        compiler_params=pltpu.CompilerParams(
            collective_id=0, has_side_effects=True, vmem_limit_bytes=67043328
        ),
    )(hidden, weight.T, factor_b.T, factor_a, magnitude, cotangent)
    return mixed, gmag[0, :18], grads[:, 72:90], grads[:, :72].T


def solution(mesh):
    return jax.shard_map(
        body,
        mesh=mesh,
        in_specs=(
            P("dp", "tensor"),
            P("tensor", "dp"),
            P("tensor", None),
            P(None, "dp"),
            P("tensor"),
            P("dp", "tensor"),
        ),
        out_specs=(
            P("dp", "tensor"),
            P(("tensor", "dp")),
            P(None, ("tensor", "dp")),
            P(("tensor", "dp"), None),
        ),
        check_vma=False,
    )
```

```python
import functools

import jax
import jax.numpy as jnp
from jax import lax
from jax.experimental import pallas as pl
from jax.experimental.pallas import tpu as pltpu
from jax.sharding import PartitionSpec as P

TOK, HID, COLS, OUT, HALF = 320, 2304, 144, 576, 288
MESH = pl.DeviceIdType.MESH
F32, BF = jnp.float32, jnp.bfloat16
CHUNKS = ((0, 80), (80, 64))
FIRST, LAST = 192, 128
PARTS = ((0, 2 * FIRST), (2 * FIRST, 2 * LAST))


def remote(src, dst, send, recv, dp, tensor):
    return pltpu.make_async_remote_copy(
        src_ref=src, dst_ref=dst, send_sem=send, recv_sem=recv,
        device_id=(dp, tensor), device_id_type=MESH,
    )


def kernel(h_ref, w_ref, b_hbm, a_hbm, mag_hbm, cot_hbm, mixed_ref, grads_ref, gmag_ref,
           b_ref, a_ref, mag_ref, cot_ref, own, toks, wts, outgoing, arrived, turned, halves,
           sq_out, sq_in, msg_f, msg, msgs, a_all, sq_all, norms, scales, low_in, back_in, low_out, back_out,
           dpre, extra, cots,
           spread, spread_in, plane, plane_in, mag_out, mag_in, sums, results,
           loc_sem, w_send, w_recv, t_send, t_recv, y_send, y_recv, x_send, x_recv,
           s_send, s_recv, m_send, m_recv, l_send, l_recv, b_send, b_recv, d_send, d_recv, p_send, p_recv,
           g_send, g_recv,
           met):
    dp, tensor = lax.axis_index("dp"), lax.axis_index("tensor")
    x_hi, z, core = dp // 16, (dp // 2) % 8, dp % 2
    x_lo, y = tensor // 4, tensor % 4
    other = 1 - core

    def dp_of(a, b, c):
        return a * 16 + b * 2 + c

    def rows(part, of):
        if part == 0:
            return pl.ds(of * FIRST, FIRST), pl.ds(0, FIRST)
        return pl.ds(2 * FIRST + of * LAST, LAST), pl.ds(FIRST, LAST)

    load_h = pltpu.make_async_copy(h_ref, own, loc_sem.at[0])
    place = []
    for part in range(2):
        there, here = rows(part, core)
        place.append(pltpu.make_async_copy(h_ref.at[here], toks.at[0, there], loc_sem.at[6 + part]))
    load_w = pltpu.make_async_copy(w_ref, wts.at[0], loc_sem.at[1])
    loads = [pltpu.make_async_copy(src, dst, loc_sem.at[2 + i]) for i, (src, dst) in enumerate(
        ((a_hbm, a_ref), (b_hbm, b_ref), (mag_hbm, mag_ref), (cot_hbm, cot_ref)))]
    load_w.start()
    loads[0].start()
    loads[1].start()
    load_h.start()
    place[0].start()
    place[1].start()
    loads[2].start()
    loads[3].start()

    barrier = pltpu.get_barrier_semaphore()

    def greet(p):
        pl.semaphore_signal(barrier, inc=1, device_id=p, device_id_type=MESH)

    near = [(dp, (tensor + k) % 8) for k in range(1, 8)]
    near += [(dp_of(x_hi, (z + 1) % 8, core), tensor), (dp_of(x_hi, (z + 7) % 8, core), tensor),
             (dp_of(x_hi, z, other), tensor), (dp_of(1 - x_hi, z, core), tensor), (dp_of(1 - x_hi, z, other), tensor)]
    for p in near:
        greet(p)
    spread[...] = jnp.zeros_like(spread)
    msg_f[...] = jnp.zeros_like(msg_f)
    load_w.wait()
    load_h.wait()
    with jax.named_scope('barrier_wait'):
        pl.semaphore_wait(barrier, len(near))

    def tell(k):
        for to in ((z + k) % 8, (z + 8 - k) % 8)[:1 if k == 4 else 2]:
            pl.semaphore_signal(met.at[k // 2], inc=1, device_id=(dp_of(x_hi, to, core), tensor), device_id_type=MESH)

    tell(1)

    def w_copy(side, k, ch):
        at, n = CHUNKS[ch]
        src = 0 if k == 1 else 2 * (k - 1) - 1 + side
        dst = 7 if k == 4 else 2 * k - 1 + side
        to = (z + 1) % 8 if side == 0 else (z + 7) % 8
        return remote(wts.at[src, pl.ds(at, n)], wts.at[dst, pl.ds(at, n)],
                      w_send.at[side, k - 1, ch], w_recv.at[dst, ch], dp_of(x_hi, to, core), tensor)

    w_copy(0, 1, 0).start()
    w_copy(1, 1, 1).start()
    w_copy(0, 1, 1).start()
    w_copy(1, 1, 0).start()
    to_other, to_far, relay = [], [], []
    for part in range(2):
        there, here = rows(part, core)
        to_other.append(remote(own.at[here], toks.at[0, there], t_send.at[0, part], t_recv.at[0, part],
                               dp_of(x_hi, z, other), tensor))
        to_far.append(remote(own.at[here], toks.at[1, there], t_send.at[1, part], t_recv.at[1, part],
                             dp_of(1 - x_hi, z, core), tensor))
        relay.append(remote(toks.at[1, there], toks.at[1, there], t_send.at[2, part], t_recv.at[2, part],
                            dp_of(x_hi, z, other), tensor))

    to_other[0].start()
    to_other[1].start()

    owner = dp // 4
    loads[0].wait()
    loads[1].wait()
    merged = wts[0].astype(F32) + lax.dot_general(
        a_ref[...], b_ref[...], (((0,), (0,)), ((), ())), preferred_element_type=F32)
    squares = merged * merged
    lanes = squares[:, 0:128]
    for i in range(1, 18):
        lanes = lanes + squares[:, 128 * i:128 * (i + 1)]
    own_sq = jnp.sum(lanes.T, axis=0, keepdims=True)
    sq_row = jnp.broadcast_to(own_sq, (8, COLS))

    @pl.when(owner == tensor)
    def _():
        sq_in[tensor] = sq_row

    @pl.when(owner != tensor)
    def _():
        sq_out[...] = sq_row

    low_part = lax.dot_general(b_ref[...], own[...], (((1,), (1,)), ((), ())), preferred_element_type=F32)
    low_out[...] = low_part
    low_in[tensor] = low_part
    sq_copy = remote(sq_out, sq_in.at[tensor], s_send.at[0], s_recv.at[tensor], dp, owner)

    @pl.when(owner != tensor)
    def _():
        sq_copy.start()

    def over_tensor(src, dst, send, recv, act):
        def body(i, carry):
            to = (tensor + i) % 8
            if act == "recv":
                remote(src, dst.at[to], send.at[i], recv.at[to], dp, to).wait_recv()
            elif act == "start":
                remote(src, dst.at[tensor], send.at[i], recv.at[tensor], dp, to).start()
            else:
                remote(src, dst.at[tensor], send.at[i], recv.at[tensor], dp, to).wait_send()
            return carry
        lax.fori_loop(1, 8, body, 0)

    over_tensor(low_out, low_in, l_send, l_recv, "start")
    to_far[0].start()
    to_far[1].start()

    pl.semaphore_wait(met.at[0], 2)
    tell(2)
    loads[2].wait()
    loads[3].wait()

    def zsrc_of(j):
        k = (j + 1) // 2
        return (z + 8 + k - 2 * k * (j % 2)) % 8

    def summer_at(owner_y, g, of):
        return (owner_y + jnp.where(g == 0, 3 - 2 * of, 2 * of)) % 4

    def summer(j, g):
        return summer_at(zsrc_of(j) // 2, g, core)

    def y_copy(j, g, part):
        lanes = pl.ds(*PARTS[part])
        return remote(outgoing.at[j, g, :, lanes], arrived.at[j, y, :, lanes], y_send.at[j, g, part],
                      y_recv.at[j, y, part], dp, x_lo * 4 + summer(j, g))

    def local(j, g):
        return summer(j, g) == y

    def item(j, g, parts):
        lo, hi = PARTS[parts[0]][0], sum(PARTS[parts[-1]])
        p = lax.dot_general(toks[g, lo:hi], wts[j], (((1,), (1,)), ((), ())), preferred_element_type=F32)
        p = p.T.astype(BF)
        here = local(j, g)

        @pl.when(here)
        def _():
            arrived[j, y, :, lo:hi] = p

        @pl.when(jnp.logical_not(here))
        def _():
            outgoing[j, g, :, lo:hi] = p
            for part in parts:
                y_copy(j, g, part).start()

    def items(lo, hi, g, parts=(0, 1)):
        def body(j, carry):
            item(j, g, parts)
            return carry
        lax.fori_loop(lo, hi, body, 0)

    def items_both(lo, hi):
        def body(i, carry):
            item(lo + i // 2, i % 2, (0, 1))
            return carry
        lax.fori_loop(0, 2 * (hi - lo), body, 0)

    def msg_copy(i):
        return remote(msg, msgs.at[dp % 4], m_send.at[i], m_recv.at[dp % 4], (dp + i) % 32, tensor)

    def publish():
        def arrive(i, carry):
            frm = (tensor + i) % 8
            remote(sq_out, sq_in.at[frm], s_send.at[0], s_recv.at[frm], dp, frm).wait_recv()
            return carry
        lax.fori_loop(1, 8, arrive, 0)
        total = sq_in[0]
        for i in range(1, 8):
            total = total + sq_in[i]
        total = total[0:1]
        high = total.astype(BF).astype(F32)
        rest = total - high
        msg_f[:, 0:COLS] = a_ref[...].astype(F32)
        for i in range(3):
            msg_f[i:i + 1, 144:192] = high[:, 48 * i:48 * (i + 1)]
            msg_f[3 + i:4 + i, 144:192] = rest[:, 48 * i:48 * (i + 1)]
        packed = msg_f[...].astype(BF)
        msg[...] = packed
        msgs[dp % 4] = packed

        def send(i, carry):
            msg_copy(i).start()
            return carry
        lax.fori_loop(1, 32, send, 0)

    def receive():
        for j in range(4):
            @pl.when(dp != tensor * 4 + j)
            def _():
                remote(msg, msgs.at[j], m_send.at[0], m_recv.at[j], dp, tensor).wait_recv()
        for j in range(4):
            m = msgs[j].astype(F32)
            zp, at = j // 2, COLS * (j % 2)
            a_all[zp, :, at:at + COLS] = m[:, 0:COLS]
            for i in range(3):
                sq_all[zp, :, at + 48 * i:at + 48 * (i + 1)] = m[i:i + 1, 144:192] + m[3 + i:4 + i, 144:192]

    def backward():
        back = None
        mags = mag_ref[...].reshape(1, OUT)
        for zp in range(2):
            norm = jnp.sqrt(sq_all[zp] + 1e-6)
            scale = mags[:, HALF * zp:HALF * (zp + 1)] / norm
            norms[zp] = norm
            scales[zp] = scale
            cot = cot_ref[:, HALF * zp:HALF * (zp + 1)].astype(F32)
            cots[zp] = cot
            d = (cot * scale).astype(BF)
            dpre[zp] = d
            part = lax.dot_general(a_all[zp].astype(BF), d, (((1,), (1,)), ((), ())), preferred_element_type=F32)
            back = part if back is None else back + part
        back_out[...] = back
        back_in[tensor] = back
        over_tensor(back_out, back_in, b_send, b_recv, "start")

    group = x_hi * 2 + core

    def spread_copy(i):
        to = (group + i) % 4
        return remote(spread.at[to], spread_in.at[group], d_send.at[i], d_recv.at[group],
                      dp_of(to // 2, z, to % 2), tensor)

    def gradients():
        over_tensor(low_out, low_in, l_send, l_recv, "recv")
        over_tensor(back_out, back_in, b_send, b_recv, "recv")
        low, back = low_in[0], back_in[0]
        for i in range(1, 8):
            low = low + low_in[i]
            back = back + back_in[i]
        low, back = low.astype(BF), back.astype(BF)
        grad_b = jnp.dot(back, own[...], preferred_element_type=F32)
        grad_a = [jnp.dot(low, dpre[zp], preferred_element_type=F32) for zp in range(2)]
        for x in range(2):
            for zz in range(8):
                for c in range(2):
                    i = x * 16 + zz * 2 + c
                    spread[x * 2 + c, zz, :, 0:72] = grad_b[:, 72 * i:72 * (i + 1)]
                    spread[x * 2 + c, zz, :, 72:90] = grad_a[x][:, 18 * (i % 16):18 * (i % 16 + 1)]
        for i in range(1, 4):
            spread_copy(i).start()
        for zp in range(2):
            extra[zp] = lax.dot_general(low, a_all[zp].astype(BF), (((0,), (0,)), ((), ())),
                                        preferred_element_type=F32)

    def plane_copy(i):
        to = (z + i) % 8
        return remote(plane.at[to], plane_in.at[z], p_send.at[i], p_recv.at[z], dp_of(x_hi, to, core), tensor)

    def sum_plane():
        total = spread[group]
        for i in range(1, 4):
            frm = (group + i) % 4
            remote(spread.at[0], spread_in.at[frm], d_send.at[0], d_recv.at[frm], dp, tensor).wait_recv()
            total = total + spread_in[frm]
        plane[...] = total

        def send(i, carry):
            plane_copy(i).start()
            return carry
        lax.fori_loop(1, 8, send, 0)

    def sum_planes():
        total = plane[z]
        for i in range(1, 8):
            frm = (z + i) % 8
            remote(plane.at[0], plane_in.at[frm], p_send.at[0], p_recv.at[frm], dp, tensor).wait_recv()
            total = total + plane_in[frm]
        grads_ref[...] = total

    def ring(k, first):
        for side in (0, 1):
            ch = first if side == 0 else 1 - first
            w_copy(side, k, ch).wait_recv()
            if k < 3 or first == 0:
                w_copy(side, k + 1, ch).start()

    def x_copy(j, g, ct):
        zs = zsrc_of(j)
        tok_hi = jnp.where(g == 0, x_hi, 1 - x_hi)
        return remote(turned.at[j, ct], halves.at[x_lo, zs % 2, core], x_send.at[j, ct],
                      x_recv.at[x_lo, zs % 2, core], dp_of(tok_hi, z, ct), x_hi * 4 + zs // 2)

    def to_self(j, g, ct):
        same = jnp.logical_and(g == 0, x_lo == x_hi)
        return jnp.logical_and(same, jnp.logical_and(zsrc_of(j) // 2 == y, core == ct))

    def active(j, g):
        return summer(j, g) == y

    def stage_two(j, g):
        for k in range(1, 4):
            ys = (y + k) % 4
            for part in range(2):
                lanes = pl.ds(*PARTS[part])
                remote(outgoing.at[0, 0, :, lanes], arrived.at[j, ys, :, lanes], y_send.at[0, 0, part],
                       y_recv.at[j, ys, part], dp, tensor).wait_recv()
        total = arrived[j, 0].astype(F32)
        for ys in range(1, 4):
            total = total + arrived[j, ys].astype(F32)
        total = total.astype(BF)
        for ct in range(2):
            part = jnp.concatenate(
                [total[:, ct * FIRST:(ct + 1) * FIRST],
                 total[:, 2 * FIRST + ct * LAST:2 * FIRST + (ct + 1) * LAST]], axis=1)
            mine_too = to_self(j, g, ct)

            @pl.when(mine_too)
            def _():
                halves[x_lo, zsrc_of(j) % 2, core] = part

            @pl.when(jnp.logical_not(mine_too))
            def _():
                turned[j, ct] = part
                x_copy(j, g, ct).start()

    def second(lo, hi, g):
        def unit(j, carry):
            pl.when(active(j, g))(lambda: stage_two(j, g))
            return carry
        lax.fori_loop(lo, hi, unit, 0)

    def steps_of(zp):
        away = (2 * y + zp - z + 8) % 8
        return jnp.where(away > 4, 8 - away, away)

    with jax.named_scope("a0"):
        for part in range(2):
            place[part].wait()
            to_other[part].wait_recv()
    items(0, 1, 0)
    pl.semaphore_wait(met.at[1], 2)
    tell(4)

    def publish_when_met():
        pl.semaphore_wait(met.at[2], 1)
        publish()
    with jax.named_scope("a1_publish"):
        pl.when(owner == tensor)(publish_when_met)
    with jax.named_scope("a2_ring10"):
        ring(1, 0)

    @pl.when(owner != tensor)
    def _():
        pl.semaphore_wait(met.at[2], 1)
    with jax.named_scope("a3_ring11"):
        ring(1, 1)
    items(1, 3, 0)
    with jax.named_scope("a4_far0"):
        to_far[0].wait_recv()
    relay[0].start()
    with jax.named_scope("a5_ring20"):
        ring(2, 0)
    with jax.named_scope("a6_relay0"):
        relay[0].wait_recv()
    items(0, 3, 1, (0,))
    with jax.named_scope("a8_ring21"):
        ring(2, 1)
    items(3, 5, 0)
    items(3, 5, 1, (0,))
    with jax.named_scope("a9_far1"):
        to_far[1].wait_recv()
    relay[1].start()
    with jax.named_scope("aa_receive"):
        receive()
    backward()
    with jax.named_scope("aa_second"):
        second(0, 3, 0)
    with jax.named_scope("ab_relay1"):
        relay[1].wait_recv()
    items(0, 5, 1, (1,))
    with jax.named_scope("ac_ring30"):
        ring(3, 0)
    with jax.named_scope("b1_ring31"):
        ring(3, 1)
    with jax.named_scope("b2_items"):
        items_both(5, 7)
    with jax.named_scope("b5_last"):
        w_copy(0, 4, 0).wait_recv()
        w_copy(1, 4, 1).wait_recv()
    with jax.named_scope("b6_items"):
        items_both(7, 8)
    with jax.named_scope("b7_second"):
        second(3, 5, 0)
    with jax.named_scope("b8_grads"):
        gradients()
    with jax.named_scope("b9_second"):
        second(0, 5, 1)
    with jax.named_scope("ba_second"):
        second(5, 7, 0)
        second(5, 7, 1)
    with jax.named_scope("bb_second"):
        second(7, 8, 0)
        second(7, 8, 1)

    def finish(i, carry):
        zp = jnp.where(steps_of(0) <= steps_of(1), i, 1 - i)
        away = jnp.where(x_lo == x_hi, 0, 1)
        parts = []
        for cs in range(2):
            for xl in range(2):
                frm = summer_at(y, away, cs)
                own_part = jnp.logical_and(jnp.logical_and(x_lo == x_hi, xl == x_lo),
                                           jnp.logical_and(frm == y, core == cs))

                @pl.when(jnp.logical_not(own_part))
                def _():
                    remote(turned.at[0, 0], halves.at[xl, zp, cs], x_send.at[0, 0], x_recv.at[xl, zp, cs],
                           dp, tensor).wait_recv()
            parts.append(halves[0, zp, cs].astype(F32) + halves[1, zp, cs].astype(F32))
        pre = extra[zp] + jnp.concatenate(parts, axis=0).T
        sums[zp] = jnp.sum(cots[zp] * pre, axis=0, keepdims=True) / norms[zp]
        results[zp] = pre * scales[zp]
        return carry
    with jax.named_scope("c0_finish"):
        lax.fori_loop(0, 2, finish, 0)
    for i in range(32):
        mag_out[i, :, 0:18] = sums[i // 16][:, 18 * (i % 16):18 * (i % 16 + 1)]

    def mag_copy(i):
        to = (dp + i) % 32
        return remote(mag_out.at[to], mag_in.at[dp], g_send.at[i], g_recv.at[dp], to, tensor)

    def mag_start(i, carry):
        mag_copy(i).start()
        return carry
    with jax.named_scope("c1_mag"):
        lax.fori_loop(1, 32, mag_start, 0)
    with jax.named_scope("c2_plane"):
        sum_plane()
    with jax.named_scope("c2_mixed"):
        for zp in range(2):
            mixed_ref[:, HALF * zp:HALF * (zp + 1)] = results[zp].astype(BF)
    with jax.named_scope("c4_planes"):
        sum_planes()

    for k in (1, 2, 3, 4):
        for side in (0, 1):
            for ch in (0, 1):
                if k < 4 or ch == side:
                    w_copy(side, k, ch).wait_send()
    @pl.when(owner != tensor)
    def _():
        sq_copy.wait_send()

    @pl.when(owner == tensor)
    def _():
        def sent(i, carry):
            msg_copy(i).wait_send()
            return carry
        lax.fori_loop(1, 32, sent, 0)
    over_tensor(low_out, low_in, l_send, l_recv, "send")
    over_tensor(back_out, back_in, b_send, b_recv, "send")
    for i in range(1, 4):
        spread_copy(i).wait_send()

    def plane_sent(i, carry):
        plane_copy(i).wait_send()
        return carry
    lax.fori_loop(1, 8, plane_sent, 0)
    for copies in (to_other, to_far, relay):
        for part in range(2):
            copies[part].wait_send()
    def drain(j, carry):
        for g in range(2):
            @pl.when(jnp.logical_not(local(j, g)))
            def _():
                for part in range(2):
                    y_copy(j, g, part).wait_send()
            for ct in range(2):
                @pl.when(jnp.logical_and(active(j, g), jnp.logical_not(to_self(j, g, ct))))
                def _():
                    x_copy(j, g, ct).wait_send()
        return carry
    lax.fori_loop(0, 8, drain, 0)

    def mag_arrive(i, total):
        frm = (dp + i) % 32
        remote(mag_out.at[0], mag_in.at[frm], g_send.at[0], g_recv.at[frm], dp, tensor).wait_recv()
        return total + mag_in[frm]
    with jax.named_scope("c5_gmag"):
        gmag_ref[...] = lax.fori_loop(1, 32, mag_arrive, mag_out[dp])

    def mag_sent(i, carry):
        mag_copy(i).wait_send()
        return carry
    lax.fori_loop(1, 32, mag_sent, 0)


def body(hidden, weight, factor_b, factor_a, magnitude, cotangent):
    hbm_spec, vmem_spec = pl.BlockSpec(memory_space=pltpu.HBM), pl.BlockSpec(memory_space=pltpu.VMEM)
    dma, vmem = pltpu.SemaphoreType.DMA, pltpu.VMEM
    mixed, grads, gmag = pl.pallas_call(
        kernel,
        name="dora",
        out_shape=(jax.ShapeDtypeStruct((TOK, OUT), BF), jax.ShapeDtypeStruct((16, 128), F32),
                   jax.ShapeDtypeStruct((1, 128), F32)),
        in_specs=[hbm_spec] * 6,
        out_specs=(vmem_spec,) * 3,
        scratch_shapes=[
            vmem((16, HID), BF), vmem((16, COLS), BF), vmem((OUT,), F32), vmem((TOK, OUT), BF), vmem((TOK, HID), BF),
            vmem((2, 2 * TOK, HID), BF),
            vmem((8, COLS, HID), BF),
            vmem((8, 2, COLS, 2 * TOK), BF),
            vmem((8, 4, COLS, 2 * TOK), BF),
            vmem((8, 2, COLS, TOK), BF),
            vmem((2, 2, 2, COLS, TOK), BF),
            vmem((8, COLS), F32), vmem((8, 8, COLS), F32),
            vmem((16, 256), F32), vmem((16, 256), BF), vmem((4, 16, 256), BF),
            vmem((2, 16, HALF), F32), vmem((2, 1, HALF), F32), vmem((2, 1, HALF), F32), vmem((2, 1, HALF), F32),
            vmem((8, 16, TOK), F32), vmem((8, 16, TOK), F32), vmem((16, TOK), F32), vmem((16, TOK), F32),
            vmem((2, TOK, HALF), BF), vmem((2, TOK, HALF), F32), vmem((2, TOK, HALF), F32),
            vmem((4, 8, 16, 128), F32), vmem((4, 8, 16, 128), F32),
            vmem((8, 16, 128), F32), vmem((8, 16, 128), F32),
            vmem((32, 1, 128), F32), vmem((32, 1, 128), F32), vmem((2, 1, HALF), F32), vmem((2, TOK, HALF), F32),
            dma((8,)), dma((2, 4, 2)), dma((8, 2)), dma((3, 2)), dma((3, 2)),
            dma((8, 2, 2)), dma((8, 4, 2)), dma((8, 2)), dma((2, 2, 2)),
            dma((1,)), dma((8,)), dma((32,)), dma((4,)), dma((8,)), dma((8,)), dma((8,)), dma((8,)),
            dma((4,)), dma((4,)), dma((8,)), dma((8,)), dma((32,)), dma((32,)),
            pltpu.SemaphoreType.REGULAR((3,)),
        ],
        compiler_params=pltpu.CompilerParams(
            collective_id=0, has_side_effects=True, vmem_limit_bytes=55779328
        ),
    )(hidden, weight.T, factor_b.T, factor_a, magnitude, cotangent)
    return mixed, gmag[0, :18], grads[:, 72:90], grads[:, :72].T


def solution(mesh):
    return jax.shard_map(
        body,
        mesh=mesh,
        in_specs=(
            P("dp", "tensor"),
            P("tensor", "dp"),
            P("tensor", None),
            P(None, "dp"),
            P("tensor"),
            P("dp", "tensor"),
        ),
        out_specs=(
            P("dp", "tensor"),
            P(("tensor", "dp")),
            P(None, ("tensor", "dp")),
            P(("tensor", "dp"), None),
        ),
        check_vma=False,
    )
```

```python
import functools

import jax
import jax.numpy as jnp
from jax import lax
from jax.experimental import pallas as pl
from jax.experimental.pallas import tpu as pltpu
from jax.sharding import PartitionSpec as P

TOK, HID, COLS, OUT, HALF = 320, 2304, 144, 576, 288
MESH = pl.DeviceIdType.MESH
F32, BF = jnp.float32, jnp.bfloat16
CHUNKS = ((0, 80), (80, 64))
FIRST, LAST = 192, 128
PARTS = ((0, 2 * FIRST), (2 * FIRST, 2 * LAST))


def remote(src, dst, send, recv, dp, tensor):
    return pltpu.make_async_remote_copy(
        src_ref=src, dst_ref=dst, send_sem=send, recv_sem=recv,
        device_id=(dp, tensor), device_id_type=MESH,
    )


def kernel(h_ref, w_ref, b_hbm, a_hbm, mag_hbm, cot_hbm, mixed_ref, grads_ref, gmag_ref,
           b_ref, a_ref, mag_ref, cot_ref, own, toks, wts, outgoing, arrived, turned, halves,
           sq_out, sq_in, msg_f, msg, msgs, a_all, sq_all, norms, scales, low_in, back_in, low_out, back_out,
           dpre, extra, cots,
           spread, spread_in, plane, plane_in, mag_out, mag_in, sums, results,
           loc_sem, w_send, w_recv, t_send, t_recv, y_send, y_recv, x_send, x_recv,
           s_send, s_recv, m_send, m_recv, l_send, l_recv, b_send, b_recv, d_send, d_recv, p_send, p_recv,
           g_send, g_recv,
           met):
    dp, tensor = lax.axis_index("dp"), lax.axis_index("tensor")
    x_hi, z, core = dp // 16, (dp // 2) % 8, dp % 2
    x_lo, y = tensor // 4, tensor % 4
    other = 1 - core

    def dp_of(a, b, c):
        return a * 16 + b * 2 + c

    def rows(part, of):
        if part == 0:
            return pl.ds(of * FIRST, FIRST), pl.ds(0, FIRST)
        return pl.ds(2 * FIRST + of * LAST, LAST), pl.ds(FIRST, LAST)

    load_h = pltpu.make_async_copy(h_ref, own, loc_sem.at[0])
    place = []
    for part in range(2):
        there, here = rows(part, core)
        place.append(pltpu.make_async_copy(h_ref.at[here], toks.at[0, there], loc_sem.at[6 + part]))
    load_w = pltpu.make_async_copy(w_ref, wts.at[0], loc_sem.at[1])
    loads = [pltpu.make_async_copy(src, dst, loc_sem.at[2 + i]) for i, (src, dst) in enumerate(
        ((a_hbm, a_ref), (b_hbm, b_ref), (mag_hbm, mag_ref), (cot_hbm, cot_ref)))]
    load_w.start()
    loads[0].start()
    loads[1].start()
    load_h.start()
    place[0].start()
    place[1].start()
    loads[2].start()
    loads[3].start()

    barrier = pltpu.get_barrier_semaphore()

    def greet(p):
        pl.semaphore_signal(barrier, inc=1, device_id=p, device_id_type=MESH)

    near = [(dp, (tensor + k) % 8) for k in range(1, 8)]
    near += [(dp_of(x_hi, (z + 1) % 8, core), tensor), (dp_of(x_hi, (z + 7) % 8, core), tensor),
             (dp_of(x_hi, z, other), tensor), (dp_of(1 - x_hi, z, core), tensor), (dp_of(1 - x_hi, z, other), tensor)]
    for p in near:
        greet(p)
    spread[...] = jnp.zeros_like(spread)
    msg_f[...] = jnp.zeros_like(msg_f)
    load_w.wait()
    load_h.wait()
    with jax.named_scope('barrier_wait'):
        pl.semaphore_wait(barrier, len(near))

    def tell(k):
        for to in ((z + k) % 8, (z + 8 - k) % 8)[:1 if k == 4 else 2]:
            pl.semaphore_signal(met.at[k // 2], inc=1, device_id=(dp_of(x_hi, to, core), tensor), device_id_type=MESH)

    tell(1)

    def w_copy(side, k, ch):
        at, n = CHUNKS[ch]
        src = 0 if k == 1 else 2 * (k - 1) - 1 + side
        dst = 7 if k == 4 else 2 * k - 1 + side
        to = (z + 1) % 8 if side == 0 else (z + 7) % 8
        return remote(wts.at[src, pl.ds(at, n)], wts.at[dst, pl.ds(at, n)],
                      w_send.at[side, k - 1, ch], w_recv.at[dst, ch], dp_of(x_hi, to, core), tensor)

    w_copy(0, 1, 0).start()
    w_copy(1, 1, 1).start()
    w_copy(0, 1, 1).start()
    w_copy(1, 1, 0).start()
    to_other, to_far, relay = [], [], []
    for part in range(2):
        there, here = rows(part, core)
        to_other.append(remote(own.at[here], toks.at[0, there], t_send.at[0, part], t_recv.at[0, part],
                               dp_of(x_hi, z, other), tensor))
        to_far.append(remote(own.at[here], toks.at[1, there], t_send.at[1, part], t_recv.at[1, part],
                             dp_of(1 - x_hi, z, core), tensor))
        relay.append(remote(toks.at[1, there], toks.at[1, there], t_send.at[2, part], t_recv.at[2, part],
                            dp_of(x_hi, z, other), tensor))

    to_other[0].start()
    to_other[1].start()

    owner = dp // 4
    loads[0].wait()
    loads[1].wait()
    merged = wts[0].astype(F32) + lax.dot_general(
        a_ref[...], b_ref[...], (((0,), (0,)), ((), ())), preferred_element_type=F32)
    squares = merged * merged
    lanes = squares[:, 0:128]
    for i in range(1, 18):
        lanes = lanes + squares[:, 128 * i:128 * (i + 1)]
    own_sq = jnp.sum(lanes.T, axis=0, keepdims=True)
    sq_row = jnp.broadcast_to(own_sq, (8, COLS))

    @pl.when(owner == tensor)
    def _():
        sq_in[tensor] = sq_row

    @pl.when(owner != tensor)
    def _():
        sq_out[...] = sq_row

    low_part = lax.dot_general(b_ref[...], own[...], (((1,), (1,)), ((), ())), preferred_element_type=F32)
    low_out[...] = low_part
    low_in[tensor] = low_part
    sq_copy = remote(sq_out, sq_in.at[tensor], s_send.at[0], s_recv.at[tensor], dp, owner)

    @pl.when(owner != tensor)
    def _():
        sq_copy.start()

    def over_tensor(src, dst, send, recv, act):
        def body(i, carry):
            to = (tensor + i) % 8
            if act == "recv":
                remote(src, dst.at[to], send.at[i], recv.at[to], dp, to).wait_recv()
            elif act == "start":
                remote(src, dst.at[tensor], send.at[i], recv.at[tensor], dp, to).start()
            else:
                remote(src, dst.at[tensor], send.at[i], recv.at[tensor], dp, to).wait_send()
            return carry
        lax.fori_loop(1, 8, body, 0)

    over_tensor(low_out, low_in, l_send, l_recv, "start")
    to_far[0].start()
    to_far[1].start()

    pl.semaphore_wait(met.at[0], 2)
    tell(2)
    loads[2].wait()
    loads[3].wait()

    def zsrc_of(j):
        k = (j + 1) // 2
        return (z + 8 + k - 2 * k * (j % 2)) % 8

    def summer_at(owner_y, g, of):
        return (owner_y + jnp.where(g == 0, 3 - 2 * of, 2 * of)) % 4

    def summer(j, g):
        return summer_at(zsrc_of(j) // 2, g, core)

    def y_copy(j, g, part):
        lanes = pl.ds(*PARTS[part])
        return remote(outgoing.at[j, g, :, lanes], arrived.at[j, y, :, lanes], y_send.at[j, g, part],
                      y_recv.at[j, y, part], dp, x_lo * 4 + summer(j, g))

    def local(j, g):
        return summer(j, g) == y

    def item(j, g, parts):
        lo, hi = PARTS[parts[0]][0], sum(PARTS[parts[-1]])
        p = lax.dot_general(toks[g, lo:hi], wts[j], (((1,), (1,)), ((), ())), preferred_element_type=F32)
        p = p.T.astype(BF)
        here = local(j, g)

        @pl.when(here)
        def _():
            arrived[j, y, :, lo:hi] = p

        @pl.when(jnp.logical_not(here))
        def _():
            outgoing[j, g, :, lo:hi] = p
            for part in parts:
                y_copy(j, g, part).start()

    def items(lo, hi, g, parts=(0, 1)):
        def body(j, carry):
            item(j, g, parts)
            return carry
        lax.fori_loop(lo, hi, body, 0)

    def items_both(lo, hi):
        def body(i, carry):
            item(lo + i // 2, i % 2, (0, 1))
            return carry
        lax.fori_loop(0, 2 * (hi - lo), body, 0)

    def msg_copy(i):
        return remote(msg, msgs.at[dp % 4], m_send.at[i], m_recv.at[dp % 4], (dp + i) % 32, tensor)

    def publish():
        def arrive(i, carry):
            frm = (tensor + i) % 8
            remote(sq_out, sq_in.at[frm], s_send.at[0], s_recv.at[frm], dp, frm).wait_recv()
            return carry
        lax.fori_loop(1, 8, arrive, 0)
        total = sq_in[0]
        for i in range(1, 8):
            total = total + sq_in[i]
        total = total[0:1]
        high = total.astype(BF).astype(F32)
        rest = total - high
        msg_f[:, 0:COLS] = a_ref[...].astype(F32)
        for i in range(3):
            msg_f[i:i + 1, 144:192] = high[:, 48 * i:48 * (i + 1)]
            msg_f[3 + i:4 + i, 144:192] = rest[:, 48 * i:48 * (i + 1)]
        packed = msg_f[...].astype(BF)
        msg[...] = packed
        msgs[dp % 4] = packed

        def send(i, carry):
            msg_copy(i).start()
            return carry
        lax.fori_loop(1, 32, send, 0)

    def receive():
        for j in range(4):
            @pl.when(dp != tensor * 4 + j)
            def _():
                remote(msg, msgs.at[j], m_send.at[0], m_recv.at[j], dp, tensor).wait_recv()
        for j in range(4):
            m = msgs[j].astype(F32)
            zp, at = j // 2, COLS * (j % 2)
            a_all[zp, :, at:at + COLS] = m[:, 0:COLS]
            for i in range(3):
                sq_all[zp, :, at + 48 * i:at + 48 * (i + 1)] = m[i:i + 1, 144:192] + m[3 + i:4 + i, 144:192]

    def backward():
        back = None
        mags = mag_ref[...].reshape(1, OUT)
        for zp in range(2):
            norm = jnp.sqrt(sq_all[zp] + 1e-6)
            scale = mags[:, HALF * zp:HALF * (zp + 1)] / norm
            norms[zp] = norm
            scales[zp] = scale
            cot = cot_ref[:, HALF * zp:HALF * (zp + 1)].astype(F32)
            cots[zp] = cot
            d = (cot * scale).astype(BF)
            dpre[zp] = d
            part = lax.dot_general(a_all[zp].astype(BF), d, (((1,), (1,)), ((), ())), preferred_element_type=F32)
            back = part if back is None else back + part
        back_out[...] = back
        back_in[tensor] = back
        over_tensor(back_out, back_in, b_send, b_recv, "start")

    group = x_hi * 2 + core

    def spread_copy(i):
        to = (group + i) % 4
        return remote(spread.at[to], spread_in.at[group], d_send.at[i], d_recv.at[group],
                      dp_of(to // 2, z, to % 2), tensor)

    def gradients():
        over_tensor(low_out, low_in, l_send, l_recv, "recv")
        over_tensor(back_out, back_in, b_send, b_recv, "recv")
        low, back = low_in[0], back_in[0]
        for i in range(1, 8):
            low = low + low_in[i]
            back = back + back_in[i]
        low, back = low.astype(BF), back.astype(BF)
        grad_b = jnp.dot(back, own[...], preferred_element_type=F32)
        grad_a = [jnp.dot(low, dpre[zp], preferred_element_type=F32) for zp in range(2)]
        for x in range(2):
            for zz in range(8):
                for c in range(2):
                    i = x * 16 + zz * 2 + c
                    spread[x * 2 + c, zz, :, 0:72] = grad_b[:, 72 * i:72 * (i + 1)]
                    spread[x * 2 + c, zz, :, 72:90] = grad_a[x][:, 18 * (i % 16):18 * (i % 16 + 1)]
        for i in range(1, 4):
            spread_copy(i).start()
        for zp in range(2):
            extra[zp] = lax.dot_general(low, a_all[zp].astype(BF), (((0,), (0,)), ((), ())),
                                        preferred_element_type=F32)

    def plane_copy(i):
        to = (z + i) % 8
        return remote(plane.at[to], plane_in.at[z], p_send.at[i], p_recv.at[z], dp_of(x_hi, to, core), tensor)

    def sum_plane():
        total = spread[group]
        for i in range(1, 4):
            frm = (group + i) % 4
            remote(spread.at[0], spread_in.at[frm], d_send.at[0], d_recv.at[frm], dp, tensor).wait_recv()
            total = total + spread_in[frm]
        plane[...] = total

        def send(i, carry):
            plane_copy(i).start()
            return carry
        lax.fori_loop(1, 8, send, 0)

    def sum_planes():
        total = plane[z]
        for i in range(1, 8):
            frm = (z + i) % 8
            remote(plane.at[0], plane_in.at[frm], p_send.at[0], p_recv.at[frm], dp, tensor).wait_recv()
            total = total + plane_in[frm]
        grads_ref[...] = total

    def ring(k, first):
        for side in (0, 1):
            ch = first if side == 0 else 1 - first
            w_copy(side, k, ch).wait_recv()
            if k < 3 or first == 0:
                w_copy(side, k + 1, ch).start()

    def x_copy(j, g, ct):
        zs = zsrc_of(j)
        tok_hi = jnp.where(g == 0, x_hi, 1 - x_hi)
        return remote(turned.at[j, ct], halves.at[x_lo, zs % 2, core], x_send.at[j, ct],
                      x_recv.at[x_lo, zs % 2, core], dp_of(tok_hi, z, ct), x_hi * 4 + zs // 2)

    def to_self(j, g, ct):
        same = jnp.logical_and(g == 0, x_lo == x_hi)
        return jnp.logical_and(same, jnp.logical_and(zsrc_of(j) // 2 == y, core == ct))

    def active(j, g):
        return summer(j, g) == y

    def stage_two(j, g):
        for k in range(1, 4):
            ys = (y + k) % 4
            for part in range(2):
                lanes = pl.ds(*PARTS[part])
                remote(outgoing.at[0, 0, :, lanes], arrived.at[j, ys, :, lanes], y_send.at[0, 0, part],
                       y_recv.at[j, ys, part], dp, tensor).wait_recv()
        total = arrived[j, 0].astype(F32)
        for ys in range(1, 4):
            total = total + arrived[j, ys].astype(F32)
        total = total.astype(BF)
        for ct in range(2):
            part = jnp.concatenate(
                [total[:, ct * FIRST:(ct + 1) * FIRST],
                 total[:, 2 * FIRST + ct * LAST:2 * FIRST + (ct + 1) * LAST]], axis=1)
            mine_too = to_self(j, g, ct)

            @pl.when(mine_too)
            def _():
                halves[x_lo, zsrc_of(j) % 2, core] = part

            @pl.when(jnp.logical_not(mine_too))
            def _():
                turned[j, ct] = part
                x_copy(j, g, ct).start()

    def second(lo, hi, g):
        def unit(j, carry):
            pl.when(active(j, g))(lambda: stage_two(j, g))
            return carry
        lax.fori_loop(lo, hi, unit, 0)

    def steps_of(zp):
        away = (2 * y + zp - z + 8) % 8
        return jnp.where(away > 4, 8 - away, away)

    with jax.named_scope("a0"):
        for part in range(2):
            place[part].wait()
            to_other[part].wait_recv()
    items(0, 1, 0)
    pl.semaphore_wait(met.at[1], 2)
    tell(4)

    def publish_when_met():
        pl.semaphore_wait(met.at[2], 1)
        publish()
    with jax.named_scope("a1_publish"):
        pl.when(owner == tensor)(publish_when_met)
    with jax.named_scope("a2_ring10"):
        ring(1, 0)

    @pl.when(owner != tensor)
    def _():
        pl.semaphore_wait(met.at[2], 1)
    with jax.named_scope("a3_ring11"):
        ring(1, 1)
    items(1, 3, 0)
    with jax.named_scope("a4_far0"):
        to_far[0].wait_recv()
    relay[0].start()
    with jax.named_scope("a5_ring20"):
        ring(2, 0)
    with jax.named_scope("a6_relay0"):
        relay[0].wait_recv()
    items(0, 3, 1, (0,))
    with jax.named_scope("a8_ring21"):
        ring(2, 1)
    items(3, 5, 0)
    items(3, 5, 1, (0,))
    with jax.named_scope("a9_far1"):
        to_far[1].wait_recv()
    relay[1].start()
    with jax.named_scope("aa_receive"):
        receive()
    backward()
    with jax.named_scope("aa_second"):
        second(0, 3, 0)
    with jax.named_scope("ab_relay1"):
        relay[1].wait_recv()
    items(0, 5, 1, (1,))
    with jax.named_scope("ac_ring30"):
        ring(3, 0)
    with jax.named_scope("b1_ring31"):
        ring(3, 1)
    with jax.named_scope("b2_items"):
        items_both(5, 7)
    with jax.named_scope("b3_second"):
        second(3, 5, 0)
    with jax.named_scope("b5_last"):
        w_copy(0, 4, 0).wait_recv()
        w_copy(1, 4, 1).wait_recv()
    with jax.named_scope("b6_items"):
        items_both(7, 8)
    with jax.named_scope("b8_grads"):
        gradients()
    with jax.named_scope("b9_second"):
        second(0, 5, 1)
    with jax.named_scope("ba_second"):
        second(5, 7, 0)
        second(5, 7, 1)
    with jax.named_scope("bb_second"):
        second(7, 8, 0)
        second(7, 8, 1)

    def finish(i, carry):
        zp = jnp.where(steps_of(0) <= steps_of(1), i, 1 - i)
        away = jnp.where(x_lo == x_hi, 0, 1)
        parts = []
        for cs in range(2):
            for xl in range(2):
                frm = summer_at(y, away, cs)
                own_part = jnp.logical_and(jnp.logical_and(x_lo == x_hi, xl == x_lo),
                                           jnp.logical_and(frm == y, core == cs))

                @pl.when(jnp.logical_not(own_part))
                def _():
                    remote(turned.at[0, 0], halves.at[xl, zp, cs], x_send.at[0, 0], x_recv.at[xl, zp, cs],
                           dp, tensor).wait_recv()
            parts.append(halves[0, zp, cs].astype(F32) + halves[1, zp, cs].astype(F32))
        pre = extra[zp] + jnp.concatenate(parts, axis=0).T
        sums[zp] = jnp.sum(cots[zp] * pre, axis=0, keepdims=True) / norms[zp]
        results[zp] = pre * scales[zp]
        return carry
    with jax.named_scope("c0_finish"):
        lax.fori_loop(0, 2, finish, 0)
    for i in range(32):
        mag_out[i, :, 0:18] = sums[i // 16][:, 18 * (i % 16):18 * (i % 16 + 1)]

    def mag_copy(i):
        to = (dp + i) % 32
        return remote(mag_out.at[to], mag_in.at[dp], g_send.at[i], g_recv.at[dp], to, tensor)

    def mag_start(i, carry):
        mag_copy(i).start()
        return carry
    with jax.named_scope("c1_mag"):
        lax.fori_loop(1, 32, mag_start, 0)
    with jax.named_scope("c2_plane"):
        sum_plane()
    with jax.named_scope("c2_mixed"):
        for zp in range(2):
            mixed_ref[:, HALF * zp:HALF * (zp + 1)] = results[zp].astype(BF)
    with jax.named_scope("c4_planes"):
        sum_planes()

    for k in (1, 2, 3, 4):
        for side in (0, 1):
            for ch in (0, 1):
                if k < 4 or ch == side:
                    w_copy(side, k, ch).wait_send()
    @pl.when(owner != tensor)
    def _():
        sq_copy.wait_send()

    @pl.when(owner == tensor)
    def _():
        def sent(i, carry):
            msg_copy(i).wait_send()
            return carry
        lax.fori_loop(1, 32, sent, 0)
    over_tensor(low_out, low_in, l_send, l_recv, "send")
    over_tensor(back_out, back_in, b_send, b_recv, "send")
    for i in range(1, 4):
        spread_copy(i).wait_send()

    def plane_sent(i, carry):
        plane_copy(i).wait_send()
        return carry
    lax.fori_loop(1, 8, plane_sent, 0)
    for copies in (to_other, to_far, relay):
        for part in range(2):
            copies[part].wait_send()
    def drain(j, carry):
        for g in range(2):
            @pl.when(jnp.logical_not(local(j, g)))
            def _():
                for part in range(2):
                    y_copy(j, g, part).wait_send()
            for ct in range(2):
                @pl.when(jnp.logical_and(active(j, g), jnp.logical_not(to_self(j, g, ct))))
                def _():
                    x_copy(j, g, ct).wait_send()
        return carry
    lax.fori_loop(0, 8, drain, 0)

    def mag_arrive(i, total):
        frm = (dp + i) % 32
        remote(mag_out.at[0], mag_in.at[frm], g_send.at[0], g_recv.at[frm], dp, tensor).wait_recv()
        return total + mag_in[frm]
    with jax.named_scope("c5_gmag"):
        gmag_ref[...] = lax.fori_loop(1, 32, mag_arrive, mag_out[dp])

    def mag_sent(i, carry):
        mag_copy(i).wait_send()
        return carry
    lax.fori_loop(1, 32, mag_sent, 0)


def body(hidden, weight, factor_b, factor_a, magnitude, cotangent):
    hbm_spec, vmem_spec = pl.BlockSpec(memory_space=pltpu.HBM), pl.BlockSpec(memory_space=pltpu.VMEM)
    dma, vmem = pltpu.SemaphoreType.DMA, pltpu.VMEM
    mixed, grads, gmag = pl.pallas_call(
        kernel,
        name="dora",
        out_shape=(jax.ShapeDtypeStruct((TOK, OUT), BF), jax.ShapeDtypeStruct((16, 128), F32),
                   jax.ShapeDtypeStruct((1, 128), F32)),
        in_specs=[hbm_spec] * 6,
        out_specs=(vmem_spec,) * 3,
        scratch_shapes=[
            vmem((16, HID), BF), vmem((16, COLS), BF), vmem((OUT,), F32), vmem((TOK, OUT), BF), vmem((TOK, HID), BF),
            vmem((2, 2 * TOK, HID), BF),
            vmem((8, COLS, HID), BF),
            vmem((8, 2, COLS, 2 * TOK), BF),
            vmem((8, 4, COLS, 2 * TOK), BF),
            vmem((8, 2, COLS, TOK), BF),
            vmem((2, 2, 2, COLS, TOK), BF),
            vmem((8, COLS), F32), vmem((8, 8, COLS), F32),
            vmem((16, 256), F32), vmem((16, 256), BF), vmem((4, 16, 256), BF),
            vmem((2, 16, HALF), F32), vmem((2, 1, HALF), F32), vmem((2, 1, HALF), F32), vmem((2, 1, HALF), F32),
            vmem((8, 16, TOK), F32), vmem((8, 16, TOK), F32), vmem((16, TOK), F32), vmem((16, TOK), F32),
            vmem((2, TOK, HALF), BF), vmem((2, TOK, HALF), F32), vmem((2, TOK, HALF), F32),
            vmem((4, 8, 16, 128), F32), vmem((4, 8, 16, 128), F32),
            vmem((8, 16, 128), F32), vmem((8, 16, 128), F32),
            vmem((32, 1, 128), F32), vmem((32, 1, 128), F32), vmem((2, 1, HALF), F32), vmem((2, TOK, HALF), F32),
            dma((8,)), dma((2, 4, 2)), dma((8, 2)), dma((3, 2)), dma((3, 2)),
            dma((8, 2, 2)), dma((8, 4, 2)), dma((8, 2)), dma((2, 2, 2)),
            dma((1,)), dma((8,)), dma((32,)), dma((4,)), dma((8,)), dma((8,)), dma((8,)), dma((8,)),
            dma((4,)), dma((4,)), dma((8,)), dma((8,)), dma((32,)), dma((32,)),
            pltpu.SemaphoreType.REGULAR((3,)),
        ],
        compiler_params=pltpu.CompilerParams(
            collective_id=0, has_side_effects=True, vmem_limit_bytes=55779328
        ),
    )(hidden, weight.T, factor_b.T, factor_a, magnitude, cotangent)
    return mixed, gmag[0, :18], grads[:, 72:90], grads[:, :72].T


def solution(mesh):
    return jax.shard_map(
        body,
        mesh=mesh,
        in_specs=(
            P("dp", "tensor"),
            P("tensor", "dp"),
            P("tensor", None),
            P(None, "dp"),
            P("tensor"),
            P("dp", "tensor"),
        ),
        out_specs=(
            P("dp", "tensor"),
            P(("tensor", "dp")),
            P(None, ("tensor", "dp")),
            P(("tensor", "dp"), None),
        ),
        check_vma=False,
    )
```

```python
import functools

import jax
import jax.numpy as jnp
from jax import lax
from jax.experimental import pallas as pl
from jax.experimental.pallas import tpu as pltpu
from jax.sharding import PartitionSpec as P

TOK, HID, COLS, OUT, HALF = 320, 2304, 144, 576, 288
MESH = pl.DeviceIdType.MESH
F32, BF = jnp.float32, jnp.bfloat16
CHUNKS = ((0, 80), (80, 64))
FIRST, LAST = 192, 128
PARTS = ((0, 2 * FIRST), (2 * FIRST, 2 * LAST))


def remote(src, dst, send, recv, dp, tensor):
    return pltpu.make_async_remote_copy(
        src_ref=src, dst_ref=dst, send_sem=send, recv_sem=recv,
        device_id=(dp, tensor), device_id_type=MESH,
    )


def kernel(h_ref, w_ref, b_hbm, a_hbm, mag_hbm, cot_hbm, mixed_ref, grads_ref, gmag_ref,
           b_ref, a_ref, mag_ref, cot_ref, own, toks, wts, outgoing, arrived, turned, halves,
           sq_out, sq_in, msg_f, msg, msgs, a_all, sq_all, norms, scales, low_in, back_in, low_out, back_out,
           dpre, extra, cots,
           spread, spread_in, plane, plane_in, mag_out, mag_in, sums, results,
           loc_sem, w_send, w_recv, t_send, t_recv, y_send, y_recv, x_send, x_recv,
           s_send, s_recv, m_send, m_recv, l_send, l_recv, b_send, b_recv, d_send, d_recv, p_send, p_recv,
           g_send, g_recv,
           met):
    dp, tensor = lax.axis_index("dp"), lax.axis_index("tensor")
    x_hi, z, core = dp // 16, (dp // 2) % 8, dp % 2
    x_lo, y = tensor // 4, tensor % 4
    other = 1 - core

    def dp_of(a, b, c):
        return a * 16 + b * 2 + c

    def rows(part, of):
        if part == 0:
            return pl.ds(of * FIRST, FIRST), pl.ds(0, FIRST)
        return pl.ds(2 * FIRST + of * LAST, LAST), pl.ds(FIRST, LAST)

    load_h = pltpu.make_async_copy(h_ref, own, loc_sem.at[0])
    place = []
    for part in range(2):
        there, here = rows(part, core)
        place.append(pltpu.make_async_copy(h_ref.at[here], toks.at[0, there], loc_sem.at[6 + part]))
    load_w = pltpu.make_async_copy(w_ref, wts.at[0], loc_sem.at[1])
    loads = [pltpu.make_async_copy(src, dst, loc_sem.at[2 + i]) for i, (src, dst) in enumerate(
        ((a_hbm, a_ref), (b_hbm, b_ref), (mag_hbm, mag_ref), (cot_hbm, cot_ref)))]
    load_w.start()
    loads[0].start()
    loads[1].start()
    load_h.start()
    place[0].start()
    place[1].start()
    loads[2].start()
    loads[3].start()

    barrier = pltpu.get_barrier_semaphore()

    def greet(p):
        pl.semaphore_signal(barrier, inc=1, device_id=p, device_id_type=MESH)

    near = [(dp, (tensor + k) % 8) for k in range(1, 8)]
    near += [(dp_of(x_hi, (z + 1) % 8, core), tensor), (dp_of(x_hi, (z + 7) % 8, core), tensor),
             (dp_of(x_hi, z, other), tensor), (dp_of(1 - x_hi, z, core), tensor), (dp_of(1 - x_hi, z, other), tensor)]
    for p in near:
        greet(p)
    spread[...] = jnp.zeros_like(spread)
    msg_f[...] = jnp.zeros_like(msg_f)
    load_w.wait()
    load_h.wait()
    with jax.named_scope('barrier_wait'):
        pl.semaphore_wait(barrier, len(near))

    def tell(k):
        for to in ((z + k) % 8, (z + 8 - k) % 8)[:1 if k == 4 else 2]:
            pl.semaphore_signal(met.at[k // 2], inc=1, device_id=(dp_of(x_hi, to, core), tensor), device_id_type=MESH)

    tell(1)

    def w_copy(side, k, ch):
        at, n = CHUNKS[ch]
        src = 0 if k == 1 else 2 * (k - 1) - 1 + side
        dst = 7 if k == 4 else 2 * k - 1 + side
        to = (z + 1) % 8 if side == 0 else (z + 7) % 8
        return remote(wts.at[src, pl.ds(at, n)], wts.at[dst, pl.ds(at, n)],
                      w_send.at[side, k - 1, ch], w_recv.at[dst, ch], dp_of(x_hi, to, core), tensor)

    w_copy(0, 1, 0).start()
    w_copy(1, 1, 1).start()
    w_copy(0, 1, 1).start()
    w_copy(1, 1, 0).start()
    to_other, to_far, relay = [], [], []
    for part in range(2):
        there, here = rows(part, core)
        to_other.append(remote(own.at[here], toks.at[0, there], t_send.at[0, part], t_recv.at[0, part],
                               dp_of(x_hi, z, other), tensor))
        to_far.append(remote(own.at[here], toks.at[1, there], t_send.at[1, part], t_recv.at[1, part],
                             dp_of(1 - x_hi, z, core), tensor))
        relay.append(remote(toks.at[1, there], toks.at[1, there], t_send.at[2, part], t_recv.at[2, part],
                            dp_of(x_hi, z, other), tensor))

    to_other[0].start()
    to_other[1].start()

    owner = dp // 4
    loads[0].wait()
    loads[1].wait()
    merged = wts[0].astype(F32) + lax.dot_general(
        a_ref[...], b_ref[...], (((0,), (0,)), ((), ())), preferred_element_type=F32)
    squares = merged * merged
    lanes = squares[:, 0:128]
    for i in range(1, 18):
        lanes = lanes + squares[:, 128 * i:128 * (i + 1)]
    own_sq = jnp.sum(lanes.T, axis=0, keepdims=True)
    sq_row = jnp.broadcast_to(own_sq, (8, COLS))

    @pl.when(owner == tensor)
    def _():
        sq_in[tensor] = sq_row

    @pl.when(owner != tensor)
    def _():
        sq_out[...] = sq_row

    low_part = lax.dot_general(b_ref[...], own[...], (((1,), (1,)), ((), ())), preferred_element_type=F32)
    low_out[...] = low_part
    low_in[tensor] = low_part
    sq_copy = remote(sq_out, sq_in.at[tensor], s_send.at[0], s_recv.at[tensor], dp, owner)

    @pl.when(owner != tensor)
    def _():
        sq_copy.start()

    def over_tensor(src, dst, send, recv, act):
        def body(i, carry):
            to = (tensor + i) % 8
            if act == "recv":
                remote(src, dst.at[to], send.at[i], recv.at[to], dp, to).wait_recv()
            elif act == "start":
                remote(src, dst.at[tensor], send.at[i], recv.at[tensor], dp, to).start()
            else:
                remote(src, dst.at[tensor], send.at[i], recv.at[tensor], dp, to).wait_send()
            return carry
        lax.fori_loop(1, 8, body, 0)

    over_tensor(low_out, low_in, l_send, l_recv, "start")
    to_far[0].start()
    to_far[1].start()

    pl.semaphore_wait(met.at[0], 2)
    tell(2)
    loads[2].wait()
    loads[3].wait()

    def zsrc_of(j):
        k = (j + 1) // 2
        return (z + 8 + k - 2 * k * (j % 2)) % 8

    def summer_at(owner_y, g, of):
        return (owner_y + jnp.where(g == 0, 3 - 2 * of, 2 * of)) % 4

    def summer(j, g):
        return summer_at(zsrc_of(j) // 2, g, core)

    def y_copy(j, g, part):
        lanes = pl.ds(*PARTS[part])
        return remote(outgoing.at[j, g, :, lanes], arrived.at[j, y, :, lanes], y_send.at[j, g, part],
                      y_recv.at[j, y, part], dp, x_lo * 4 + summer(j, g))

    def local(j, g):
        return summer(j, g) == y

    def item(j, g, parts):
        lo, hi = PARTS[parts[0]][0], sum(PARTS[parts[-1]])
        p = lax.dot_general(toks[g, lo:hi], wts[j], (((1,), (1,)), ((), ())), preferred_element_type=F32)
        p = p.T.astype(BF)
        here = local(j, g)

        @pl.when(here)
        def _():
            arrived[j, y, :, lo:hi] = p

        @pl.when(jnp.logical_not(here))
        def _():
            outgoing[j, g, :, lo:hi] = p
            for part in parts:
                y_copy(j, g, part).start()

    def items(lo, hi, g, parts=(0, 1)):
        def body(j, carry):
            item(j, g, parts)
            return carry
        lax.fori_loop(lo, hi, body, 0)

    def items_both(lo, hi):
        def body(i, carry):
            item(lo + i // 2, i % 2, (0, 1))
            return carry
        lax.fori_loop(0, 2 * (hi - lo), body, 0)

    def msg_copy(i):
        return remote(msg, msgs.at[dp % 4], m_send.at[i], m_recv.at[dp % 4], (dp + i) % 32, tensor)

    def publish():
        def arrive(i, carry):
            frm = (tensor + i) % 8
            remote(sq_out, sq_in.at[frm], s_send.at[0], s_recv.at[frm], dp, frm).wait_recv()
            return carry
        lax.fori_loop(1, 8, arrive, 0)
        total = sq_in[0]
        for i in range(1, 8):
            total = total + sq_in[i]
        total = total[0:1]
        high = total.astype(BF).astype(F32)
        rest = total - high
        msg_f[:, 0:COLS] = a_ref[...].astype(F32)
        for i in range(3):
            msg_f[i:i + 1, 144:192] = high[:, 48 * i:48 * (i + 1)]
            msg_f[3 + i:4 + i, 144:192] = rest[:, 48 * i:48 * (i + 1)]
        packed = msg_f[...].astype(BF)
        msg[...] = packed
        msgs[dp % 4] = packed

        def send(i, carry):
            msg_copy(i).start()
            return carry
        lax.fori_loop(1, 32, send, 0)

    def receive():
        for j in range(4):
            @pl.when(dp != tensor * 4 + j)
            def _():
                remote(msg, msgs.at[j], m_send.at[0], m_recv.at[j], dp, tensor).wait_recv()
        for j in range(4):
            m = msgs[j].astype(F32)
            zp, at = j // 2, COLS * (j % 2)
            a_all[zp, :, at:at + COLS] = m[:, 0:COLS]
            for i in range(3):
                sq_all[zp, :, at + 48 * i:at + 48 * (i + 1)] = m[i:i + 1, 144:192] + m[3 + i:4 + i, 144:192]

    def backward():
        back = None
        mags = mag_ref[...].reshape(1, OUT)
        for zp in range(2):
            norm = jnp.sqrt(sq_all[zp] + 1e-6)
            scale = mags[:, HALF * zp:HALF * (zp + 1)] / norm
            norms[zp] = norm
            scales[zp] = scale
            cot = cot_ref[:, HALF * zp:HALF * (zp + 1)].astype(F32)
            cots[zp] = cot
            d = (cot * scale).astype(BF)
            dpre[zp] = d
            part = lax.dot_general(a_all[zp].astype(BF), d, (((1,), (1,)), ((), ())), preferred_element_type=F32)
            back = part if back is None else back + part
        back_out[...] = back
        back_in[tensor] = back
        over_tensor(back_out, back_in, b_send, b_recv, "start")

    group = x_hi * 2 + core

    def spread_copy(i):
        to = (group + i) % 4
        return remote(spread.at[to], spread_in.at[group], d_send.at[i], d_recv.at[group],
                      dp_of(to // 2, z, to % 2), tensor)

    def gradients():
        over_tensor(low_out, low_in, l_send, l_recv, "recv")
        over_tensor(back_out, back_in, b_send, b_recv, "recv")
        low, back = low_in[0], back_in[0]
        for i in range(1, 8):
            low = low + low_in[i]
            back = back + back_in[i]
        low, back = low.astype(BF), back.astype(BF)
        grad_b = jnp.dot(back, own[...], preferred_element_type=F32)
        grad_a = [jnp.dot(low, dpre[zp], preferred_element_type=F32) for zp in range(2)]
        for x in range(2):
            for zz in range(8):
                for c in range(2):
                    i = x * 16 + zz * 2 + c
                    spread[x * 2 + c, zz, :, 0:72] = grad_b[:, 72 * i:72 * (i + 1)]
                    spread[x * 2 + c, zz, :, 72:90] = grad_a[x][:, 18 * (i % 16):18 * (i % 16 + 1)]
        for i in range(1, 4):
            spread_copy(i).start()
        for zp in range(2):
            extra[zp] = lax.dot_general(low, a_all[zp].astype(BF), (((0,), (0,)), ((), ())),
                                        preferred_element_type=F32)

    def plane_copy(i):
        to = (z + i) % 8
        return remote(plane.at[to], plane_in.at[z], p_send.at[i], p_recv.at[z], dp_of(x_hi, to, core), tensor)

    def sum_plane():
        total = spread[group]
        for i in range(1, 4):
            frm = (group + i) % 4
            remote(spread.at[0], spread_in.at[frm], d_send.at[0], d_recv.at[frm], dp, tensor).wait_recv()
            total = total + spread_in[frm]
        plane[...] = total

        def send(i, carry):
            plane_copy(i).start()
            return carry
        lax.fori_loop(1, 8, send, 0)

    def sum_planes():
        total = plane[z]
        for i in range(1, 8):
            frm = (z + i) % 8
            remote(plane.at[0], plane_in.at[frm], p_send.at[0], p_recv.at[frm], dp, tensor).wait_recv()
            total = total + plane_in[frm]
        grads_ref[...] = total

    def ring(k, first):
        for side in (0, 1):
            ch = first if side == 0 else 1 - first
            w_copy(side, k, ch).wait_recv()
            if k < 3 or first == 0:
                w_copy(side, k + 1, ch).start()

    def x_copy(j, g, ct):
        zs = zsrc_of(j)
        tok_hi = jnp.where(g == 0, x_hi, 1 - x_hi)
        return remote(turned.at[j, ct], halves.at[x_lo, zs % 2, core], x_send.at[j, ct],
                      x_recv.at[x_lo, zs % 2, core], dp_of(tok_hi, z, ct), x_hi * 4 + zs // 2)

    def to_self(j, g, ct):
        same = jnp.logical_and(g == 0, x_lo == x_hi)
        return jnp.logical_and(same, jnp.logical_and(zsrc_of(j) // 2 == y, core == ct))

    def active(j, g):
        return summer(j, g) == y

    def stage_two(j, g):
        for k in range(1, 4):
            ys = (y + k) % 4
            for part in range(2):
                lanes = pl.ds(*PARTS[part])
                remote(outgoing.at[0, 0, :, lanes], arrived.at[j, ys, :, lanes], y_send.at[0, 0, part],
                       y_recv.at[j, ys, part], dp, tensor).wait_recv()
        total = arrived[j, 0].astype(F32)
        for ys in range(1, 4):
            total = total + arrived[j, ys].astype(F32)
        total = total.astype(BF)
        for ct in range(2):
            part = jnp.concatenate(
                [total[:, ct * FIRST:(ct + 1) * FIRST],
                 total[:, 2 * FIRST + ct * LAST:2 * FIRST + (ct + 1) * LAST]], axis=1)
            mine_too = to_self(j, g, ct)

            @pl.when(mine_too)
            def _():
                halves[x_lo, zsrc_of(j) % 2, core] = part

            @pl.when(jnp.logical_not(mine_too))
            def _():
                turned[j, ct] = part
                x_copy(j, g, ct).start()

    def second(lo, hi, g):
        def unit(j, carry):
            pl.when(active(j, g))(lambda: stage_two(j, g))
            return carry
        lax.fori_loop(lo, hi, unit, 0)

    def steps_of(zp):
        away = (2 * y + zp - z + 8) % 8
        return jnp.where(away > 4, 8 - away, away)

    with jax.named_scope("a0"):
        for part in range(2):
            place[part].wait()
            to_other[part].wait_recv()
    items(0, 1, 0)
    pl.semaphore_wait(met.at[1], 2)
    tell(4)

    def publish_when_met():
        pl.semaphore_wait(met.at[2], 1)
        publish()
    with jax.named_scope("a1_publish"):
        pl.when(owner == tensor)(publish_when_met)
    with jax.named_scope("a2_ring10"):
        ring(1, 0)

    @pl.when(owner != tensor)
    def _():
        pl.semaphore_wait(met.at[2], 1)
    with jax.named_scope("a3_ring11"):
        ring(1, 1)
    items(1, 3, 0)
    with jax.named_scope("a4_far0"):
        to_far[0].wait_recv()
    relay[0].start()
    with jax.named_scope("a5_ring20"):
        ring(2, 0)
    with jax.named_scope("a6_relay0"):
        relay[0].wait_recv()
    items(0, 3, 1, (0,))
    with jax.named_scope("aa_second"):
        second(0, 3, 0)
    with jax.named_scope("a8_ring21"):
        ring(2, 1)
    items(3, 5, 0)
    items(3, 5, 1, (0,))
    with jax.named_scope("a9_far1"):
        to_far[1].wait_recv()
    relay[1].start()
    with jax.named_scope("aa_receive"):
        receive()
    backward()
    with jax.named_scope("ab_relay1"):
        relay[1].wait_recv()
    items(0, 5, 1, (1,))
    with jax.named_scope("ac_ring30"):
        ring(3, 0)
    with jax.named_scope("b3_second"):
        second(3, 5, 0)
    with jax.named_scope("b1_ring31"):
        ring(3, 1)
    with jax.named_scope("b2_items"):
        items_both(5, 7)
    with jax.named_scope("b5_last"):
        w_copy(0, 4, 0).wait_recv()
        w_copy(1, 4, 1).wait_recv()
    with jax.named_scope("b6_items"):
        items_both(7, 8)
    with jax.named_scope("b8_grads"):
        gradients()
    with jax.named_scope("b9_second"):
        second(0, 5, 1)
    with jax.named_scope("ba_second"):
        second(5, 7, 0)
        second(5, 7, 1)
    with jax.named_scope("bb_second"):
        second(7, 8, 0)
        second(7, 8, 1)

    def finish(i, carry):
        zp = jnp.where(steps_of(0) <= steps_of(1), i, 1 - i)
        away = jnp.where(x_lo == x_hi, 0, 1)
        parts = []
        for cs in range(2):
            for xl in range(2):
                frm = summer_at(y, away, cs)
                own_part = jnp.logical_and(jnp.logical_and(x_lo == x_hi, xl == x_lo),
                                           jnp.logical_and(frm == y, core == cs))

                @pl.when(jnp.logical_not(own_part))
                def _():
                    remote(turned.at[0, 0], halves.at[xl, zp, cs], x_send.at[0, 0], x_recv.at[xl, zp, cs],
                           dp, tensor).wait_recv()
            parts.append(halves[0, zp, cs].astype(F32) + halves[1, zp, cs].astype(F32))
        pre = extra[zp] + jnp.concatenate(parts, axis=0).T
        sums[zp] = jnp.sum(cots[zp] * pre, axis=0, keepdims=True) / norms[zp]
        results[zp] = pre * scales[zp]
        return carry
    with jax.named_scope("c0_finish"):
        lax.fori_loop(0, 2, finish, 0)
    for i in range(32):
        mag_out[i, :, 0:18] = sums[i // 16][:, 18 * (i % 16):18 * (i % 16 + 1)]

    def mag_copy(i):
        to = (dp + i) % 32
        return remote(mag_out.at[to], mag_in.at[dp], g_send.at[i], g_recv.at[dp], to, tensor)

    def mag_start(i, carry):
        mag_copy(i).start()
        return carry
    with jax.named_scope("c1_mag"):
        lax.fori_loop(1, 32, mag_start, 0)
    with jax.named_scope("c2_plane"):
        sum_plane()
    with jax.named_scope("c2_mixed"):
        for zp in range(2):
            mixed_ref[:, HALF * zp:HALF * (zp + 1)] = results[zp].astype(BF)
    with jax.named_scope("c4_planes"):
        sum_planes()

    for k in (1, 2, 3, 4):
        for side in (0, 1):
            for ch in (0, 1):
                if k < 4 or ch == side:
                    w_copy(side, k, ch).wait_send()
    @pl.when(owner != tensor)
    def _():
        sq_copy.wait_send()

    @pl.when(owner == tensor)
    def _():
        def sent(i, carry):
            msg_copy(i).wait_send()
            return carry
        lax.fori_loop(1, 32, sent, 0)
    over_tensor(low_out, low_in, l_send, l_recv, "send")
    over_tensor(back_out, back_in, b_send, b_recv, "send")
    for i in range(1, 4):
        spread_copy(i).wait_send()

    def plane_sent(i, carry):
        plane_copy(i).wait_send()
        return carry
    lax.fori_loop(1, 8, plane_sent, 0)
    for copies in (to_other, to_far, relay):
        for part in range(2):
            copies[part].wait_send()
    def drain(j, carry):
        for g in range(2):
            @pl.when(jnp.logical_not(local(j, g)))
            def _():
                for part in range(2):
                    y_copy(j, g, part).wait_send()
            for ct in range(2):
                @pl.when(jnp.logical_and(active(j, g), jnp.logical_not(to_self(j, g, ct))))
                def _():
                    x_copy(j, g, ct).wait_send()
        return carry
    lax.fori_loop(0, 8, drain, 0)

    def mag_arrive(i, total):
        frm = (dp + i) % 32
        remote(mag_out.at[0], mag_in.at[frm], g_send.at[0], g_recv.at[frm], dp, tensor).wait_recv()
        return total + mag_in[frm]
    with jax.named_scope("c5_gmag"):
        gmag_ref[...] = lax.fori_loop(1, 32, mag_arrive, mag_out[dp])

    def mag_sent(i, carry):
        mag_copy(i).wait_send()
        return carry
    lax.fori_loop(1, 32, mag_sent, 0)


def body(hidden, weight, factor_b, factor_a, magnitude, cotangent):
    hbm_spec, vmem_spec = pl.BlockSpec(memory_space=pltpu.HBM), pl.BlockSpec(memory_space=pltpu.VMEM)
    dma, vmem = pltpu.SemaphoreType.DMA, pltpu.VMEM
    mixed, grads, gmag = pl.pallas_call(
        kernel,
        name="dora",
        out_shape=(jax.ShapeDtypeStruct((TOK, OUT), BF), jax.ShapeDtypeStruct((16, 128), F32),
                   jax.ShapeDtypeStruct((1, 128), F32)),
        in_specs=[hbm_spec] * 6,
        out_specs=(vmem_spec,) * 3,
        scratch_shapes=[
            vmem((16, HID), BF), vmem((16, COLS), BF), vmem((OUT,), F32), vmem((TOK, OUT), BF), vmem((TOK, HID), BF),
            vmem((2, 2 * TOK, HID), BF),
            vmem((8, COLS, HID), BF),
            vmem((8, 2, COLS, 2 * TOK), BF),
            vmem((8, 4, COLS, 2 * TOK), BF),
            vmem((8, 2, COLS, TOK), BF),
            vmem((2, 2, 2, COLS, TOK), BF),
            vmem((8, COLS), F32), vmem((8, 8, COLS), F32),
            vmem((16, 256), F32), vmem((16, 256), BF), vmem((4, 16, 256), BF),
            vmem((2, 16, HALF), F32), vmem((2, 1, HALF), F32), vmem((2, 1, HALF), F32), vmem((2, 1, HALF), F32),
            vmem((8, 16, TOK), F32), vmem((8, 16, TOK), F32), vmem((16, TOK), F32), vmem((16, TOK), F32),
            vmem((2, TOK, HALF), BF), vmem((2, TOK, HALF), F32), vmem((2, TOK, HALF), F32),
            vmem((4, 8, 16, 128), F32), vmem((4, 8, 16, 128), F32),
            vmem((8, 16, 128), F32), vmem((8, 16, 128), F32),
            vmem((32, 1, 128), F32), vmem((32, 1, 128), F32), vmem((2, 1, HALF), F32), vmem((2, TOK, HALF), F32),
            dma((8,)), dma((2, 4, 2)), dma((8, 2)), dma((3, 2)), dma((3, 2)),
            dma((8, 2, 2)), dma((8, 4, 2)), dma((8, 2)), dma((2, 2, 2)),
            dma((1,)), dma((8,)), dma((32,)), dma((4,)), dma((8,)), dma((8,)), dma((8,)), dma((8,)),
            dma((4,)), dma((4,)), dma((8,)), dma((8,)), dma((32,)), dma((32,)),
            pltpu.SemaphoreType.REGULAR((3,)),
        ],
        compiler_params=pltpu.CompilerParams(
            collective_id=0, has_side_effects=True, vmem_limit_bytes=55779328
        ),
    )(hidden, weight.T, factor_b.T, factor_a, magnitude, cotangent)
    return mixed, gmag[0, :18], grads[:, 72:90], grads[:, :72].T


def solution(mesh):
    return jax.shard_map(
        body,
        mesh=mesh,
        in_specs=(
            P("dp", "tensor"),
            P("tensor", "dp"),
            P("tensor", None),
            P(None, "dp"),
            P("tensor"),
            P("dp", "tensor"),
        ),
        out_specs=(
            P("dp", "tensor"),
            P(("tensor", "dp")),
            P(None, ("tensor", "dp")),
            P(("tensor", "dp"), None),
        ),
        check_vma=False,
    )
```

```python
import functools

import jax
import jax.numpy as jnp
from jax import lax
from jax.experimental import pallas as pl
from jax.experimental.pallas import tpu as pltpu
from jax.sharding import PartitionSpec as P

TOK, HID, COLS, OUT, HALF = 320, 2304, 144, 576, 288
MESH = pl.DeviceIdType.MESH
F32, BF = jnp.float32, jnp.bfloat16
CHUNKS = ((0, 80), (80, 64))
FIRST, LAST = 256, 64
PARTS = ((0, 2 * FIRST), (2 * FIRST, 2 * LAST))


def remote(src, dst, send, recv, dp, tensor):
    return pltpu.make_async_remote_copy(
        src_ref=src, dst_ref=dst, send_sem=send, recv_sem=recv,
        device_id=(dp, tensor), device_id_type=MESH,
    )


def kernel(h_ref, w_ref, b_hbm, a_hbm, mag_hbm, cot_hbm, mixed_ref, grads_ref, gmag_ref,
           b_ref, a_ref, mag_ref, cot_ref, own, toks, wts, outgoing, arrived, turned, halves,
           sq_out, sq_in, msg_f, msg, msgs, a_all, sq_all, norms, scales, low_in, back_in, low_out, back_out,
           dpre, extra, cots,
           spread, spread_in, plane, plane_in, mag_out, mag_in, sums, results,
           loc_sem, w_send, w_recv, t_send, t_recv, y_send, y_recv, x_send, x_recv,
           s_send, s_recv, m_send, m_recv, l_send, l_recv, b_send, b_recv, d_send, d_recv, p_send, p_recv,
           g_send, g_recv,
           met):
    dp, tensor = lax.axis_index("dp"), lax.axis_index("tensor")
    x_hi, z, core = dp // 16, (dp // 2) % 8, dp % 2
    x_lo, y = tensor // 4, tensor % 4
    other = 1 - core

    def dp_of(a, b, c):
        return a * 16 + b * 2 + c

    def rows(part, of):
        if part == 0:
            return pl.ds(of * FIRST, FIRST), pl.ds(0, FIRST)
        return pl.ds(2 * FIRST + of * LAST, LAST), pl.ds(FIRST, LAST)

    load_h = pltpu.make_async_copy(h_ref, own, loc_sem.at[0])
    place = []
    for part in range(2):
        there, here = rows(part, core)
        place.append(pltpu.make_async_copy(h_ref.at[here], toks.at[0, there], loc_sem.at[6 + part]))
    load_w = pltpu.make_async_copy(w_ref, wts.at[0], loc_sem.at[1])
    loads = [pltpu.make_async_copy(src, dst, loc_sem.at[2 + i]) for i, (src, dst) in enumerate(
        ((a_hbm, a_ref), (b_hbm, b_ref), (mag_hbm, mag_ref), (cot_hbm, cot_ref)))]
    load_w.start()
    loads[0].start()
    loads[1].start()
    load_h.start()
    place[0].start()
    place[1].start()
    loads[2].start()
    loads[3].start()

    barrier = pltpu.get_barrier_semaphore()

    def greet(p):
        pl.semaphore_signal(barrier, inc=1, device_id=p, device_id_type=MESH)

    near = [(dp, (tensor + k) % 8) for k in range(1, 8)]
    near += [(dp_of(x_hi, (z + 1) % 8, core), tensor), (dp_of(x_hi, (z + 7) % 8, core), tensor),
             (dp_of(x_hi, z, other), tensor), (dp_of(1 - x_hi, z, core), tensor), (dp_of(1 - x_hi, z, other), tensor)]
    for p in near:
        greet(p)
    spread[...] = jnp.zeros_like(spread)
    msg_f[...] = jnp.zeros_like(msg_f)
    load_w.wait()
    load_h.wait()
    with jax.named_scope('barrier_wait'):
        pl.semaphore_wait(barrier, len(near))

    def tell(k):
        for to in ((z + k) % 8, (z + 8 - k) % 8)[:1 if k == 4 else 2]:
            pl.semaphore_signal(met.at[k // 2], inc=1, device_id=(dp_of(x_hi, to, core), tensor), device_id_type=MESH)

    tell(1)

    def w_copy(side, k, ch):
        at, n = CHUNKS[ch]
        src = 0 if k == 1 else 2 * (k - 1) - 1 + side
        dst = 7 if k == 4 else 2 * k - 1 + side
        to = (z + 1) % 8 if side == 0 else (z + 7) % 8
        return remote(wts.at[src, pl.ds(at, n)], wts.at[dst, pl.ds(at, n)],
                      w_send.at[side, k - 1, ch], w_recv.at[dst, ch], dp_of(x_hi, to, core), tensor)

    w_copy(0, 1, 0).start()
    w_copy(1, 1, 1).start()
    w_copy(0, 1, 1).start()
    w_copy(1, 1, 0).start()
    to_other, to_far, relay = [], [], []
    for part in range(2):
        there, here = rows(part, core)
        to_other.append(remote(own.at[here], toks.at[0, there], t_send.at[0, part], t_recv.at[0, part],
                               dp_of(x_hi, z, other), tensor))
        to_far.append(remote(own.at[here], toks.at[1, there], t_send.at[1, part], t_recv.at[1, part],
                             dp_of(1 - x_hi, z, core), tensor))
        relay.append(remote(toks.at[1, there], toks.at[1, there], t_send.at[2, part], t_recv.at[2, part],
                            dp_of(x_hi, z, other), tensor))

    to_other[0].start()
    to_other[1].start()

    owner = dp // 4
    loads[0].wait()
    loads[1].wait()
    merged = wts[0].astype(F32) + lax.dot_general(
        a_ref[...], b_ref[...], (((0,), (0,)), ((), ())), preferred_element_type=F32)
    squares = merged * merged
    lanes = squares[:, 0:128]
    for i in range(1, 18):
        lanes = lanes + squares[:, 128 * i:128 * (i + 1)]
    own_sq = jnp.sum(lanes.T, axis=0, keepdims=True)
    sq_row = jnp.broadcast_to(own_sq, (8, COLS))

    @pl.when(owner == tensor)
    def _():
        sq_in[tensor] = sq_row

    @pl.when(owner != tensor)
    def _():
        sq_out[...] = sq_row

    low_part = lax.dot_general(b_ref[...], own[...], (((1,), (1,)), ((), ())), preferred_element_type=F32)
    low_out[...] = low_part
    low_in[tensor] = low_part
    sq_copy = remote(sq_out, sq_in.at[tensor], s_send.at[0], s_recv.at[tensor], dp, owner)

    @pl.when(owner != tensor)
    def _():
        sq_copy.start()

    def over_tensor(src, dst, send, recv, act):
        def body(i, carry):
            to = (tensor + i) % 8
            if act == "recv":
                remote(src, dst.at[to], send.at[i], recv.at[to], dp, to).wait_recv()
            elif act == "start":
                remote(src, dst.at[tensor], send.at[i], recv.at[tensor], dp, to).start()
            else:
                remote(src, dst.at[tensor], send.at[i], recv.at[tensor], dp, to).wait_send()
            return carry
        lax.fori_loop(1, 8, body, 0)

    over_tensor(low_out, low_in, l_send, l_recv, "start")
    to_far[0].start()
    to_far[1].start()

    pl.semaphore_wait(met.at[0], 2)
    tell(2)
    loads[2].wait()
    loads[3].wait()

    def zsrc_of(j):
        k = (j + 1) // 2
        return (z + 8 + k - 2 * k * (j % 2)) % 8

    def summer_at(owner_y, g, of):
        return (owner_y + jnp.where(g == 0, 3 - 2 * of, 2 * of)) % 4

    def summer(j, g):
        return summer_at(zsrc_of(j) // 2, g, core)

    def y_copy(j, g, part):
        lanes = pl.ds(*PARTS[part])
        return remote(outgoing.at[j, g, :, lanes], arrived.at[j, y, :, lanes], y_send.at[j, g, part],
                      y_recv.at[j, y, part], dp, x_lo * 4 + summer(j, g))

    def local(j, g):
        return summer(j, g) == y

    def item(j, g, parts):
        lo, hi = PARTS[parts[0]][0], sum(PARTS[parts[-1]])
        p = lax.dot_general(toks[g, lo:hi], wts[j], (((1,), (1,)), ((), ())), preferred_element_type=F32)
        p = p.T.astype(BF)
        here = local(j, g)

        @pl.when(here)
        def _():
            arrived[j, y, :, lo:hi] = p

        @pl.when(jnp.logical_not(here))
        def _():
            outgoing[j, g, :, lo:hi] = p
            for part in parts:
                y_copy(j, g, part).start()

    def items(lo, hi, g, parts=(0, 1)):
        def body(j, carry):
            item(j, g, parts)
            return carry
        lax.fori_loop(lo, hi, body, 0)

    def items_both(lo, hi):
        def body(i, carry):
            item(lo + i // 2, i % 2, (0, 1))
            return carry
        lax.fori_loop(0, 2 * (hi - lo), body, 0)

    def msg_copy(i):
        return remote(msg, msgs.at[dp % 4], m_send.at[i], m_recv.at[dp % 4], (dp + i) % 32, tensor)

    def publish():
        def arrive(i, carry):
            frm = (tensor + i) % 8
            remote(sq_out, sq_in.at[frm], s_send.at[0], s_recv.at[frm], dp, frm).wait_recv()
            return carry
        lax.fori_loop(1, 8, arrive, 0)
        total = sq_in[0]
        for i in range(1, 8):
            total = total + sq_in[i]
        total = total[0:1]
        high = total.astype(BF).astype(F32)
        rest = total - high
        msg_f[:, 0:COLS] = a_ref[...].astype(F32)
        for i in range(3):
            msg_f[i:i + 1, 144:192] = high[:, 48 * i:48 * (i + 1)]
            msg_f[3 + i:4 + i, 144:192] = rest[:, 48 * i:48 * (i + 1)]
        packed = msg_f[...].astype(BF)
        msg[...] = packed
        msgs[dp % 4] = packed

        def send(i, carry):
            msg_copy(i).start()
            return carry
        lax.fori_loop(1, 32, send, 0)

    def receive():
        for j in range(4):
            @pl.when(dp != tensor * 4 + j)
            def _():
                remote(msg, msgs.at[j], m_send.at[0], m_recv.at[j], dp, tensor).wait_recv()
        for j in range(4):
            m = msgs[j].astype(F32)
            zp, at = j // 2, COLS * (j % 2)
            a_all[zp, :, at:at + COLS] = m[:, 0:COLS]
            for i in range(3):
                sq_all[zp, :, at + 48 * i:at + 48 * (i + 1)] = m[i:i + 1, 144:192] + m[3 + i:4 + i, 144:192]

    def backward():
        back = None
        mags = mag_ref[...].reshape(1, OUT)
        for zp in range(2):
            norm = jnp.sqrt(sq_all[zp] + 1e-6)
            scale = mags[:, HALF * zp:HALF * (zp + 1)] / norm
            norms[zp] = norm
            scales[zp] = scale
            cot = cot_ref[:, HALF * zp:HALF * (zp + 1)].astype(F32)
            cots[zp] = cot
            d = (cot * scale).astype(BF)
            dpre[zp] = d
            part = lax.dot_general(a_all[zp].astype(BF), d, (((1,), (1,)), ((), ())), preferred_element_type=F32)
            back = part if back is None else back + part
        back_out[...] = back
        back_in[tensor] = back
        over_tensor(back_out, back_in, b_send, b_recv, "start")

    group = x_hi * 2 + core

    def spread_copy(i):
        to = (group + i) % 4
        return remote(spread.at[to], spread_in.at[group], d_send.at[i], d_recv.at[group],
                      dp_of(to // 2, z, to % 2), tensor)

    def gradients():
        over_tensor(low_out, low_in, l_send, l_recv, "recv")
        over_tensor(back_out, back_in, b_send, b_recv, "recv")
        low, back = low_in[0], back_in[0]
        for i in range(1, 8):
            low = low + low_in[i]
            back = back + back_in[i]
        low, back = low.astype(BF), back.astype(BF)
        grad_b = jnp.dot(back, own[...], preferred_element_type=F32)
        grad_a = [jnp.dot(low, dpre[zp], preferred_element_type=F32) for zp in range(2)]
        for x in range(2):
            for zz in range(8):
                for c in range(2):
                    i = x * 16 + zz * 2 + c
                    spread[x * 2 + c, zz, :, 0:72] = grad_b[:, 72 * i:72 * (i + 1)]
                    spread[x * 2 + c, zz, :, 72:90] = grad_a[x][:, 18 * (i % 16):18 * (i % 16 + 1)]
        for i in range(1, 4):
            spread_copy(i).start()
        for zp in range(2):
            extra[zp] = lax.dot_general(low, a_all[zp].astype(BF), (((0,), (0,)), ((), ())),
                                        preferred_element_type=F32)

    def plane_copy(i):
        to = (z + i) % 8
        return remote(plane.at[to], plane_in.at[z], p_send.at[i], p_recv.at[z], dp_of(x_hi, to, core), tensor)

    def sum_plane():
        total = spread[group]
        for i in range(1, 4):
            frm = (group + i) % 4
            remote(spread.at[0], spread_in.at[frm], d_send.at[0], d_recv.at[frm], dp, tensor).wait_recv()
            total = total + spread_in[frm]
        plane[...] = total

        def send(i, carry):
            plane_copy(i).start()
            return carry
        lax.fori_loop(1, 8, send, 0)

    def sum_planes():
        total = plane[z]
        for i in range(1, 8):
            frm = (z + i) % 8
            remote(plane.at[0], plane_in.at[frm], p_send.at[0], p_recv.at[frm], dp, tensor).wait_recv()
            total = total + plane_in[frm]
        grads_ref[...] = total

    def ring(k, first):
        for side in (0, 1):
            ch = first if side == 0 else 1 - first
            w_copy(side, k, ch).wait_recv()
            if k < 3 or first == 0:
                w_copy(side, k + 1, ch).start()

    def x_copy(j, g, ct):
        zs = zsrc_of(j)
        tok_hi = jnp.where(g == 0, x_hi, 1 - x_hi)
        return remote(turned.at[j, ct], halves.at[x_lo, zs % 2, core], x_send.at[j, ct],
                      x_recv.at[x_lo, zs % 2, core], dp_of(tok_hi, z, ct), x_hi * 4 + zs // 2)

    def to_self(j, g, ct):
        same = jnp.logical_and(g == 0, x_lo == x_hi)
        return jnp.logical_and(same, jnp.logical_and(zsrc_of(j) // 2 == y, core == ct))

    def active(j, g):
        return summer(j, g) == y

    def stage_two(j, g):
        for k in range(1, 4):
            ys = (y + k) % 4
            for part in range(2):
                lanes = pl.ds(*PARTS[part])
                remote(outgoing.at[0, 0, :, lanes], arrived.at[j, ys, :, lanes], y_send.at[0, 0, part],
                       y_recv.at[j, ys, part], dp, tensor).wait_recv()
        total = arrived[j, 0].astype(F32)
        for ys in range(1, 4):
            total = total + arrived[j, ys].astype(F32)
        total = total.astype(BF)
        for ct in range(2):
            part = jnp.concatenate(
                [total[:, ct * FIRST:(ct + 1) * FIRST],
                 total[:, 2 * FIRST + ct * LAST:2 * FIRST + (ct + 1) * LAST]], axis=1)
            mine_too = to_self(j, g, ct)

            @pl.when(mine_too)
            def _():
                halves[x_lo, zsrc_of(j) % 2, core] = part

            @pl.when(jnp.logical_not(mine_too))
            def _():
                turned[j, ct] = part
                x_copy(j, g, ct).start()

    def second(lo, hi, g):
        def unit(j, carry):
            pl.when(active(j, g))(lambda: stage_two(j, g))
            return carry
        lax.fori_loop(lo, hi, unit, 0)

    def steps_of(zp):
        away = (2 * y + zp - z + 8) % 8
        return jnp.where(away > 4, 8 - away, away)

    with jax.named_scope("a0"):
        for part in range(2):
            place[part].wait()
            to_other[part].wait_recv()
    items(0, 1, 0)
    pl.semaphore_wait(met.at[1], 2)
    tell(4)

    def publish_when_met():
        pl.semaphore_wait(met.at[2], 1)
        publish()
    with jax.named_scope("a1_publish"):
        pl.when(owner == tensor)(publish_when_met)
    with jax.named_scope("a2_ring10"):
        ring(1, 0)

    @pl.when(owner != tensor)
    def _():
        pl.semaphore_wait(met.at[2], 1)
    with jax.named_scope("a3_ring11"):
        ring(1, 1)
    items(1, 3, 0)
    with jax.named_scope("a5_ring20"):
        ring(2, 0)
    with jax.named_scope("a4_far0"):
        to_far[0].wait_recv()
    relay[0].start()
    with jax.named_scope("a6_relay0"):
        relay[0].wait_recv()
    items(0, 3, 1, (0,))
    with jax.named_scope("a8_ring21"):
        ring(2, 1)
    items(3, 5, 0)
    items(3, 5, 1, (0,))
    with jax.named_scope("a9_far1"):
        to_far[1].wait_recv()
    relay[1].start()
    with jax.named_scope("aa_receive"):
        receive()
    backward()
    with jax.named_scope("aa_second"):
        second(0, 3, 0)
    with jax.named_scope("ab_relay1"):
        relay[1].wait_recv()
    items(0, 5, 1, (1,))
    with jax.named_scope("ac_ring30"):
        ring(3, 0)
    with jax.named_scope("b1_ring31"):
        ring(3, 1)
    with jax.named_scope("b2_items"):
        items_both(5, 7)
    with jax.named_scope("b3_second"):
        second(3, 5, 0)
    with jax.named_scope("b5_last"):
        w_copy(0, 4, 0).wait_recv()
        w_copy(1, 4, 1).wait_recv()
    with jax.named_scope("b6_items"):
        items_both(7, 8)
    with jax.named_scope("b8_grads"):
        gradients()
    with jax.named_scope("b9_second"):
        second(0, 5, 1)
    with jax.named_scope("ba_second"):
        second(5, 7, 0)
        second(5, 7, 1)
    with jax.named_scope("bb_second"):
        second(7, 8, 0)
        second(7, 8, 1)

    def finish(i, carry):
        zp = jnp.where(steps_of(0) <= steps_of(1), i, 1 - i)
        away = jnp.where(x_lo == x_hi, 0, 1)
        parts = []
        for cs in range(2):
            for xl in range(2):
                frm = summer_at(y, away, cs)
                own_part = jnp.logical_and(jnp.logical_and(x_lo == x_hi, xl == x_lo),
                                           jnp.logical_and(frm == y, core == cs))

                @pl.when(jnp.logical_not(own_part))
                def _():
                    remote(turned.at[0, 0], halves.at[xl, zp, cs], x_send.at[0, 0], x_recv.at[xl, zp, cs],
                           dp, tensor).wait_recv()
            parts.append(halves[0, zp, cs].astype(F32) + halves[1, zp, cs].astype(F32))
        pre = extra[zp] + jnp.concatenate(parts, axis=0).T
        sums[zp] = jnp.sum(cots[zp] * pre, axis=0, keepdims=True) / norms[zp]
        results[zp] = pre * scales[zp]
        return carry
    with jax.named_scope("c0_finish"):
        lax.fori_loop(0, 2, finish, 0)
    for i in range(32):
        mag_out[i, :, 0:18] = sums[i // 16][:, 18 * (i % 16):18 * (i % 16 + 1)]

    def mag_copy(i):
        to = (dp + i) % 32
        return remote(mag_out.at[to], mag_in.at[dp], g_send.at[i], g_recv.at[dp], to, tensor)

    def mag_start(i, carry):
        mag_copy(i).start()
        return carry
    with jax.named_scope("c1_mag"):
        lax.fori_loop(1, 32, mag_start, 0)
    with jax.named_scope("c2_plane"):
        sum_plane()
    with jax.named_scope("c2_mixed"):
        for zp in range(2):
            mixed_ref[:, HALF * zp:HALF * (zp + 1)] = results[zp].astype(BF)
    with jax.named_scope("c4_planes"):
        sum_planes()

    for k in (1, 2, 3, 4):
        for side in (0, 1):
            for ch in (0, 1):
                if k < 4 or ch == side:
                    w_copy(side, k, ch).wait_send()
    @pl.when(owner != tensor)
    def _():
        sq_copy.wait_send()

    @pl.when(owner == tensor)
    def _():
        def sent(i, carry):
            msg_copy(i).wait_send()
            return carry
        lax.fori_loop(1, 32, sent, 0)
    over_tensor(low_out, low_in, l_send, l_recv, "send")
    over_tensor(back_out, back_in, b_send, b_recv, "send")
    for i in range(1, 4):
        spread_copy(i).wait_send()

    def plane_sent(i, carry):
        plane_copy(i).wait_send()
        return carry
    lax.fori_loop(1, 8, plane_sent, 0)
    for copies in (to_other, to_far, relay):
        for part in range(2):
            copies[part].wait_send()
    def drain(j, carry):
        for g in range(2):
            @pl.when(jnp.logical_not(local(j, g)))
            def _():
                for part in range(2):
                    y_copy(j, g, part).wait_send()
            for ct in range(2):
                @pl.when(jnp.logical_and(active(j, g), jnp.logical_not(to_self(j, g, ct))))
                def _():
                    x_copy(j, g, ct).wait_send()
        return carry
    lax.fori_loop(0, 8, drain, 0)

    def mag_arrive(i, total):
        frm = (dp + i) % 32
        remote(mag_out.at[0], mag_in.at[frm], g_send.at[0], g_recv.at[frm], dp, tensor).wait_recv()
        return total + mag_in[frm]
    with jax.named_scope("c5_gmag"):
        gmag_ref[...] = lax.fori_loop(1, 32, mag_arrive, mag_out[dp])

    def mag_sent(i, carry):
        mag_copy(i).wait_send()
        return carry
    lax.fori_loop(1, 32, mag_sent, 0)


def body(hidden, weight, factor_b, factor_a, magnitude, cotangent):
    hbm_spec, vmem_spec = pl.BlockSpec(memory_space=pltpu.HBM), pl.BlockSpec(memory_space=pltpu.VMEM)
    dma, vmem = pltpu.SemaphoreType.DMA, pltpu.VMEM
    mixed, grads, gmag = pl.pallas_call(
        kernel,
        name="dora",
        out_shape=(jax.ShapeDtypeStruct((TOK, OUT), BF), jax.ShapeDtypeStruct((16, 128), F32),
                   jax.ShapeDtypeStruct((1, 128), F32)),
        in_specs=[hbm_spec] * 6,
        out_specs=(vmem_spec,) * 3,
        scratch_shapes=[
            vmem((16, HID), BF), vmem((16, COLS), BF), vmem((OUT,), F32), vmem((TOK, OUT), BF), vmem((TOK, HID), BF),
            vmem((2, 2 * TOK, HID), BF),
            vmem((8, COLS, HID), BF),
            vmem((8, 2, COLS, 2 * TOK), BF),
            vmem((8, 4, COLS, 2 * TOK), BF),
            vmem((8, 2, COLS, TOK), BF),
            vmem((2, 2, 2, COLS, TOK), BF),
            vmem((8, COLS), F32), vmem((8, 8, COLS), F32),
            vmem((16, 256), F32), vmem((16, 256), BF), vmem((4, 16, 256), BF),
            vmem((2, 16, HALF), F32), vmem((2, 1, HALF), F32), vmem((2, 1, HALF), F32), vmem((2, 1, HALF), F32),
            vmem((8, 16, TOK), F32), vmem((8, 16, TOK), F32), vmem((16, TOK), F32), vmem((16, TOK), F32),
            vmem((2, TOK, HALF), BF), vmem((2, TOK, HALF), F32), vmem((2, TOK, HALF), F32),
            vmem((4, 8, 16, 128), F32), vmem((4, 8, 16, 128), F32),
            vmem((8, 16, 128), F32), vmem((8, 16, 128), F32),
            vmem((32, 1, 128), F32), vmem((32, 1, 128), F32), vmem((2, 1, HALF), F32), vmem((2, TOK, HALF), F32),
            dma((8,)), dma((2, 4, 2)), dma((8, 2)), dma((3, 2)), dma((3, 2)),
            dma((8, 2, 2)), dma((8, 4, 2)), dma((8, 2)), dma((2, 2, 2)),
            dma((1,)), dma((8,)), dma((32,)), dma((4,)), dma((8,)), dma((8,)), dma((8,)), dma((8,)),
            dma((4,)), dma((4,)), dma((8,)), dma((8,)), dma((32,)), dma((32,)),
            pltpu.SemaphoreType.REGULAR((3,)),
        ],
        compiler_params=pltpu.CompilerParams(
            collective_id=0, has_side_effects=True, vmem_limit_bytes=55779328
        ),
    )(hidden, weight.T, factor_b.T, factor_a, magnitude, cotangent)
    return mixed, gmag[0, :18], grads[:, 72:90], grads[:, :72].T


def solution(mesh):
    return jax.shard_map(
        body,
        mesh=mesh,
        in_specs=(
            P("dp", "tensor"),
            P("tensor", "dp"),
            P("tensor", None),
            P(None, "dp"),
            P("tensor"),
            P("dp", "tensor"),
        ),
        out_specs=(
            P("dp", "tensor"),
            P(("tensor", "dp")),
            P(None, ("tensor", "dp")),
            P(("tensor", "dp"), None),
        ),
        check_vma=False,
    )
```

```python
import functools

import jax
import jax.numpy as jnp
from jax import lax
from jax.experimental import pallas as pl
from jax.experimental.pallas import tpu as pltpu
from jax.sharding import PartitionSpec as P

TOK, HID, COLS, OUT, HALF = 320, 2304, 144, 576, 288
MESH = pl.DeviceIdType.MESH
F32, BF = jnp.float32, jnp.bfloat16
CHUNKS = ((0, 80), (80, 64))
FIRST, LAST = 192, 128
PARTS = ((0, 2 * FIRST), (2 * FIRST, 2 * LAST))


def remote(src, dst, send, recv, dp, tensor):
    return pltpu.make_async_remote_copy(
        src_ref=src, dst_ref=dst, send_sem=send, recv_sem=recv,
        device_id=(dp, tensor), device_id_type=MESH,
    )


def kernel(h_ref, w_ref, b_hbm, a_hbm, mag_hbm, cot_hbm, mixed_ref, grads_ref, gmag_ref,
           b_ref, a_ref, mag_ref, cot_ref, own, toks, wts, outgoing, arrived, turned, halves,
           sq_out, sq_in, msg_f, msg, msgs, a_all, sq_all, norms, scales, low_in, back_in, low_out, back_out,
           dpre, extra, cots,
           spread, spread_in, plane, plane_in, mag_out, mag_in, sums, results,
           loc_sem, w_send, w_recv, t_send, t_recv, y_send, y_recv, x_send, x_recv,
           s_send, s_recv, m_send, m_recv, l_send, l_recv, b_send, b_recv, d_send, d_recv, p_send, p_recv,
           g_send, g_recv,
           met):
    dp, tensor = lax.axis_index("dp"), lax.axis_index("tensor")
    x_hi, z, core = dp // 16, (dp // 2) % 8, dp % 2
    x_lo, y = tensor // 4, tensor % 4
    other = 1 - core

    def dp_of(a, b, c):
        return a * 16 + b * 2 + c

    def rows(part, of):
        if part == 0:
            return pl.ds(of * FIRST, FIRST), pl.ds(0, FIRST)
        return pl.ds(2 * FIRST + of * LAST, LAST), pl.ds(FIRST, LAST)

    load_h = pltpu.make_async_copy(h_ref, own, loc_sem.at[0])
    place = []
    for part in range(2):
        there, here = rows(part, core)
        place.append(pltpu.make_async_copy(h_ref.at[here], toks.at[0, there], loc_sem.at[6 + part]))
    load_w = pltpu.make_async_copy(w_ref, wts.at[0], loc_sem.at[1])
    loads = [pltpu.make_async_copy(src, dst, loc_sem.at[2 + i]) for i, (src, dst) in enumerate(
        ((a_hbm, a_ref), (b_hbm, b_ref), (mag_hbm, mag_ref), (cot_hbm, cot_ref)))]
    load_w.start()
    loads[0].start()
    loads[1].start()
    load_h.start()
    place[0].start()
    place[1].start()
    loads[2].start()
    loads[3].start()

    barrier = pltpu.get_barrier_semaphore()

    def greet(p):
        pl.semaphore_signal(barrier, inc=1, device_id=p, device_id_type=MESH)

    near = [(dp, (tensor + k) % 8) for k in range(1, 8)]
    near += [(dp_of(x_hi, (z + 1) % 8, core), tensor), (dp_of(x_hi, (z + 7) % 8, core), tensor),
             (dp_of(x_hi, z, other), tensor), (dp_of(1 - x_hi, z, core), tensor), (dp_of(1 - x_hi, z, other), tensor)]
    for p in near:
        greet(p)
    spread[...] = jnp.zeros_like(spread)
    msg_f[...] = jnp.zeros_like(msg_f)
    load_w.wait()
    load_h.wait()
    with jax.named_scope('barrier_wait'):
        pl.semaphore_wait(barrier, len(near))

    def tell(k):
        for to in ((z + k) % 8, (z + 8 - k) % 8)[:1 if k == 4 else 2]:
            pl.semaphore_signal(met.at[k // 2], inc=1, device_id=(dp_of(x_hi, to, core), tensor), device_id_type=MESH)

    tell(1)

    def w_copy(side, k, ch):
        at, n = CHUNKS[ch]
        src = 0 if k == 1 else 2 * (k - 1) - 1 + side
        dst = 7 if k == 4 else 2 * k - 1 + side
        to = (z + 1) % 8 if side == 0 else (z + 7) % 8
        return remote(wts.at[src, pl.ds(at, n)], wts.at[dst, pl.ds(at, n)],
                      w_send.at[side, k - 1, ch], w_recv.at[dst, ch], dp_of(x_hi, to, core), tensor)

    w_copy(0, 1, 0).start()
    w_copy(1, 1, 1).start()
    w_copy(0, 1, 1).start()
    w_copy(1, 1, 0).start()
    to_other, to_far, relay = [], [], []
    for part in range(2):
        there, here = rows(part, core)
        to_other.append(remote(own.at[here], toks.at[0, there], t_send.at[0, part], t_recv.at[0, part],
                               dp_of(x_hi, z, other), tensor))
        to_far.append(remote(own.at[here], toks.at[1, there], t_send.at[1, part], t_recv.at[1, part],
                             dp_of(1 - x_hi, z, core), tensor))
        relay.append(remote(toks.at[1, there], toks.at[1, there], t_send.at[2, part], t_recv.at[2, part],
                            dp_of(x_hi, z, other), tensor))

    to_other[0].start()
    to_other[1].start()

    owner = dp // 4
    loads[0].wait()
    loads[1].wait()
    merged = wts[0].astype(F32) + lax.dot_general(
        a_ref[...], b_ref[...], (((0,), (0,)), ((), ())), preferred_element_type=F32)
    squares = merged * merged
    lanes = squares[:, 0:128]
    for i in range(1, 18):
        lanes = lanes + squares[:, 128 * i:128 * (i + 1)]
    own_sq = jnp.sum(lanes.T, axis=0, keepdims=True)
    sq_row = jnp.broadcast_to(own_sq, (8, COLS))

    @pl.when(owner == tensor)
    def _():
        sq_in[tensor] = sq_row

    @pl.when(owner != tensor)
    def _():
        sq_out[...] = sq_row

    low_part = lax.dot_general(b_ref[...], own[...], (((1,), (1,)), ((), ())), preferred_element_type=F32)
    low_out[...] = low_part
    low_in[tensor] = low_part
    sq_copy = remote(sq_out, sq_in.at[tensor], s_send.at[0], s_recv.at[tensor], dp, owner)

    @pl.when(owner != tensor)
    def _():
        sq_copy.start()

    def over_tensor(src, dst, send, recv, act):
        def body(i, carry):
            to = (tensor + i) % 8
            if act == "recv":
                remote(src, dst.at[to], send.at[i], recv.at[to], dp, to).wait_recv()
            elif act == "start":
                remote(src, dst.at[tensor], send.at[i], recv.at[tensor], dp, to).start()
            else:
                remote(src, dst.at[tensor], send.at[i], recv.at[tensor], dp, to).wait_send()
            return carry
        lax.fori_loop(1, 8, body, 0)

    over_tensor(low_out, low_in, l_send, l_recv, "start")
    to_far[0].start()
    to_far[1].start()

    pl.semaphore_wait(met.at[0], 2)
    tell(2)
    loads[2].wait()
    loads[3].wait()

    def zsrc_of(j):
        k = (j + 1) // 2
        return (z + 8 + k - 2 * k * (j % 2)) % 8

    def summer_at(owner_y, g, of):
        return (owner_y + jnp.where(g == 0, 3 - 2 * of, 2 * of)) % 4

    def summer(j, g):
        return summer_at(zsrc_of(j) // 2, g, core)

    def y_copy(j, g, part):
        lanes = pl.ds(*PARTS[part])
        return remote(outgoing.at[j, g, :, lanes], arrived.at[j, y, :, lanes], y_send.at[j, g, part],
                      y_recv.at[j, y, part], dp, x_lo * 4 + summer(j, g))

    def local(j, g):
        return summer(j, g) == y

    def item(j, g, parts):
        lo, hi = PARTS[parts[0]][0], sum(PARTS[parts[-1]])
        p = lax.dot_general(toks[g, lo:hi], wts[j], (((1,), (1,)), ((), ())), preferred_element_type=F32)
        p = p.T.astype(BF)
        here = local(j, g)

        @pl.when(here)
        def _():
            arrived[j, y, :, lo:hi] = p

        @pl.when(jnp.logical_not(here))
        def _():
            outgoing[j, g, :, lo:hi] = p
            for part in parts:
                y_copy(j, g, part).start()

    def items(lo, hi, g, parts=(0, 1)):
        def body(j, carry):
            item(j, g, parts)
            return carry
        lax.fori_loop(lo, hi, body, 0)

    def items_both(lo, hi):
        def body(i, carry):
            item(lo + i // 2, i % 2, (0, 1))
            return carry
        lax.fori_loop(0, 2 * (hi - lo), body, 0)

    def msg_copy(i):
        return remote(msg, msgs.at[dp % 4], m_send.at[i], m_recv.at[dp % 4], (dp + i) % 32, tensor)

    def publish():
        def arrive(i, carry):
            frm = (tensor + i) % 8
            remote(sq_out, sq_in.at[frm], s_send.at[0], s_recv.at[frm], dp, frm).wait_recv()
            return carry
        lax.fori_loop(1, 8, arrive, 0)
        total = sq_in[0]
        for i in range(1, 8):
            total = total + sq_in[i]
        total = total[0:1]
        high = total.astype(BF).astype(F32)
        rest = total - high
        msg_f[:, 0:COLS] = a_ref[...].astype(F32)
        for i in range(3):
            msg_f[i:i + 1, 144:192] = high[:, 48 * i:48 * (i + 1)]
            msg_f[3 + i:4 + i, 144:192] = rest[:, 48 * i:48 * (i + 1)]
        packed = msg_f[...].astype(BF)
        msg[...] = packed
        msgs[dp % 4] = packed

        def send(i, carry):
            msg_copy(i).start()
            return carry
        lax.fori_loop(1, 32, send, 0)

    def receive():
        for j in range(4):
            @pl.when(dp != tensor * 4 + j)
            def _():
                remote(msg, msgs.at[j], m_send.at[0], m_recv.at[j], dp, tensor).wait_recv()
        for j in range(4):
            m = msgs[j].astype(F32)
            zp, at = j // 2, COLS * (j % 2)
            a_all[zp, :, at:at + COLS] = m[:, 0:COLS]
            for i in range(3):
                sq_all[zp, :, at + 48 * i:at + 48 * (i + 1)] = m[i:i + 1, 144:192] + m[3 + i:4 + i, 144:192]

    def backward():
        back = None
        mags = mag_ref[...].reshape(1, OUT)
        for zp in range(2):
            norm = jnp.sqrt(sq_all[zp] + 1e-6)
            scale = mags[:, HALF * zp:HALF * (zp + 1)] / norm
            norms[zp] = norm
            scales[zp] = scale
            cot = cot_ref[:, HALF * zp:HALF * (zp + 1)].astype(F32)
            cots[zp] = cot
            d = (cot * scale).astype(BF)
            dpre[zp] = d
            part = lax.dot_general(a_all[zp].astype(BF), d, (((1,), (1,)), ((), ())), preferred_element_type=F32)
            back = part if back is None else back + part
        back_out[...] = back
        back_in[tensor] = back
        over_tensor(back_out, back_in, b_send, b_recv, "start")

    group = x_hi * 2 + core

    def spread_copy(i):
        to = (group + i) % 4
        return remote(spread.at[to], spread_in.at[group], d_send.at[i], d_recv.at[group],
                      dp_of(to // 2, z, to % 2), tensor)

    def gradients():
        over_tensor(low_out, low_in, l_send, l_recv, "recv")
        over_tensor(back_out, back_in, b_send, b_recv, "recv")
        low, back = low_in[0], back_in[0]
        for i in range(1, 8):
            low = low + low_in[i]
            back = back + back_in[i]
        low, back = low.astype(BF), back.astype(BF)
        grad_b = jnp.dot(back, own[...], preferred_element_type=F32)
        grad_a = [jnp.dot(low, dpre[zp], preferred_element_type=F32) for zp in range(2)]
        for x in range(2):
            for zz in range(8):
                for c in range(2):
                    i = x * 16 + zz * 2 + c
                    spread[x * 2 + c, zz, :, 0:72] = grad_b[:, 72 * i:72 * (i + 1)]
                    spread[x * 2 + c, zz, :, 72:90] = grad_a[x][:, 18 * (i % 16):18 * (i % 16 + 1)]
        for i in range(1, 4):
            spread_copy(i).start()
        for zp in range(2):
            extra[zp] = lax.dot_general(low, a_all[zp].astype(BF), (((0,), (0,)), ((), ())),
                                        preferred_element_type=F32)

    def plane_copy(i):
        to = (z + i) % 8
        return remote(plane.at[to], plane_in.at[z], p_send.at[i], p_recv.at[z], dp_of(x_hi, to, core), tensor)

    def sum_plane():
        total = spread[group]
        for i in range(1, 4):
            frm = (group + i) % 4
            remote(spread.at[0], spread_in.at[frm], d_send.at[0], d_recv.at[frm], dp, tensor).wait_recv()
            total = total + spread_in[frm]
        plane[...] = total

        def send(i, carry):
            plane_copy(i).start()
            return carry
        lax.fori_loop(1, 8, send, 0)

    def sum_planes():
        total = plane[z]
        for i in range(1, 8):
            frm = (z + i) % 8
            remote(plane.at[0], plane_in.at[frm], p_send.at[0], p_recv.at[frm], dp, tensor).wait_recv()
            total = total + plane_in[frm]
        grads_ref[...] = total

    def ring(k, first):
        for side in (0, 1):
            ch = first if side == 0 else 1 - first
            w_copy(side, k, ch).wait_recv()
            if k < 3 or first == 0:
                w_copy(side, k + 1, ch).start()

    def x_copy(j, g, ct):
        zs = zsrc_of(j)
        tok_hi = jnp.where(g == 0, x_hi, 1 - x_hi)
        return remote(turned.at[j, ct], halves.at[x_lo, zs % 2, core], x_send.at[j, ct],
                      x_recv.at[x_lo, zs % 2, core], dp_of(tok_hi, z, ct), x_hi * 4 + zs // 2)

    def to_self(j, g, ct):
        same = jnp.logical_and(g == 0, x_lo == x_hi)
        return jnp.logical_and(same, jnp.logical_and(zsrc_of(j) // 2 == y, core == ct))

    def active(j, g):
        return summer(j, g) == y

    def stage_two(j, g):
        for k in range(1, 4):
            ys = (y + k) % 4
            for part in range(2):
                lanes = pl.ds(*PARTS[part])
                remote(outgoing.at[0, 0, :, lanes], arrived.at[j, ys, :, lanes], y_send.at[0, 0, part],
                       y_recv.at[j, ys, part], dp, tensor).wait_recv()
        total = arrived[j, 0].astype(F32)
        for ys in range(1, 4):
            total = total + arrived[j, ys].astype(F32)
        total = total.astype(BF)
        for ct in range(2):
            part = jnp.concatenate(
                [total[:, ct * FIRST:(ct + 1) * FIRST],
                 total[:, 2 * FIRST + ct * LAST:2 * FIRST + (ct + 1) * LAST]], axis=1)
            mine_too = to_self(j, g, ct)

            @pl.when(mine_too)
            def _():
                halves[x_lo, zsrc_of(j) % 2, core] = part

            @pl.when(jnp.logical_not(mine_too))
            def _():
                turned[j, ct] = part
                x_copy(j, g, ct).start()

    def second(lo, hi, g):
        def unit(j, carry):
            pl.when(active(j, g))(lambda: stage_two(j, g))
            return carry
        lax.fori_loop(lo, hi, unit, 0)

    def steps_of(zp):
        away = (2 * y + zp - z + 8) % 8
        return jnp.where(away > 4, 8 - away, away)

    with jax.named_scope("a0"):
        for part in range(2):
            place[part].wait()
            to_other[part].wait_recv()
    items(0, 1, 0)
    pl.semaphore_wait(met.at[1], 2)
    tell(4)

    def publish_when_met():
        pl.semaphore_wait(met.at[2], 1)
        publish()
    with jax.named_scope("a1_publish"):
        pl.when(owner == tensor)(publish_when_met)
    with jax.named_scope("a2_ring10"):
        ring(1, 0)

    @pl.when(owner != tensor)
    def _():
        pl.semaphore_wait(met.at[2], 1)
    with jax.named_scope("a3_ring11"):
        ring(1, 1)
    items(1, 3, 0)
    with jax.named_scope("a4_far0"):
        to_far[0].wait_recv()
    relay[0].start()
    with jax.named_scope("a5_ring20"):
        ring(2, 0)
    with jax.named_scope("a6_relay0"):
        relay[0].wait_recv()
    items(0, 3, 1, (0,))
    with jax.named_scope("a8_ring21"):
        ring(2, 1)
    items(3, 5, 0)
    items(3, 5, 1, (0,))
    with jax.named_scope("a9_far1"):
        to_far[1].wait_recv()
    relay[1].start()
    with jax.named_scope("aa_receive"):
        receive()
    backward()
    with jax.named_scope("aa_second"):
        second(0, 3, 0)
    with jax.named_scope("ab_relay1"):
        relay[1].wait_recv()
    items(0, 5, 1, (1,))
    with jax.named_scope("ac_ring30"):
        ring(3, 0)
    with jax.named_scope("b1_ring31"):
        ring(3, 1)
    with jax.named_scope("b2_items"):
        items_both(5, 7)
    with jax.named_scope("b3_second"):
        second(3, 5, 0)
    with jax.named_scope("b5_last"):
        w_copy(0, 4, 0).wait_recv()
        w_copy(1, 4, 1).wait_recv()
    with jax.named_scope("b6_items"):
        items_both(7, 8)
    with jax.named_scope("b9_second"):
        second(0, 5, 1)
    with jax.named_scope("ba_second"):
        second(5, 7, 0)
        second(5, 7, 1)
    with jax.named_scope("b8_grads"):
        gradients()
    with jax.named_scope("bb_second"):
        second(7, 8, 0)
        second(7, 8, 1)

    def finish(i, carry):
        zp = jnp.where(steps_of(0) <= steps_of(1), i, 1 - i)
        away = jnp.where(x_lo == x_hi, 0, 1)
        parts = []
        for cs in range(2):
            for xl in range(2):
                frm = summer_at(y, away, cs)
                own_part = jnp.logical_and(jnp.logical_and(x_lo == x_hi, xl == x_lo),
                                           jnp.logical_and(frm == y, core == cs))

                @pl.when(jnp.logical_not(own_part))
                def _():
                    remote(turned.at[0, 0], halves.at[xl, zp, cs], x_send.at[0, 0], x_recv.at[xl, zp, cs],
                           dp, tensor).wait_recv()
            parts.append(halves[0, zp, cs].astype(F32) + halves[1, zp, cs].astype(F32))
        pre = extra[zp] + jnp.concatenate(parts, axis=0).T
        sums[zp] = jnp.sum(cots[zp] * pre, axis=0, keepdims=True) / norms[zp]
        results[zp] = pre * scales[zp]
        return carry
    with jax.named_scope("c0_finish"):
        lax.fori_loop(0, 2, finish, 0)
    for i in range(32):
        mag_out[i, :, 0:18] = sums[i // 16][:, 18 * (i % 16):18 * (i % 16 + 1)]

    def mag_copy(i):
        to = (dp + i) % 32
        return remote(mag_out.at[to], mag_in.at[dp], g_send.at[i], g_recv.at[dp], to, tensor)

    def mag_start(i, carry):
        mag_copy(i).start()
        return carry
    with jax.named_scope("c1_mag"):
        lax.fori_loop(1, 32, mag_start, 0)
    with jax.named_scope("c2_plane"):
        sum_plane()
    with jax.named_scope("c2_mixed"):
        for zp in range(2):
            mixed_ref[:, HALF * zp:HALF * (zp + 1)] = results[zp].astype(BF)
    with jax.named_scope("c4_planes"):
        sum_planes()

    for k in (1, 2, 3, 4):
        for side in (0, 1):
            for ch in (0, 1):
                if k < 4 or ch == side:
                    w_copy(side, k, ch).wait_send()
    @pl.when(owner != tensor)
    def _():
        sq_copy.wait_send()

    @pl.when(owner == tensor)
    def _():
        def sent(i, carry):
            msg_copy(i).wait_send()
            return carry
        lax.fori_loop(1, 32, sent, 0)
    over_tensor(low_out, low_in, l_send, l_recv, "send")
    over_tensor(back_out, back_in, b_send, b_recv, "send")
    for i in range(1, 4):
        spread_copy(i).wait_send()

    def plane_sent(i, carry):
        plane_copy(i).wait_send()
        return carry
    lax.fori_loop(1, 8, plane_sent, 0)
    for copies in (to_other, to_far, relay):
        for part in range(2):
            copies[part].wait_send()
    def drain(j, carry):
        for g in range(2):
            @pl.when(jnp.logical_not(local(j, g)))
            def _():
                for part in range(2):
                    y_copy(j, g, part).wait_send()
            for ct in range(2):
                @pl.when(jnp.logical_and(active(j, g), jnp.logical_not(to_self(j, g, ct))))
                def _():
                    x_copy(j, g, ct).wait_send()
        return carry
    lax.fori_loop(0, 8, drain, 0)

    def mag_arrive(i, total):
        frm = (dp + i) % 32
        remote(mag_out.at[0], mag_in.at[frm], g_send.at[0], g_recv.at[frm], dp, tensor).wait_recv()
        return total + mag_in[frm]
    with jax.named_scope("c5_gmag"):
        gmag_ref[...] = lax.fori_loop(1, 32, mag_arrive, mag_out[dp])

    def mag_sent(i, carry):
        mag_copy(i).wait_send()
        return carry
    lax.fori_loop(1, 32, mag_sent, 0)


def body(hidden, weight, factor_b, factor_a, magnitude, cotangent):
    hbm_spec, vmem_spec = pl.BlockSpec(memory_space=pltpu.HBM), pl.BlockSpec(memory_space=pltpu.VMEM)
    dma, vmem = pltpu.SemaphoreType.DMA, pltpu.VMEM
    mixed, grads, gmag = pl.pallas_call(
        kernel,
        name="dora",
        out_shape=(jax.ShapeDtypeStruct((TOK, OUT), BF), jax.ShapeDtypeStruct((16, 128), F32),
                   jax.ShapeDtypeStruct((1, 128), F32)),
        in_specs=[hbm_spec] * 6,
        out_specs=(vmem_spec,) * 3,
        scratch_shapes=[
            vmem((16, HID), BF), vmem((16, COLS), BF), vmem((OUT,), F32), vmem((TOK, OUT), BF), vmem((TOK, HID), BF),
            vmem((2, 2 * TOK, HID), BF),
            vmem((8, COLS, HID), BF),
            vmem((8, 2, COLS, 2 * TOK), BF),
            vmem((8, 4, COLS, 2 * TOK), BF),
            vmem((8, 2, COLS, TOK), BF),
            vmem((2, 2, 2, COLS, TOK), BF),
            vmem((8, COLS), F32), vmem((8, 8, COLS), F32),
            vmem((16, 256), F32), vmem((16, 256), BF), vmem((4, 16, 256), BF),
            vmem((2, 16, HALF), F32), vmem((2, 1, HALF), F32), vmem((2, 1, HALF), F32), vmem((2, 1, HALF), F32),
            vmem((8, 16, TOK), F32), vmem((8, 16, TOK), F32), vmem((16, TOK), F32), vmem((16, TOK), F32),
            vmem((2, TOK, HALF), BF), vmem((2, TOK, HALF), F32), vmem((2, TOK, HALF), F32),
            vmem((4, 8, 16, 128), F32), vmem((4, 8, 16, 128), F32),
            vmem((8, 16, 128), F32), vmem((8, 16, 128), F32),
            vmem((32, 1, 128), F32), vmem((32, 1, 128), F32), vmem((2, 1, HALF), F32), vmem((2, TOK, HALF), F32),
            dma((8,)), dma((2, 4, 2)), dma((8, 2)), dma((3, 2)), dma((3, 2)),
            dma((8, 2, 2)), dma((8, 4, 2)), dma((8, 2)), dma((2, 2, 2)),
            dma((1,)), dma((8,)), dma((32,)), dma((4,)), dma((8,)), dma((8,)), dma((8,)), dma((8,)),
            dma((4,)), dma((4,)), dma((8,)), dma((8,)), dma((32,)), dma((32,)),
            pltpu.SemaphoreType.REGULAR((3,)),
        ],
        compiler_params=pltpu.CompilerParams(
            collective_id=0, has_side_effects=True, vmem_limit_bytes=55779328
        ),
    )(hidden, weight.T, factor_b.T, factor_a, magnitude, cotangent)
    return mixed, gmag[0, :18], grads[:, 72:90], grads[:, :72].T


def solution(mesh):
    return jax.shard_map(
        body,
        mesh=mesh,
        in_specs=(
            P("dp", "tensor"),
            P("tensor", "dp"),
            P("tensor", None),
            P(None, "dp"),
            P("tensor"),
            P("dp", "tensor"),
        ),
        out_specs=(
            P("dp", "tensor"),
            P(("tensor", "dp")),
            P(None, ("tensor", "dp")),
            P(("tensor", "dp"), None),
        ),
        check_vma=False,
    )
```
